32 devices in a mesh: data: 32 (over z, y, x, core).
Axes of the slice: x: 2, y: 2, z: 4, core: 2. Of those that a mesh axis runs over, the one named last changes fastest.
Arguments:
- act_in: bfloat16 [16384, 1024], P('data')
- pre_act: bfloat16 [16384, 4096], P('data')
- grad_out: bfloat16 [16384, 4096], P('data')
- q_init: float32 [4096, 8], replicated
- err_mem: float32 [32, 1024, 4096], P('data')
Outputs:
- output 1: float32 [1024, 8], replicated
- output 2: float32 [4096, 8], replicated
- output 3: float32 [32, 1024, 4096], P('data')
All inputs are finite; a program needn't handle non-finite values.
Results may differ from the reference program's by a relative error of at most 0.001.
Values sent between devices are 32-bit elements.
A program may use at most 1 GiB of HBM per device.

```python
import math
import jax
import jax.numpy as jnp
from jax import lax

GROUP_SIZE = 32
TOKENS = 512
D_IN = 1024
D_OUT = 4096
LOW_RANK = 8

MIX_RANK = 4 * LOW_RANK
COHERE = 2.0 * math.sqrt(max(1.0, D_IN / TOKENS))
DY_SCALE = math.sqrt(TOKENS)
ERR_SCALE = 0.6 * math.sqrt(1.0 + COHERE * COHERE)
EXACT_PREC = lax.Precision.HIGHEST


def setup_inputs(seed: int = 0) -> dict:
    key_list = jax.random.split(jax.random.key(seed), 7)
    all_rows = GROUP_SIZE * TOKENS
    act_f32 = jax.random.normal(key_list[0], (all_rows, D_IN), jnp.float32)
    mix_left = jax.random.normal(key_list[1], (D_IN, MIX_RANK), jnp.float32) * D_IN ** -0.5
    mix_right = jax.random.normal(key_list[2], (MIX_RANK, D_OUT), jnp.float32) * MIX_RANK ** -0.5
    signal = jnp.dot(jnp.dot(act_f32, mix_left), mix_right)
    noise_part = jax.random.normal(key_list[3], (all_rows, D_OUT), jnp.float32)
    grad_out = (COHERE * signal + noise_part) * DY_SCALE
    pre_act = jax.random.normal(key_list[4], (all_rows, D_OUT), jnp.float32)
    q_init = jax.random.normal(key_list[5], (D_OUT, LOW_RANK), jnp.float32) * D_OUT ** -0.5
    err_mem = jax.random.normal(key_list[6], (GROUP_SIZE, D_IN, D_OUT), jnp.float32) * ERR_SCALE
    return {'act_in': act_f32.astype(jnp.bfloat16), 'pre_act': pre_act.astype(jnp.bfloat16), 'grad_out': grad_out.astype(jnp.bfloat16), 'q_init': q_init, 'err_mem': err_mem}


def gelu_grad(pre_act, grad_out):
    z_f32 = pre_act.astype(jnp.float32)
    _, pullback = jax.vjp(jax.nn.gelu, z_f32)
    return pullback(grad_out.astype(jnp.float32))[0]


def orthonormalize(p_sum):
    def gs_step(col_idx, ortho_cols):
        column = lax.dynamic_slice_in_dim(p_sum, col_idx, 1, axis=1)
        proj_coef = jnp.dot(column.T, ortho_cols, precision=EXACT_PREC)
        residual = column - jnp.dot(ortho_cols, proj_coef.T, precision=EXACT_PREC)
        unit_col = residual / jnp.sqrt(jnp.sum(residual * residual))
        return lax.dynamic_update_slice_in_dim(ortho_cols, unit_col, col_idx, axis=1)
    return lax.fori_loop(0, p_sum.shape[1], gs_step, jnp.zeros_like(p_sum))


def reference(act_in, pre_act, grad_out, q_init, err_mem):
    act_dev = act_in.reshape(GROUP_SIZE, TOKENS, D_IN)
    pre_dev = pre_act.reshape(GROUP_SIZE, TOKENS, D_OUT)
    dy_dev = grad_out.reshape(GROUP_SIZE, TOKENS, D_OUT)

    def merged_grad(blk_tuple):
        act_blk, pre_blk, dy_blk, err_blk = blk_tuple
        grad_pre = gelu_grad(pre_blk, dy_blk).astype(jnp.bfloat16)
        grad_w = jnp.dot(act_blk.T, grad_pre, preferred_element_type=jnp.float32) / TOKENS
        return grad_w + err_blk

    merged = lax.map(merged_grad, (act_dev, pre_dev, dy_dev, err_mem))
    p_sum = jnp.einsum('gij,jr->ir', merged, q_init, precision=EXACT_PREC)
    p_factor = orthonormalize(p_sum)
    q_factor = jnp.einsum('gij,ir->jr', merged, p_factor, precision=EXACT_PREC) / GROUP_SIZE
    err_new = merged - jnp.dot(p_factor, q_factor.T, precision=EXACT_PREC)[None]
    return p_factor, q_factor, err_new
```

```python
import functools

import jax
import jax.numpy as jnp
from jax import lax
from jax.experimental import pallas as pl
from jax.experimental.pallas import tpu as pltpu
from jax.sharding import PartitionSpec as P

F32 = jnp.float32
BF16 = jnp.bfloat16
MESH = pl.DeviceIdType.MESH
RANK = 8
CB = 256
RB = 256
NT = (((1,), (1,)), ((), ()))


def split3(x):
    hi = x.astype(BF16)
    rest = x - hi.astype(F32)
    mid = rest.astype(BF16)
    low = (rest - mid.astype(F32)).astype(BF16)
    return hi, mid, low


def stack3(x):
    parts = [p.astype(F32) for p in split3(x)]
    return jnp.concatenate(parts + [jnp.zeros_like(x)], axis=0).astype(BF16)


def fold3(y):
    return (y[16:24] + y[8:16]) + y[0:8]


def mm(a, b):
    return jnp.dot(a, b, preferred_element_type=F32)


def mm_nt(a, b):
    return lax.dot_general(a, b, NT, preferred_element_type=F32)


def gelu_grad(z, dy):
    c = 0.7978845608028654
    x = z.astype(F32)
    x2 = x * x
    t = jnp.tanh(x * (x2 * (c * 0.044715) + c))
    up = 1.0 + t
    slope = ((x * up) * (1.0 - t)) * (x2 * (1.5 * c * 0.044715) + 0.5 * c)
    return (0.5 * up + slope) * dy.astype(F32)


def orthonormalize(p):
    row = lax.broadcasted_iota(jnp.int32, (RANK, 1), 0)
    w = p
    norm2 = jnp.zeros((RANK, 1), F32)
    for j in range(RANK):
        v = w[j:j + 1]
        d = jnp.sum(jnp.where(row > j, p, w) * v, axis=1, keepdims=True)
        norm2 = jnp.where(row == j, d, norm2)
        if j + 1 < RANK:
            coef = jnp.where(row > j, d / d[j:j + 1], 0.0)
            w = w - coef * v
    return w / jnp.sqrt(norm2)


def reduce_kernel(n, a_hbm, z_hbm, dy_hbm, qt_ref, e_hbm, pleft_ref, pt_ref, q_ref, m_ref,
                  parts, g, a_v, at_v, qs, p_acc, h_acc, p_own, p_recv, p_all, y_own, y_recv,
                  in_sem, a_sem, ps_sem, pr_sem, pbs_sem, pbr_sem, ys_sem, yr_sem, ybs_sem, ybr_sem):
    me = lax.axis_index("data")
    d_in, d_out = m_ref.shape
    tokens = g.shape[0]
    nc = d_out // CB
    n_p = d_in // 128
    n_y = n // 2
    cw = d_out // n_y
    base = n // 4
    rel = lax.rem(me + (n - base), n)
    p_owner = (rel < 2 * n_p) & (lax.rem(rel, 2) == 1)
    p_mine = jnp.minimum(lax.div(rel, 2), n_p - 1)
    y_owner = rel < n_y
    y_mine = jnp.minimum(rel, n_y - 1)

    barrier = pltpu.get_barrier_semaphore()

    @pl.loop(1, n)
    def _(k):
        pl.semaphore_signal(barrier, inc=1, device_id=(lax.rem(me + k, n),), device_id_type=MESH)

    def e_copy(c):
        cols = pl.ds(pl.multiple_of(c * CB, CB), CB)
        return pltpu.make_async_copy(e_hbm.at[0, :, cols], m_ref.at[:, cols], in_sem.at[0, c])

    def z_copy(c):
        cols = pl.ds(pl.multiple_of(c * CB, CB), CB)
        return pltpu.make_async_copy(z_hbm.at[:, cols], parts.at[pl.ds(0, tokens), cols], in_sem.at[1, c])

    def dy_copy(c):
        cols = pl.ds(pl.multiple_of(c * CB, CB), CB)
        return pltpu.make_async_copy(dy_hbm.at[:, cols], parts.at[pl.ds(tokens, tokens), cols], in_sem.at[2, c])

    a_copy = pltpu.make_async_copy(a_hbm, a_v, a_sem)

    @pl.loop(0, nc)
    def _(c):
        e_copy(c).start()
        z_copy(c).start()
        dy_copy(c).start()

        @pl.when(c == nc // 2)
        def _():
            a_copy.start()

    qt = qt_ref[...]
    q_max = jnp.max(jnp.abs(qt), axis=1, keepdims=True)
    qs[...] = stack3((qt / q_max) * (1.0 / d_out))
    p_acc[...] = jnp.zeros_like(p_acc)
    h_acc[...] = jnp.zeros_like(h_acc)

    @pl.loop(0, nc)
    def _(c):
        e_copy(c).wait()
        z_copy(c).wait()
        dy_copy(c).wait()
        cols = pl.ds(pl.multiple_of(c * CB, CB), CB)
        qc = qs[:, cols]
        for r in range(d_in // RB):
            rows = pl.ds(r * RB, RB)
            e1, e2, e3 = split3(m_ref[rows, cols])
            p_acc[:, rows] += (mm_nt(qc, e3) + mm_nt(qc, e2)) + mm_nt(qc, e1)
        for r in range(tokens // RB):
            rows = pl.ds(r * RB, RB)
            gb = gelu_grad(parts[rows, cols], parts[pl.ds(tokens + r * RB, RB), cols]).astype(BF16)
            g[rows, cols] = gb
            h_acc[:, rows] += mm_nt(qc, gb)

    a_copy.wait()
    hs = stack3(fold3(h_acc[...]))
    pt = (fold3(p_acc[...]) + fold3(mm(hs, a_v[...])) * (1.0 / tokens)) * q_max * float(d_out)
    for b in range(n_p):
        p_own[b] = pt[:, b * 128:(b + 1) * 128]

    pl.semaphore_wait(barrier, n - 1)

    def p_send(b):
        owner = base + 2 * b + 1
        return pltpu.make_async_remote_copy(
            src_ref=p_own.at[b], dst_ref=p_recv.at[lax.rem(me - owner + 2 * n - 1, n)],
            send_sem=ps_sem, recv_sem=pr_sem, device_id=(owner,), device_id_type=MESH)

    for b in range(n_p):
        @pl.when(me != base + 2 * b + 1)
        def _():
            p_send(b).start()

    at_v[...] = a_v[...].T

    def build(c):
        cols = pl.ds(pl.multiple_of(c * CB, CB), CB)
        for r in range(d_in // RB):
            rows = pl.ds(r * RB, RB)
            m = mm(at_v[rows, :], g[:, cols]) * (1.0 / tokens) + m_ref[rows, cols]
            m_ref[rows, cols] = m
            for i, part in enumerate(split3(m)):
                parts[pl.ds(i * d_in + r * RB, RB), cols] = part

    pl.loop(0, nc // 2)(build)

    def spread(buf, index, send_sem, recv_sem, k):
        return pltpu.make_async_remote_copy(
            src_ref=buf.at[index], dst_ref=buf.at[index], send_sem=send_sem, recv_sem=recv_sem,
            device_id=(lax.rem(me + k, n),), device_id_type=MESH)

    def bulk(ref, send_sem, recv_sem):
        return pltpu.make_async_remote_copy(
            src_ref=ref, dst_ref=ref, send_sem=send_sem, recv_sem=recv_sem, device_id=(me,), device_id_type=MESH)

    @pl.when(p_owner)
    def _():
        bulk(p_recv, ps_sem, pr_sem).wait_recv()
        p_all[p_mine] = p_own[p_mine] + jnp.sum(p_recv[...], axis=0)

        @pl.loop(1, n)
        def _(k):
            spread(p_all, p_mine, pbs_sem, pbr_sem.at[p_mine], k).start()

    pl.loop(nc // 2, nc)(build)

    for b in range(n_p):
        @pl.when(me != base + 2 * b + 1)
        def _():
            bulk(p_all.at[b], pbs_sem, pbr_sem.at[b]).wait_recv()

    p = orthonormalize(jnp.concatenate([p_all[b] for b in range(n_p)], axis=1))
    pt_ref[...] = p
    ps = stack3(p)

    def y_send(t):
        owner = base + t
        return pltpu.make_async_remote_copy(
            src_ref=y_own.at[t], dst_ref=y_recv.at[lax.rem(me - owner + 2 * n - 1, n)],
            send_sem=ys_sem, recv_sem=yr_sem, device_id=(owner,), device_id_type=MESH)

    @pl.loop(0, n_y // 2)
    def _(s):
        for i in range(2):
            t = 2 * s + i
            cols = pl.ds(pl.multiple_of(t * cw, cw), cw)
            y = mm(ps, parts[pl.ds(2 * d_in, d_in), cols]) + mm(ps, parts[pl.ds(d_in, d_in), cols])
            y_own[t] = fold3(y + mm(ps, parts[pl.ds(0, d_in), cols]))
        for i in range(2):
            t = 2 * s + i

            @pl.when(me != base + t)
            def _():
                y_send(t).start()

    p1, p2, p3 = [x.astype(F32) for x in split3(p)]
    fill = jnp.zeros((128 - 9 * RANK, d_in), F32)
    pleft_ref[...] = jnp.concatenate([p1] * 3 + [p2] * 3 + [p3] * 3 + [fill], axis=0).T.astype(BF16)

    @pl.when(y_owner)
    def _():
        bulk(y_recv, ys_sem, yr_sem).wait_recv()
        q_ref[y_mine] = (y_own[y_mine] + jnp.sum(y_recv[...], axis=0)) * (1.0 / n)

        @pl.loop(1, n)
        def _(k):
            spread(q_ref, y_mine, ybs_sem, ybr_sem.at[y_mine], k).start()

    for t in range(n_y):
        @pl.when(me != base + t)
        def _():
            bulk(q_ref.at[t], ybs_sem, ybr_sem.at[t]).wait_recv()

    @pl.when(p_owner)
    def _():
        bulk(p_own.at[pl.ds(0, n_p - 1)], ps_sem, pr_sem).wait_send()
        bulk(p_recv, pbs_sem, pr_sem).wait_send()

    @pl.when(jnp.logical_not(p_owner))
    def _():
        bulk(p_own, ps_sem, pr_sem).wait_send()

    @pl.when(y_owner)
    def _():
        bulk(y_own.at[pl.ds(0, n_y - 1)], ys_sem, yr_sem).wait_send()
        bulk(y_recv, ybs_sem, yr_sem).wait_send()

    @pl.when(jnp.logical_not(y_owner))
    def _():
        bulk(y_own, ys_sem, yr_sem).wait_send()


def apply_kernel(pleft_ref, pt_ref, q_ref, m_ref, p_out, q_out, e_out, qr, qt, stage, sem, e_sem):
    d_in, d_out = m_ref.shape
    n_y, _, cw = q_ref.shape
    p_copy = pltpu.make_async_copy(pt_ref, p_out, sem.at[0])
    p_copy.start()
    fill = jnp.zeros((128 - 9 * RANK, cw), F32)
    for t in range(n_y):
        q = q_ref[t]
        qt[:, t * cw:(t + 1) * cw] = q
        three = [x.astype(F32) for x in split3(q)]
        qr[:, t * cw:(t + 1) * cw] = jnp.concatenate(three * 3 + [fill], axis=0).astype(BF16)
    q_copy = pltpu.make_async_copy(qt, q_out, sem.at[1])
    q_copy.start()

    def e_copy(c):
        cols = pl.ds(pl.multiple_of(c * CB, CB), CB)
        return pltpu.make_async_copy(stage.at[:, cols], e_out.at[0, :, cols], e_sem.at[c])

    @pl.loop(0, d_out // CB)
    def _(c):
        cols = pl.ds(pl.multiple_of(c * CB, CB), CB)
        qc = qr[:, cols]
        for r in range(d_in // RB):
            rows = pl.ds(r * RB, RB)
            stage[rows, cols] = m_ref[rows, cols] - mm(pleft_ref[rows, :], qc)
        e_copy(c).start()

    p_copy.wait()
    q_copy.wait()

    @pl.loop(0, d_out // CB)
    def _(c):
        e_copy(c).wait()


def solution(mesh):
    n = mesh.shape["data"]

    def per_device(act_in, pre_act, grad_out, q_init, err_mem):
        tokens, d_in = act_in.shape
        d_out = pre_act.shape[1]
        nc, n_p, n_y = d_out // CB, d_in // 128, n // 2
        cw = d_out // n_y
        hbm = pl.BlockSpec(memory_space=pltpu.HBM)
        vmem = pl.BlockSpec(memory_space=pltpu.VMEM)
        pleft, pt, q, m = pl.pallas_call(
            functools.partial(reduce_kernel, n),
            out_shape=(
                pltpu.VMEM((d_in, 128), BF16),
                pltpu.VMEM((RANK, d_in), F32),
                pltpu.VMEM((n_y, RANK, cw), F32),
                pltpu.VMEM((d_in, d_out), F32),
            ),
            in_specs=[hbm, hbm, hbm, vmem, hbm],
            out_specs=(vmem,) * 4,
            scratch_shapes=[
                pltpu.VMEM((3 * d_in, d_out), BF16),
                pltpu.VMEM((tokens, d_out), BF16),
                pltpu.VMEM((tokens, d_in), BF16),
                pltpu.VMEM((d_in, tokens), BF16),
                pltpu.VMEM((32, d_out), BF16),
                pltpu.VMEM((32, d_in), F32),
                pltpu.VMEM((32, tokens), F32),
                pltpu.VMEM((n_p, RANK, 128), F32),
                pltpu.VMEM((n - 1, RANK, 128), F32),
                pltpu.VMEM((n_p, RANK, 128), F32),
                pltpu.VMEM((n_y, RANK, cw), F32),
                pltpu.VMEM((n - 1, RANK, cw), F32),
                pltpu.SemaphoreType.DMA((3, nc)),
                pltpu.SemaphoreType.DMA,
                pltpu.SemaphoreType.DMA,
                pltpu.SemaphoreType.DMA,
                pltpu.SemaphoreType.DMA,
                pltpu.SemaphoreType.DMA((n_p,)),
                pltpu.SemaphoreType.DMA,
                pltpu.SemaphoreType.DMA,
                pltpu.SemaphoreType.DMA,
                pltpu.SemaphoreType.DMA((n_y,)),
            ],
            compiler_params=pltpu.CompilerParams(
                collective_id=0, has_side_effects=True, vmem_limit_bytes=42 * 1024 * 1024),
            name="reduce_kernel",
        )(act_in, pre_act, grad_out, q_init.T, err_mem)
        p_t, q_t, err_new = pl.pallas_call(
            apply_kernel,
            out_shape=(
                jax.ShapeDtypeStruct((RANK, d_in), F32),
                jax.ShapeDtypeStruct((RANK, d_out), F32),
                jax.ShapeDtypeStruct((1, d_in, d_out), F32),
            ),
            in_specs=[vmem] * 4,
            out_specs=(hbm,) * 3,
            scratch_shapes=[
                pltpu.VMEM((128, d_out), BF16),
                pltpu.VMEM((RANK, d_out), F32),
                pltpu.VMEM((d_in, d_out), F32),
                pltpu.SemaphoreType.DMA((2,)),
                pltpu.SemaphoreType.DMA((nc,)),
            ],
            compiler_params=pltpu.CompilerParams(vmem_limit_bytes=24 * 1024 * 1024),
            name="apply_kernel",
        )(pleft, pt, q, m)
        return p_t.T, q_t.T, err_new

    return jax.shard_map(
        per_device, mesh=mesh,
        in_specs=(P("data", None), P("data", None), P("data", None), P(None, None), P("data", None, None)),
        out_specs=(P(None, None), P(None, None), P("data", None, None)), check_vma=False)
```

```python
import functools

import jax
import jax.numpy as jnp
from jax import lax
from jax.experimental import pallas as pl
from jax.experimental.pallas import tpu as pltpu
from jax.sharding import PartitionSpec as P

F32 = jnp.float32
BF16 = jnp.bfloat16
MESH = pl.DeviceIdType.MESH
RANK = 8
CB = 256
RB = 256
NT = (((1,), (1,)), ((), ()))


def split3(x):
    hi = x.astype(BF16)
    rest = x - hi.astype(F32)
    mid = rest.astype(BF16)
    low = (rest - mid.astype(F32)).astype(BF16)
    return hi, mid, low


def stack3(x):
    parts = [p.astype(F32) for p in split3(x)]
    return jnp.concatenate(parts + [jnp.zeros_like(x)], axis=0).astype(BF16)


def fold3(y):
    return (y[16:24] + y[8:16]) + y[0:8]


def mm(a, b):
    return jnp.dot(a, b, preferred_element_type=F32)


def mm_nt(a, b):
    return lax.dot_general(a, b, NT, preferred_element_type=F32)


def gelu_grad(z, dy):
    c = 0.7978845608028654
    x = z.astype(F32)
    x2 = x * x
    t = jnp.tanh(x * (x2 * (c * 0.044715) + c))
    up = 1.0 + t
    slope = ((x * up) * (1.0 - t)) * (x2 * (1.5 * c * 0.044715) + 0.5 * c)
    return (0.5 * up + slope) * dy.astype(F32)


def orthonormalize(p):
    row = lax.broadcasted_iota(jnp.int32, (RANK, 1), 0)
    w = p
    norm2 = jnp.zeros((RANK, 1), F32)
    for j in range(RANK):
        v = w[j:j + 1]
        d = jnp.sum(jnp.where(row > j, p, w) * v, axis=1, keepdims=True)
        norm2 = jnp.where(row == j, d, norm2)
        if j + 1 < RANK:
            coef = jnp.where(row > j, d / d[j:j + 1], 0.0)
            w = w - coef * v
    return w / jnp.sqrt(norm2)


def far_first():
    places = [(i, fy, fx, fc) for i in range(4) for fy in range(2) for fx in range(2) for fc in range(2)]
    places.remove((3, 0, 0, 0))
    return sorted(places, key=lambda p: -((2, 1, 1, 0)[p[0]] + p[1] + p[2]))


def reduce_kernel(n, a_hbm, z_hbm, dy_hbm, qt_hbm, e_hbm, pleft_ref, pt_ref, q_ref, m_ref,
                  parts, g, z_v, dy_v, a_v, at_v, qt_v, qs, p_acc, h_acc, p_own, p_recv, p_all,
                  y_mate, y_own, y_recv,
                  in_sem, q_sem, a_sem, ps_sem, pr_sem, pbs_sem, pbr_sem,
                  ms_sem, mr_sem, ys_sem, yr_sem, ybs_sem, ybr_sem):
    me = lax.axis_index("data")
    d_in, d_out = m_ref.shape
    tokens = z_v.shape[0]
    n_p = d_in // 128
    n_half = y_own.shape[0]
    cw = d_out // (2 * n_half)
    core = lax.rem(me, 2)
    fx = lax.rem(lax.div(me, 2), 2)
    fy = lax.rem(lax.div(me, 4), 2)
    fz = lax.div(me, 8)
    central = (fz >= 1) & (fz <= 2)
    mine = jnp.minimum(jnp.maximum(fz - 1, 0), 1) + 2 * (fx + 2 * fy)

    def owner_chip(s):
        return 4 * (1 + lax.rem(s, 2)) + lax.div(s, 2)

    barrier = pltpu.get_barrier_semaphore()

    def e_copy(c):
        cols = pl.ds(pl.multiple_of(c * CB, CB), CB)
        return pltpu.make_async_copy(e_hbm.at[0, :, cols], m_ref.at[:, cols], in_sem.at[c])

    def z_copy(c):
        cols = pl.ds(pl.multiple_of(c * CB, CB), CB)
        return pltpu.make_async_copy(z_hbm.at[:, cols], z_v.at[:, cols], in_sem.at[c])

    def dy_copy(c):
        cols = pl.ds(pl.multiple_of(c * CB, CB), CB)
        return pltpu.make_async_copy(dy_hbm.at[:, cols], dy_v.at[:, cols], in_sem.at[c])

    nc = d_out // CB
    q_copy = pltpu.make_async_copy(qt_hbm, qt_v, q_sem)
    a_copy = pltpu.make_async_copy(a_hbm, a_v, a_sem)
    q_copy.start()

    @pl.loop(0, nc)
    def _(c):
        z_copy(c).start()
        dy_copy(c).start()
        e_copy(c).start()

        @pl.when(c == nc // 2)
        def _():
            a_copy.start()

    @pl.loop(1, n)
    def _(k):
        pl.semaphore_signal(barrier, inc=1, device_id=(lax.rem(me + k, n),), device_id_type=MESH)

    p_acc[...] = jnp.zeros_like(p_acc)
    h_acc[...] = jnp.zeros_like(h_acc)
    q_copy.wait()
    qt = qt_v[...]
    q_max = jnp.max(jnp.abs(qt), axis=1, keepdims=True)
    qs[...] = stack3((qt / q_max) * (1.0 / d_out))

    def arrive(c):
        whole = parts.at[pl.ds(2 * c, 2), pl.ds(0, 2 * (d_in + tokens))]
        pltpu.make_async_copy(whole, whole, in_sem.at[c]).wait()

    def stream(first, count):
        for i in range(count):
            arrive(first + i)
        for i in range(count):
            c = first + i
            cols = pl.ds(pl.multiple_of(c * CB, CB), CB)
            qc = qs[:, cols]
            for r in range(d_in // RB):
                rows = pl.ds(r * RB, RB)
                e1, e2, e3 = split3(m_ref[rows, cols])
                p_acc[:, rows] += (mm_nt(qc, e3) + mm_nt(qc, e2)) + mm_nt(qc, e1)
                if r % 2 == 1 and r // 2 < tokens // RB:
                    rows = pl.ds(r // 2 * RB, RB)
                    gb = gelu_grad(z_v[rows, cols], dy_v[rows, cols]).astype(BF16)
                    for h in range(CB // 128):
                        g[2 * c + h, rows, :] = gb[:, h * 128:(h + 1) * 128]
                    h_acc[:, rows] += mm_nt(qc, gb)

    stream(0, 1)

    @pl.loop(0, (nc - 2) // 2)
    def _(s):
        stream(1 + 2 * s, 2)

    stream(nc - 1, 1)

    a_copy.wait()
    hs = stack3(fold3(h_acc[...]))
    pt = (fold3(p_acc[...]) + fold3(mm(hs, a_v[...])) * (1.0 / tokens)) * q_max * float(d_out)
    for b in range(n_p):
        p_own[b] = pt[:, b * 128:(b + 1) * 128]

    pl.semaphore_wait(barrier, n - 1)

    def remote(src, dst, send_sem, recv_sem, device):
        return pltpu.make_async_remote_copy(
            src_ref=src, dst_ref=dst, send_sem=send_sem, recv_sem=recv_sem, device_id=(device,), device_id_type=MESH)

    def bulk(ref, send_sem, recv_sem):
        return remote(ref, ref, send_sem, recv_sem, me)

    def broadcast(buf, index, send_sem, recv_sem):
        for plane, gy, gx, gc in far_first():
            there = (3, 0, 2, 1)[plane]
            z = there * (2 - fz) + (3 - there) * (fz - 1)
            y = 1 - fy if gy else fy
            x = 1 - fx if gx else fx
            c = 1 - core if gc else core
            remote(buf.at[index], buf.at[index], send_sem, recv_sem, z * 8 + y * 4 + x * 2 + c).start()

    p_owner = central & (core == 1)

    @pl.loop(0, n_p)
    def _(b):
        owner = 2 * owner_chip(b) + 1

        @pl.when(me != owner)
        def _():
            remote(p_own.at[b], p_recv.at[lax.rem(me - owner + 2 * n - 1, n)], ps_sem, pr_sem, owner).start()

    @pl.loop(0, d_in // RB)
    def _(r):
        rows = pl.ds(pl.multiple_of(r * RB, RB), RB)
        at_v[rows, :] = a_v[:, rows].T

    def build(c):
        cols = pl.ds(pl.multiple_of(c * CB, CB), CB)
        gc = jnp.concatenate([g[2 * c + h] for h in range(CB // 128)], axis=1)
        for r in range(d_in // RB):
            rows = pl.ds(r * RB, RB)
            m = mm(at_v[rows, :], gc) * (1.0 / tokens) + m_ref[rows, cols]
            m_ref[rows, cols] = m
            for i, part in enumerate(split3(m)):
                for h in range(CB // 128):
                    parts[2 * c + h, pl.ds(i * d_in + r * RB, RB), :] = part[:, h * 128:(h + 1) * 128]

    pl.loop(0, nc // 2 + 1)(build)

    @pl.when(p_owner)
    def _():
        bulk(p_recv, ps_sem, pr_sem).wait_recv()
        p_all[mine] = p_own[mine] + jnp.sum(p_recv[...], axis=0)
        broadcast(p_all, mine, pbs_sem, pbr_sem)

    pl.loop(nc // 2 + 1, nc)(build)

    @pl.when(p_owner)
    def _():
        bulk(p_all.at[pl.ds(0, n_p - 1)], pbs_sem, pbr_sem).wait_recv()

    @pl.when(jnp.logical_not(p_owner))
    def _():
        bulk(p_all, pbs_sem, pbr_sem).wait_recv()

    p = orthonormalize(jnp.concatenate([p_all[b] for b in range(n_p)], axis=1))
    pt_ref[...] = p
    ps = stack3(p)

    def y_tile(t):
        def part(i):
            return jnp.concatenate(
                [parts[t * (cw // 128) + h, pl.ds(i * d_in, d_in), :] for h in range(cw // 128)], axis=1)
        y = mm(ps, part(2)) + mm(ps, part(1))
        return fold3(y + mm(ps, part(0)))

    mate = me + 1 - 2 * core

    @pl.loop(0, n_half // 2)
    def _(k):
        for i in range(2):
            s = 2 * k + i
            y_mate[s] = y_tile((1 - core) * n_half + s)
        for i in range(2):
            s = 2 * k + i
            remote(y_mate.at[s], y_mate.at[n_half + s], ms_sem, mr_sem.at[s], mate).start()

    @pl.loop(0, n_half // 2)
    def _(k):
        for i in range(2):
            s = 2 * k + i
            bulk(y_mate.at[n_half + s], ms_sem, mr_sem.at[s]).wait_recv()
        for i in range(2):
            s = 2 * k + i
            y_own[s] = y_tile(core * n_half + s) + y_mate[n_half + s]
        for i in range(2):
            s = 2 * k + i
            chip = owner_chip(s)
            slot = lax.rem(lax.div(me, 2) - chip + n - 1, n // 2)

            @pl.when(me != 2 * chip + core)
            def _():
                remote(y_own.at[s], y_recv.at[slot], ys_sem, yr_sem, 2 * chip + core).start()

    p1, p2, p3 = [x.astype(F32) for x in split3(p)]
    fill = jnp.zeros((128 - 9 * RANK, d_in), F32)
    pleft_ref[...] = jnp.concatenate([p1] * 3 + [p2] * 3 + [p3] * 3 + [fill], axis=0).T.astype(BF16)
    q_mine = core * n_half + mine

    @pl.when(central)
    def _():
        bulk(y_recv, ys_sem, yr_sem).wait_recv()
        q_ref[q_mine] = (y_own[mine] + jnp.sum(y_recv[...], axis=0)) * (1.0 / n)
        broadcast(q_ref, q_mine, ybs_sem, ybr_sem)

    bulk(y_mate.at[pl.ds(0, n_half)], ms_sem, yr_sem).wait_send()

    @pl.when(p_owner)
    def _():
        bulk(p_own.at[pl.ds(0, n_p - 1)], ps_sem, pr_sem).wait_send()
        bulk(p_recv, pbs_sem, pr_sem).wait_send()

    @pl.when(jnp.logical_not(p_owner))
    def _():
        bulk(p_own, ps_sem, pr_sem).wait_send()

    @pl.when(central)
    def _():
        bulk(y_own.at[pl.ds(0, n_half - 1)], ys_sem, yr_sem).wait_send()
        bulk(q_ref.at[pl.ds(0, 2 * n_half - 1)], ybs_sem, ybr_sem).wait_recv()
        bulk(parts.at[0, pl.ds(0, (n - 1) * RANK * cw // 64)], ybs_sem, yr_sem).wait_send()

    @pl.when(jnp.logical_not(central))
    def _():
        bulk(y_own, ys_sem, yr_sem).wait_send()
        bulk(q_ref, ybs_sem, ybr_sem).wait_recv()


def apply_kernel(pleft_ref, pt_ref, q_ref, m_ref, p_out, q_out, e_out, stage, p_sem, q_sem, e_sem):
    d_in, d_out = m_ref.shape
    n_y, _, cw = q_ref.shape
    p_copy = pltpu.make_async_copy(pt_ref, p_out, p_sem)
    fill = jnp.zeros((128 - 9 * RANK, cw), F32)

    def q_copy(c):
        cols = pl.ds(pl.multiple_of(c * cw, cw), cw)
        return pltpu.make_async_copy(q_ref.at[c], q_out.at[:, cols], q_sem)

    def e_copy(c):
        cols = pl.ds(pl.multiple_of(c * cw, cw), cw)
        return pltpu.make_async_copy(stage.at[:, cols], e_out.at[0, :, cols], e_sem)

    @pl.loop(0, n_y)
    def _(c):
        cols = pl.ds(pl.multiple_of(c * cw, cw), cw)
        three = [x.astype(F32) for x in split3(q_ref[c])]
        qc = jnp.concatenate(three * 3 + [fill], axis=0).astype(BF16)
        for r in range(d_in // RB):
            rows = pl.ds(r * RB, RB)
            stage[rows, cols] = m_ref[rows, cols] - mm(pleft_ref[rows, :], qc)
        e_copy(c).start()

    p_copy.start()

    @pl.loop(0, n_y)
    def _(c):
        q_copy(c).start()

    p_copy.wait()
    pltpu.make_async_copy(q_ref, q_ref, q_sem).wait()
    pltpu.make_async_copy(stage, e_out.at[0], e_sem).wait()


def solution(mesh):
    n = mesh.shape["data"]

    def per_device(act_in, pre_act, grad_out, q_init, err_mem):
        tokens, d_in = act_in.shape
        d_out = pre_act.shape[1]
        nc, n_p, n_y = d_out // CB, d_in // 128, n // 2
        cw = d_out // n_y
        hbm = pl.BlockSpec(memory_space=pltpu.HBM)
        vmem = pl.BlockSpec(memory_space=pltpu.VMEM)
        pleft, pt, q, m = pl.pallas_call(
            functools.partial(reduce_kernel, n),
            out_shape=(
                pltpu.VMEM((d_in, 128), BF16),
                pltpu.VMEM((RANK, d_in), F32),
                pltpu.VMEM((n_y, RANK, cw), F32),
                pltpu.VMEM((d_in, d_out), F32),
            ),
            in_specs=[hbm] * 5,
            out_specs=(vmem,) * 4,
            scratch_shapes=[
                pltpu.VMEM((d_out // 128, 3 * d_in, 128), BF16),
                pltpu.VMEM((d_out // 128, tokens, 128), BF16),
                pltpu.VMEM((tokens, d_out), BF16),
                pltpu.VMEM((tokens, d_out), BF16),
                pltpu.VMEM((tokens, d_in), BF16),
                pltpu.VMEM((d_in, tokens), BF16),
                pltpu.VMEM((RANK, d_out), F32),
                pltpu.VMEM((32, d_out), BF16),
                pltpu.VMEM((32, d_in), F32),
                pltpu.VMEM((32, tokens), F32),
                pltpu.VMEM((n_p, RANK, 128), F32),
                pltpu.VMEM((n - 1, RANK, 128), F32),
                pltpu.VMEM((n_p, RANK, 128), F32),
                pltpu.VMEM((n_y, RANK, cw), F32),
                pltpu.VMEM((n_y // 2, RANK, cw), F32),
                pltpu.VMEM((n // 2 - 1, RANK, cw), F32),
                pltpu.SemaphoreType.DMA((nc,)),
            ] + [pltpu.SemaphoreType.DMA] * 7 + [pltpu.SemaphoreType.DMA((n_y // 2,))]
            + [pltpu.SemaphoreType.DMA] * 4,
            compiler_params=pltpu.CompilerParams(
                collective_id=0, has_side_effects=True, vmem_limit_bytes=46 * 1024 * 1024),
            name="reduce_kernel",
        )(act_in, pre_act, grad_out, q_init.T, err_mem)
        p_t, q_t, err_new = pl.pallas_call(
            apply_kernel,
            out_shape=(
                jax.ShapeDtypeStruct((RANK, d_in), F32),
                jax.ShapeDtypeStruct((RANK, d_out), F32),
                jax.ShapeDtypeStruct((1, d_in, d_out), F32),
            ),
            in_specs=[vmem] * 4,
            out_specs=(hbm,) * 3,
            scratch_shapes=[
                pltpu.VMEM((d_in, d_out), F32),
            ] + [pltpu.SemaphoreType.DMA] * 3,
            compiler_params=pltpu.CompilerParams(vmem_limit_bytes=24 * 1024 * 1024),
            name="apply_kernel",
        )(pleft, pt, q, m)
        return p_t.T, q_t.T, err_new

    return jax.shard_map(
        per_device, mesh=mesh,
        in_specs=(P("data", None), P("data", None), P("data", None), P(None, None), P("data", None, None)),
        out_specs=(P(None, None), P(None, None), P("data", None, None)), check_vma=False)
```

```python
import functools

import jax
import jax.numpy as jnp
from jax import lax
from jax.experimental import pallas as pl
from jax.experimental.pallas import tpu as pltpu
from jax.sharding import PartitionSpec as P

F32 = jnp.float32
BF16 = jnp.bfloat16
MESH = pl.DeviceIdType.MESH
RANK = 8
CB = 256
RB = 256
NT = (((1,), (1,)), ((), ()))


def split3(x):
    hi = x.astype(BF16)
    rest = x - hi.astype(F32)
    mid = rest.astype(BF16)
    low = (rest - mid.astype(F32)).astype(BF16)
    return hi, mid, low


def stack3(x):
    parts = [p.astype(F32) for p in split3(x)]
    return jnp.concatenate(parts + [jnp.zeros_like(x)], axis=0).astype(BF16)


def fold3(y):
    return (y[16:24] + y[8:16]) + y[0:8]


def mm(a, b):
    return jnp.dot(a, b, preferred_element_type=F32)


def mm_nt(a, b):
    return lax.dot_general(a, b, NT, preferred_element_type=F32)


def gelu_grad(z, dy):
    c = 0.7978845608028654
    x = z.astype(F32)
    x2 = x * x
    t = jnp.tanh(x * (x2 * (c * 0.044715) + c))
    up = 1.0 + t
    slope = ((x * up) * (1.0 - t)) * (x2 * (1.5 * c * 0.044715) + 0.5 * c)
    return (0.5 * up + slope) * dy.astype(F32)


def orthonormalize(p):
    row = lax.broadcasted_iota(jnp.int32, (RANK, 1), 0)
    w = p
    norm2 = jnp.zeros((RANK, 1), F32)
    for j in range(RANK):
        v = w[j:j + 1]
        d = jnp.sum(jnp.where(row > j, p, w) * v, axis=1, keepdims=True)
        norm2 = jnp.where(row == j, d, norm2)
        if j + 1 < RANK:
            coef = jnp.where(row > j, d / d[j:j + 1], 0.0)
            w = w - coef * v
    return w / jnp.sqrt(norm2)


def reduce_kernel(n, a_hbm, z_hbm, dy_hbm, qt_hbm, e_hbm, pleft_ref, pt_ref, q_ref, m_ref,
                  parts, g, z_v, dy_v, a_v, at_v, qt_v, qs, p_acc, h_acc, p_own, p_recv, p_all,
                  y_mate, y_own, y_recv,
                  in_sem, q_sem, a_sem, ps_sem, pr_sem, pbs_sem, pbr_sem,
                  ms_sem, mr_sem, ys_sem, yr_sem, ybs_sem, ybr_sem):
    me = lax.axis_index("data")
    d_in, d_out = m_ref.shape
    tokens = z_v.shape[0]
    n_p = d_in // 128
    n_half = y_own.shape[0]
    cw = d_out // (2 * n_half)
    core = lax.rem(me, 2)
    fx = lax.rem(lax.div(me, 2), 2)
    fy = lax.rem(lax.div(me, 4), 2)
    fz = lax.div(me, 8)
    place = fx + 2 * fy
    p_owner = (fz >= 2) & (core == 1)
    p_mine = jnp.minimum(jnp.maximum(fz - 2, 0), 1) + 2 * place
    y_owner = fz <= 1
    y_mine = jnp.maximum(1 - fz, 0) + 2 * (3 - place)

    def p_chip(b):
        return 4 * (2 + lax.rem(b, 2)) + lax.div(b, 2)

    def y_chip(s):
        return 4 * (1 - lax.rem(s, 2)) + 3 - lax.div(s, 2)

    barrier = pltpu.get_barrier_semaphore()

    def e_copy(c):
        cols = pl.ds(pl.multiple_of(c * CB, CB), CB)
        return pltpu.make_async_copy(e_hbm.at[0, :, cols], m_ref.at[:, cols], in_sem.at[c])

    def z_copy(c):
        cols = pl.ds(pl.multiple_of(c * CB, CB), CB)
        return pltpu.make_async_copy(z_hbm.at[:, cols], z_v.at[:, cols], in_sem.at[c])

    def dy_copy(c):
        cols = pl.ds(pl.multiple_of(c * CB, CB), CB)
        return pltpu.make_async_copy(dy_hbm.at[:, cols], dy_v.at[:, cols], in_sem.at[c])

    nc = d_out // CB
    q_copy = pltpu.make_async_copy(qt_hbm, qt_v, q_sem)
    a_copy = pltpu.make_async_copy(a_hbm, a_v, a_sem)
    q_copy.start()

    @pl.loop(0, nc)
    def _(c):
        z_copy(c).start()
        dy_copy(c).start()
        e_copy(c).start()

        @pl.when(c == nc // 2)
        def _():
            a_copy.start()

    @pl.loop(1, n)
    def _(k):
        pl.semaphore_signal(barrier, inc=1, device_id=(lax.rem(me + k, n),), device_id_type=MESH)

    p_acc[...] = jnp.zeros_like(p_acc)
    h_acc[...] = jnp.zeros_like(h_acc)
    q_copy.wait()
    qt = qt_v[...]
    q_max = jnp.max(jnp.abs(qt), axis=1, keepdims=True)
    qs[...] = stack3((qt / q_max) * (1.0 / d_out))

    def arrive(c):
        whole = parts.at[pl.ds(2 * c, 2), pl.ds(0, 2 * (d_in + tokens))]
        pltpu.make_async_copy(whole, whole, in_sem.at[c]).wait()

    def stream(first, count):
        for i in range(count):
            arrive(first + i)
        for i in range(count):
            c = first + i
            cols = pl.ds(pl.multiple_of(c * CB, CB), CB)
            qc = qs[:, cols]
            for r in range(d_in // RB):
                rows = pl.ds(r * RB, RB)
                e1, e2, e3 = split3(m_ref[rows, cols])
                p_acc[:, rows] += (mm_nt(qc, e3) + mm_nt(qc, e2)) + mm_nt(qc, e1)
                if r % 2 == 1 and r // 2 < tokens // RB:
                    rows = pl.ds(r // 2 * RB, RB)
                    gb = gelu_grad(z_v[rows, cols], dy_v[rows, cols]).astype(BF16)
                    for h in range(CB // 128):
                        g[2 * c + h, rows, :] = gb[:, h * 128:(h + 1) * 128]
                    h_acc[:, rows] += mm_nt(qc, gb)

    stream(0, 1)

    @pl.loop(0, (nc - 2) // 2)
    def _(s):
        stream(1 + 2 * s, 2)

    stream(nc - 1, 1)

    a_copy.wait()
    hs = stack3(fold3(h_acc[...]))
    pt = (fold3(p_acc[...]) + fold3(mm(hs, a_v[...])) * (1.0 / tokens)) * q_max * float(d_out)
    for b in range(n_p):
        p_own[b] = pt[:, b * 128:(b + 1) * 128]

    pl.semaphore_wait(barrier, n - 1)

    def remote(src, dst, send_sem, recv_sem, device):
        return pltpu.make_async_remote_copy(
            src_ref=src, dst_ref=dst, send_sem=send_sem, recv_sem=recv_sem, device_id=(device,), device_id_type=MESH)

    def bulk(ref, send_sem, recv_sem):
        return remote(ref, ref, send_sem, recv_sem, me)

    def broadcast(buf, index, send_sem, recv_sem, planes):
        for z in planes:
            for low in range(8):
                there = 8 * z + low

                @pl.when(me != there)
                def _():
                    remote(buf.at[index], buf.at[index], send_sem, recv_sem, there).start()

    @pl.loop(0, n_p)
    def _(b):
        owner = 2 * p_chip(b) + 1

        @pl.when(me != owner)
        def _():
            remote(p_own.at[b], p_recv.at[lax.rem(me - owner + 2 * n - 1, n)], ps_sem, pr_sem, owner).start()

    @pl.loop(0, d_in // RB)
    def _(r):
        rows = pl.ds(pl.multiple_of(r * RB, RB), RB)
        at_v[rows, :] = a_v[:, rows].T

    def build(c):
        cols = pl.ds(pl.multiple_of(c * CB, CB), CB)
        gc = jnp.concatenate([g[2 * c + h] for h in range(CB // 128)], axis=1)
        for r in range(d_in // RB):
            rows = pl.ds(r * RB, RB)
            m = mm(at_v[rows, :], gc) * (1.0 / tokens) + m_ref[rows, cols]
            m_ref[rows, cols] = m
            for i, part in enumerate(split3(m)):
                for h in range(CB // 128):
                    parts[2 * c + h, pl.ds(i * d_in + r * RB, RB), :] = part[:, h * 128:(h + 1) * 128]

    early = jnp.minimum(2 + 3 * ((1 - fx) + (1 - fy) + (3 - fz)), nc)
    pl.loop(0, early)(build)

    @pl.when(p_owner)
    def _():
        bulk(p_recv, ps_sem, pr_sem).wait_recv()
        p_all[p_mine] = p_own[p_mine] + jnp.sum(p_recv[...], axis=0)
        broadcast(p_all, p_mine, pbs_sem, pbr_sem, (0, 3, 1, 2))

    pl.loop(early, nc)(build)

    @pl.when(p_owner)
    def _():
        bulk(p_all.at[pl.ds(0, n_p - 1)], pbs_sem, pbr_sem).wait_recv()

    @pl.when(jnp.logical_not(p_owner))
    def _():
        bulk(p_all, pbs_sem, pbr_sem).wait_recv()

    p = orthonormalize(jnp.concatenate([p_all[b] for b in range(n_p)], axis=1))
    pt_ref[...] = p
    ps = stack3(p)

    def y_tile(t):
        def part(i):
            return jnp.concatenate(
                [parts[t * (cw // 128) + h, pl.ds(i * d_in, d_in), :] for h in range(cw // 128)], axis=1)
        y = mm(ps, part(2)) + mm(ps, part(1))
        return fold3(y + mm(ps, part(0)))

    mate = me + 1 - 2 * core

    @pl.loop(0, n_half // 2)
    def _(k):
        for i in range(2):
            s = 2 * k + i
            y_mate[s] = y_tile((1 - core) * n_half + s)
        for i in range(2):
            s = 2 * k + i
            remote(y_mate.at[s], y_mate.at[n_half + s], ms_sem, mr_sem.at[s], mate).start()

    @pl.loop(0, n_half // 2)
    def _(k):
        for i in range(2):
            s = 2 * k + i
            bulk(y_mate.at[n_half + s], ms_sem, mr_sem.at[s]).wait_recv()
        for i in range(2):
            s = 2 * k + i
            y_own[s] = y_tile(core * n_half + s) + y_mate[n_half + s]
        for i in range(2):
            s = 2 * k + i
            chip = y_chip(s)
            slot = lax.rem(lax.div(me, 2) - chip + n - 1, n // 2)

            @pl.when(me != 2 * chip + core)
            def _():
                remote(y_own.at[s], y_recv.at[slot], ys_sem, yr_sem, 2 * chip + core).start()

    p1, p2, p3 = [x.astype(F32) for x in split3(p)]
    fill = jnp.zeros((128 - 9 * RANK, d_in), F32)
    pleft_ref[...] = jnp.concatenate([p1] * 3 + [p2] * 3 + [p3] * 3 + [fill], axis=0).T.astype(BF16)
    q_mine = core * n_half + y_mine

    @pl.when(y_owner)
    def _():
        bulk(y_recv, ys_sem, yr_sem).wait_recv()
        q_ref[q_mine] = (y_own[y_mine] + jnp.sum(y_recv[...], axis=0)) * (1.0 / n)
        broadcast(q_ref, q_mine, ybs_sem, ybr_sem, range(4))

    bulk(y_mate.at[pl.ds(0, n_half)], ms_sem, yr_sem).wait_send()

    @pl.when(p_owner)
    def _():
        bulk(p_own.at[pl.ds(0, n_p - 1)], ps_sem, pr_sem).wait_send()
        bulk(p_recv, pbs_sem, pr_sem).wait_send()

    @pl.when(jnp.logical_not(p_owner))
    def _():
        bulk(p_own, ps_sem, pr_sem).wait_send()

    @pl.when(y_owner)
    def _():
        bulk(y_own.at[pl.ds(0, n_half - 1)], ys_sem, yr_sem).wait_send()
        bulk(q_ref.at[pl.ds(0, 2 * n_half - 1)], ybs_sem, ybr_sem).wait_recv()
        bulk(parts.at[0, pl.ds(0, (n - 1) * RANK * cw // 64)], ybs_sem, yr_sem).wait_send()

    @pl.when(jnp.logical_not(y_owner))
    def _():
        bulk(y_own, ys_sem, yr_sem).wait_send()
        bulk(q_ref, ybs_sem, ybr_sem).wait_recv()


def apply_kernel(pleft_ref, pt_ref, q_ref, m_ref, p_out, q_out, e_out, stage, p_sem, q_sem, e_sem):
    d_in, d_out = m_ref.shape
    n_y, _, cw = q_ref.shape
    p_copy = pltpu.make_async_copy(pt_ref, p_out, p_sem)
    fill = jnp.zeros((128 - 9 * RANK, cw), F32)

    def q_copy(c):
        cols = pl.ds(pl.multiple_of(c * cw, cw), cw)
        return pltpu.make_async_copy(q_ref.at[c], q_out.at[:, cols], q_sem)

    def e_copy(c):
        cols = pl.ds(pl.multiple_of(c * cw, cw), cw)
        return pltpu.make_async_copy(stage.at[:, cols], e_out.at[0, :, cols], e_sem)

    @pl.loop(0, n_y)
    def _(c):
        cols = pl.ds(pl.multiple_of(c * cw, cw), cw)
        three = [x.astype(F32) for x in split3(q_ref[c])]
        qc = jnp.concatenate(three * 3 + [fill], axis=0).astype(BF16)
        for r in range(d_in // RB):
            rows = pl.ds(r * RB, RB)
            stage[rows, cols] = m_ref[rows, cols] - mm(pleft_ref[rows, :], qc)
        e_copy(c).start()

    p_copy.start()

    @pl.loop(0, n_y)
    def _(c):
        q_copy(c).start()

    p_copy.wait()
    pltpu.make_async_copy(q_ref, q_ref, q_sem).wait()
    pltpu.make_async_copy(stage, e_out.at[0], e_sem).wait()


def solution(mesh):
    n = mesh.shape["data"]

    def per_device(act_in, pre_act, grad_out, q_init, err_mem):
        tokens, d_in = act_in.shape
        d_out = pre_act.shape[1]
        nc, n_p, n_y = d_out // CB, d_in // 128, n // 2
        cw = d_out // n_y
        hbm = pl.BlockSpec(memory_space=pltpu.HBM)
        vmem = pl.BlockSpec(memory_space=pltpu.VMEM)
        pleft, pt, q, m = pl.pallas_call(
            functools.partial(reduce_kernel, n),
            out_shape=(
                pltpu.VMEM((d_in, 128), BF16),
                pltpu.VMEM((RANK, d_in), F32),
                pltpu.VMEM((n_y, RANK, cw), F32),
                pltpu.VMEM((d_in, d_out), F32),
            ),
            in_specs=[hbm] * 5,
            out_specs=(vmem,) * 4,
            scratch_shapes=[
                pltpu.VMEM((d_out // 128, 3 * d_in, 128), BF16),
                pltpu.VMEM((d_out // 128, tokens, 128), BF16),
                pltpu.VMEM((tokens, d_out), BF16),
                pltpu.VMEM((tokens, d_out), BF16),
                pltpu.VMEM((tokens, d_in), BF16),
                pltpu.VMEM((d_in, tokens), BF16),
                pltpu.VMEM((RANK, d_out), F32),
                pltpu.VMEM((32, d_out), BF16),
                pltpu.VMEM((32, d_in), F32),
                pltpu.VMEM((32, tokens), F32),
                pltpu.VMEM((n_p, RANK, 128), F32),
                pltpu.VMEM((n - 1, RANK, 128), F32),
                pltpu.VMEM((n_p, RANK, 128), F32),
                pltpu.VMEM((n_y, RANK, cw), F32),
                pltpu.VMEM((n_y // 2, RANK, cw), F32),
                pltpu.VMEM((n // 2 - 1, RANK, cw), F32),
                pltpu.SemaphoreType.DMA((nc,)),
            ] + [pltpu.SemaphoreType.DMA] * 7 + [pltpu.SemaphoreType.DMA((n_y // 2,))]
            + [pltpu.SemaphoreType.DMA] * 4,
            compiler_params=pltpu.CompilerParams(
                collective_id=0, has_side_effects=True, vmem_limit_bytes=46 * 1024 * 1024),
            name="reduce_kernel",
        )(act_in, pre_act, grad_out, q_init.T, err_mem)
        p_t, q_t, err_new = pl.pallas_call(
            apply_kernel,
            out_shape=(
                jax.ShapeDtypeStruct((RANK, d_in), F32),
                jax.ShapeDtypeStruct((RANK, d_out), F32),
                jax.ShapeDtypeStruct((1, d_in, d_out), F32),
            ),
            in_specs=[vmem] * 4,
            out_specs=(hbm,) * 3,
            scratch_shapes=[
                pltpu.VMEM((d_in, d_out), F32),
            ] + [pltpu.SemaphoreType.DMA] * 3,
            compiler_params=pltpu.CompilerParams(vmem_limit_bytes=24 * 1024 * 1024),
            name="apply_kernel",
        )(pleft, pt, q, m)
        return p_t.T, q_t.T, err_new

    return jax.shard_map(
        per_device, mesh=mesh,
        in_specs=(P("data", None), P("data", None), P("data", None), P(None, None), P("data", None, None)),
        out_specs=(P(None, None), P(None, None), P("data", None, None)), check_vma=False)
```

```python
import functools

import jax
import jax.numpy as jnp
from jax import lax
from jax.experimental import pallas as pl
from jax.experimental.pallas import tpu as pltpu
from jax.sharding import PartitionSpec as P

F32 = jnp.float32
BF16 = jnp.bfloat16
MESH = pl.DeviceIdType.MESH
RANK = 8
CB = 256
RB = 256
NT = (((1,), (1,)), ((), ()))


def split3(x):
    hi = x.astype(BF16)
    rest = x - hi.astype(F32)
    mid = rest.astype(BF16)
    low = (rest - mid.astype(F32)).astype(BF16)
    return hi, mid, low


def stack3(x):
    parts = [p.astype(F32) for p in split3(x)]
    return jnp.concatenate(parts + [jnp.zeros_like(x)], axis=0).astype(BF16)


def fold3(y):
    return (y[16:24] + y[8:16]) + y[0:8]


def mm(a, b):
    return jnp.dot(a, b, preferred_element_type=F32)


def mm_nt(a, b):
    return lax.dot_general(a, b, NT, preferred_element_type=F32)


def gelu_grad(z, dy):
    c = 0.7978845608028654
    x = z.astype(F32)
    x2 = x * x
    t = jnp.tanh(x * (x2 * (c * 0.044715) + c))
    up = 1.0 + t
    slope = ((x * up) * (1.0 - t)) * (x2 * (1.5 * c * 0.044715) + 0.5 * c)
    return (0.5 * up + slope) * dy.astype(F32)


def orthonormalize(p):
    row = lax.broadcasted_iota(jnp.int32, (RANK, 1), 0)
    w = p
    norm2 = jnp.zeros((RANK, 1), F32)
    for j in range(RANK):
        v = w[j:j + 1]
        d = jnp.sum(jnp.where(row > j, p, w) * v, axis=1, keepdims=True)
        norm2 = jnp.where(row == j, d, norm2)
        if j + 1 < RANK:
            coef = jnp.where(row > j, d / d[j:j + 1], 0.0)
            w = w - coef * v
    return w / jnp.sqrt(norm2)


def reduce_kernel(n, a_hbm, z_hbm, dy_hbm, qt_hbm, e_hbm, pleft_ref, pt_ref, q_ref, m_ref,
                  parts, g, z_v, dy_v, a_v, at_v, qt_v, qs, p_acc, h_acc, p_own, p_recv, p_all,
                  y_mate, y_own, y_recv,
                  in_sem, q_sem, a_sem, ps_sem, pr_sem, pbs_sem, pbr_sem,
                  ms_sem, mr_sem, ys_sem, yr_sem, ybs_sem, ybr_sem, qs_sem, qm_sem):
    me = lax.axis_index("data")
    d_in, d_out = m_ref.shape
    tokens = z_v.shape[0]
    n_p = d_in // 128
    n_half = y_own.shape[0]
    cw = d_out // (2 * n_half)
    core = lax.rem(me, 2)
    fx = lax.rem(lax.div(me, 2), 2)
    fy = lax.rem(lax.div(me, 4), 2)
    fz = lax.div(me, 8)
    place = fx + 2 * fy
    p_owner = (fz >= 2) & (core == 1)
    p_mine = jnp.minimum(jnp.maximum(fz - 2, 0), 1) + 2 * place
    y_owner = (fz >= 1) & (fz <= 2)
    y_mine = jnp.minimum(jnp.maximum(2 - fz, 0), 1) + 2 * (3 - place)

    def p_chip(b):
        return 4 * (2 + lax.rem(b, 2)) + lax.div(b, 2)

    def y_chip(s):
        return 4 * (2 - lax.rem(s, 2)) + 3 - lax.div(s, 2)

    barrier = pltpu.get_barrier_semaphore()

    def e_copy(c):
        cols = pl.ds(pl.multiple_of(c * CB, CB), CB)
        return pltpu.make_async_copy(e_hbm.at[0, :, cols], m_ref.at[:, cols], in_sem.at[c])

    def z_copy(c):
        cols = pl.ds(pl.multiple_of(c * CB, CB), CB)
        return pltpu.make_async_copy(z_hbm.at[:, cols], z_v.at[:, cols], in_sem.at[c])

    def dy_copy(c):
        cols = pl.ds(pl.multiple_of(c * CB, CB), CB)
        return pltpu.make_async_copy(dy_hbm.at[:, cols], dy_v.at[:, cols], in_sem.at[c])

    nc = d_out // CB
    q_copy = pltpu.make_async_copy(qt_hbm, qt_v, q_sem)
    a_copy = pltpu.make_async_copy(a_hbm, a_v, a_sem)
    q_copy.start()

    @pl.loop(0, nc)
    def _(c):
        z_copy(c).start()
        dy_copy(c).start()
        e_copy(c).start()

        @pl.when(c == nc // 2)
        def _():
            a_copy.start()

    @pl.loop(1, n)
    def _(k):
        pl.semaphore_signal(barrier, inc=1, device_id=(lax.rem(me + k, n),), device_id_type=MESH)

    p_acc[...] = jnp.zeros_like(p_acc)
    h_acc[...] = jnp.zeros_like(h_acc)
    q_copy.wait()
    qt = qt_v[...]
    q_max = jnp.max(jnp.abs(qt), axis=1, keepdims=True)
    qs[...] = stack3((qt / q_max) * (1.0 / d_out))

    def arrive(c):
        whole = parts.at[pl.ds(2 * c, 2), pl.ds(0, 2 * (d_in + tokens))]
        pltpu.make_async_copy(whole, whole, in_sem.at[c]).wait()

    def stream(first, count):
        for i in range(count):
            arrive(first + i)
        for i in range(count):
            c = first + i
            cols = pl.ds(pl.multiple_of(c * CB, CB), CB)
            qc = qs[:, cols]
            for r in range(d_in // RB):
                rows = pl.ds(r * RB, RB)
                e1, e2, e3 = split3(m_ref[rows, cols])
                p_acc[:, rows] += (mm_nt(qc, e3) + mm_nt(qc, e2)) + mm_nt(qc, e1)
                if r % 2 == 1 and r // 2 < tokens // RB:
                    rows = pl.ds(r // 2 * RB, RB)
                    gb = gelu_grad(z_v[rows, cols], dy_v[rows, cols]).astype(BF16)
                    for h in range(CB // 128):
                        g[2 * c + h, rows, :] = gb[:, h * 128:(h + 1) * 128]
                    h_acc[:, rows] += mm_nt(qc, gb)

    stream(0, 1)

    @pl.loop(0, (nc - 2) // 2)
    def _(s):
        stream(1 + 2 * s, 2)

    stream(nc - 1, 1)

    a_copy.wait()
    hs = stack3(fold3(h_acc[...]))
    pt = (fold3(p_acc[...]) + fold3(mm(hs, a_v[...])) * (1.0 / tokens)) * q_max * float(d_out)
    for b in range(n_p):
        p_own[b] = pt[:, b * 128:(b + 1) * 128]

    pl.semaphore_wait(barrier, n - 1)

    def remote(src, dst, send_sem, recv_sem, device):
        return pltpu.make_async_remote_copy(
            src_ref=src, dst_ref=dst, send_sem=send_sem, recv_sem=recv_sem, device_id=(device,), device_id_type=MESH)

    def bulk(ref, send_sem, recv_sem):
        return remote(ref, ref, send_sem, recv_sem, me)

    def broadcast(buf, index, send_sem, recv_sem, planes):
        for z in planes:
            for low in range(8):
                there = 8 * z + low

                @pl.when(me != there)
                def _():
                    remote(buf.at[index], buf.at[index], send_sem, recv_sem, there).start()

    @pl.loop(0, n_p)
    def _(b):
        owner = 2 * p_chip(b) + 1

        @pl.when(me != owner)
        def _():
            remote(p_own.at[b], p_recv.at[lax.rem(me - owner + 2 * n - 1, n)], ps_sem, pr_sem, owner).start()

    @pl.loop(0, d_in // RB)
    def _(r):
        rows = pl.ds(pl.multiple_of(r * RB, RB), RB)
        at_v[rows, :] = a_v[:, rows].T

    def build(c):
        cols = pl.ds(pl.multiple_of(c * CB, CB), CB)
        gc = jnp.concatenate([g[2 * c + h] for h in range(CB // 128)], axis=1)
        for r in range(d_in // RB):
            rows = pl.ds(r * RB, RB)
            m = mm(at_v[rows, :], gc) * (1.0 / tokens) + m_ref[rows, cols]
            m_ref[rows, cols] = m
            for i, part in enumerate(split3(m)):
                for h in range(CB // 128):
                    parts[2 * c + h, pl.ds(i * d_in + r * RB, RB), :] = part[:, h * 128:(h + 1) * 128]

    early = jnp.minimum(2 + 3 * ((1 - fx) + (1 - fy) + (3 - fz)), nc)
    pl.loop(0, early)(build)

    @pl.when(p_owner)
    def _():
        bulk(p_recv, ps_sem, pr_sem).wait_recv()
        p_all[p_mine] = p_own[p_mine] + jnp.sum(p_recv[...], axis=0)
        broadcast(p_all, p_mine, pbs_sem, pbr_sem, (0, 3, 1, 2))

    pl.loop(early, nc)(build)

    @pl.when(p_owner)
    def _():
        bulk(p_all.at[pl.ds(0, n_p - 1)], pbs_sem, pbr_sem).wait_recv()

    @pl.when(jnp.logical_not(p_owner))
    def _():
        bulk(p_all, pbs_sem, pbr_sem).wait_recv()

    p = orthonormalize(jnp.concatenate([p_all[b] for b in range(n_p)], axis=1))
    pt_ref[...] = p
    ps = stack3(p)

    def y_tile(t):
        def part(i):
            return jnp.concatenate(
                [parts[t * (cw // 128) + h, pl.ds(i * d_in, d_in), :] for h in range(cw // 128)], axis=1)
        y = mm(ps, part(2)) + mm(ps, part(1))
        return fold3(y + mm(ps, part(0)))

    mate = me + 1 - 2 * core

    @pl.loop(0, n_half // 2)
    def _(k):
        for i in range(2):
            s = 2 * k + i
            y_mate[s] = y_tile((1 - core) * n_half + s)
        for i in range(2):
            s = 2 * k + i
            remote(y_mate.at[s], y_mate.at[n_half + s], ms_sem, mr_sem.at[s], mate).start()

    @pl.loop(0, n_half // 2)
    def _(k):
        for i in range(2):
            s = 2 * k + i
            bulk(y_mate.at[n_half + s], ms_sem, mr_sem.at[s]).wait_recv()
        for i in range(2):
            s = 2 * k + i
            y_own[s] = y_tile(core * n_half + s) + y_mate[n_half + s]
        for i in range(2):
            s = 2 * k + i
            chip = y_chip(s)
            slot = lax.rem(lax.div(me, 2) - chip + n - 1, n // 2)

            @pl.when(me != 2 * chip + core)
            def _():
                remote(y_own.at[s], y_recv.at[slot], ys_sem, yr_sem, 2 * chip + core).start()

    p1, p2, p3 = [x.astype(F32) for x in split3(p)]
    fill = jnp.zeros((128 - 9 * RANK, d_in), F32)
    pleft_ref[...] = jnp.concatenate([p1] * 3 + [p2] * 3 + [p3] * 3 + [fill], axis=0).T.astype(BF16)
    q_mine = core * n_half + y_mine

    @pl.when(y_owner)
    def _():
        bulk(y_recv, ys_sem, yr_sem).wait_recv()
        q_ref[q_mine] = (y_own[y_mine] + jnp.sum(y_recv[...], axis=0)) * (1.0 / n)
        tile = q_ref.at[q_mine]
        for chip in range(n // 2):
            @pl.when(lax.div(me, 2) != chip)
            def _():
                remote(tile, tile, ybs_sem, ybr_sem.at[y_mine], 2 * chip + core).start()
        remote(tile, tile, ybs_sem, qm_sem, mate).start()

    for s in range(n_half):
        @pl.when(lax.div(me, 2) != y_chip(s))
        def _():
            tile = q_ref.at[core * n_half + s]
            bulk(tile, ybs_sem, ybr_sem.at[s]).wait_recv()
            remote(tile, tile, qs_sem, qm_sem, mate).start()

    bulk(q_ref.at[pl.ds(0, n_half)], qs_sem, qm_sem).wait_recv()
    bulk(y_mate.at[pl.ds(0, n_half)], ms_sem, yr_sem).wait_send()

    @pl.when(p_owner)
    def _():
        bulk(p_own.at[pl.ds(0, n_p - 1)], ps_sem, pr_sem).wait_send()
        bulk(p_recv, pbs_sem, pr_sem).wait_send()

    @pl.when(jnp.logical_not(p_owner))
    def _():
        bulk(p_own, ps_sem, pr_sem).wait_send()

    @pl.when(y_owner)
    def _():
        bulk(y_own.at[pl.ds(0, n_half - 1)], ys_sem, yr_sem).wait_send()
        bulk(q_ref, ybs_sem, qm_sem).wait_send()
        bulk(q_ref.at[pl.ds(0, n_half - 1)], qs_sem, qm_sem).wait_send()

    @pl.when(jnp.logical_not(y_owner))
    def _():
        bulk(y_own, ys_sem, yr_sem).wait_send()
        bulk(q_ref.at[pl.ds(0, n_half)], qs_sem, qm_sem).wait_send()


def apply_kernel(pleft_ref, pt_ref, q_ref, m_ref, p_out, q_out, e_out, stage, p_sem, q_sem, e_sem):
    d_in, d_out = m_ref.shape
    n_y, _, cw = q_ref.shape
    p_copy = pltpu.make_async_copy(pt_ref, p_out, p_sem)
    fill = jnp.zeros((128 - 9 * RANK, cw), F32)

    def q_copy(c):
        cols = pl.ds(pl.multiple_of(c * cw, cw), cw)
        return pltpu.make_async_copy(q_ref.at[c], q_out.at[:, cols], q_sem)

    def e_copy(c):
        cols = pl.ds(pl.multiple_of(c * cw, cw), cw)
        return pltpu.make_async_copy(stage.at[:, cols], e_out.at[0, :, cols], e_sem)

    @pl.loop(0, n_y)
    def _(c):
        cols = pl.ds(pl.multiple_of(c * cw, cw), cw)
        three = [x.astype(F32) for x in split3(q_ref[c])]
        qc = jnp.concatenate(three * 3 + [fill], axis=0).astype(BF16)
        for r in range(d_in // RB):
            rows = pl.ds(r * RB, RB)
            stage[rows, cols] = m_ref[rows, cols] - mm(pleft_ref[rows, :], qc)
        e_copy(c).start()

    p_copy.start()

    @pl.loop(0, n_y)
    def _(c):
        q_copy(c).start()

    p_copy.wait()
    pltpu.make_async_copy(q_ref, q_ref, q_sem).wait()
    pltpu.make_async_copy(stage, e_out.at[0], e_sem).wait()


def solution(mesh):
    n = mesh.shape["data"]

    def per_device(act_in, pre_act, grad_out, q_init, err_mem):
        tokens, d_in = act_in.shape
        d_out = pre_act.shape[1]
        nc, n_p, n_y = d_out // CB, d_in // 128, n // 2
        cw = d_out // n_y
        hbm = pl.BlockSpec(memory_space=pltpu.HBM)
        vmem = pl.BlockSpec(memory_space=pltpu.VMEM)
        pleft, pt, q, m = pl.pallas_call(
            functools.partial(reduce_kernel, n),
            out_shape=(
                pltpu.VMEM((d_in, 128), BF16),
                pltpu.VMEM((RANK, d_in), F32),
                pltpu.VMEM((n_y, RANK, cw), F32),
                pltpu.VMEM((d_in, d_out), F32),
            ),
            in_specs=[hbm] * 5,
            out_specs=(vmem,) * 4,
            scratch_shapes=[
                pltpu.VMEM((d_out // 128, 3 * d_in, 128), BF16),
                pltpu.VMEM((d_out // 128, tokens, 128), BF16),
                pltpu.VMEM((tokens, d_out), BF16),
                pltpu.VMEM((tokens, d_out), BF16),
                pltpu.VMEM((tokens, d_in), BF16),
                pltpu.VMEM((d_in, tokens), BF16),
                pltpu.VMEM((RANK, d_out), F32),
                pltpu.VMEM((32, d_out), BF16),
                pltpu.VMEM((32, d_in), F32),
                pltpu.VMEM((32, tokens), F32),
                pltpu.VMEM((n_p, RANK, 128), F32),
                pltpu.VMEM((n - 1, RANK, 128), F32),
                pltpu.VMEM((n_p, RANK, 128), F32),
                pltpu.VMEM((n_y, RANK, cw), F32),
                pltpu.VMEM((n_y // 2, RANK, cw), F32),
                pltpu.VMEM((n // 2 - 1, RANK, cw), F32),
                pltpu.SemaphoreType.DMA((nc,)),
            ] + [pltpu.SemaphoreType.DMA] * 7 + [pltpu.SemaphoreType.DMA((n_y // 2,))]
            + [pltpu.SemaphoreType.DMA] * 3 + [pltpu.SemaphoreType.DMA((n_y // 2,))] + [pltpu.SemaphoreType.DMA] * 2,
            compiler_params=pltpu.CompilerParams(
                collective_id=0, has_side_effects=True, vmem_limit_bytes=46 * 1024 * 1024),
            name="reduce_kernel",
        )(act_in, pre_act, grad_out, q_init.T, err_mem)
        p_t, q_t, err_new = pl.pallas_call(
            apply_kernel,
            out_shape=(
                jax.ShapeDtypeStruct((RANK, d_in), F32),
                jax.ShapeDtypeStruct((RANK, d_out), F32),
                jax.ShapeDtypeStruct((1, d_in, d_out), F32),
            ),
            in_specs=[vmem] * 4,
            out_specs=(hbm,) * 3,
            scratch_shapes=[
                pltpu.VMEM((d_in, d_out), F32),
            ] + [pltpu.SemaphoreType.DMA] * 3,
            compiler_params=pltpu.CompilerParams(vmem_limit_bytes=24 * 1024 * 1024),
            name="apply_kernel",
        )(pleft, pt, q, m)
        return p_t.T, q_t.T, err_new

    return jax.shard_map(
        per_device, mesh=mesh,
        in_specs=(P("data", None), P("data", None), P("data", None), P(None, None), P("data", None, None)),
        out_specs=(P(None, None), P(None, None), P("data", None, None)), check_vma=False)
```

```python
import functools

import jax
import jax.numpy as jnp
from jax import lax
from jax.experimental import pallas as pl
from jax.experimental.pallas import tpu as pltpu
from jax.sharding import PartitionSpec as P

F32 = jnp.float32
BF16 = jnp.bfloat16
MESH = pl.DeviceIdType.MESH
RANK = 8
CB = 256
RB = 256
NT = (((1,), (1,)), ((), ()))


def split3(x):
    hi = x.astype(BF16)
    rest = x - hi.astype(F32)
    mid = rest.astype(BF16)
    low = (rest - mid.astype(F32)).astype(BF16)
    return hi, mid, low


def stack3(x):
    parts = [p.astype(F32) for p in split3(x)]
    return jnp.concatenate(parts + [jnp.zeros_like(x)], axis=0).astype(BF16)


def fold3(y):
    return (y[16:24] + y[8:16]) + y[0:8]


def mm(a, b):
    return jnp.dot(a, b, preferred_element_type=F32)


def mm_nt(a, b):
    return lax.dot_general(a, b, NT, preferred_element_type=F32)


def gelu_grad(z, dy):
    c = 0.7978845608028654
    x = z.astype(F32)
    x2 = x * x
    t = jnp.tanh(x * (x2 * (c * 0.044715) + c))
    up = 1.0 + t
    slope = ((x * up) * (1.0 - t)) * (x2 * (1.5 * c * 0.044715) + 0.5 * c)
    return (0.5 * up + slope) * dy.astype(F32)


def orthonormalize(p):
    row = lax.broadcasted_iota(jnp.int32, (RANK, 1), 0)
    w = p
    norm2 = jnp.zeros((RANK, 1), F32)
    for j in range(RANK):
        v = w[j:j + 1]
        d = jnp.sum(jnp.where(row > j, p, w) * v, axis=1, keepdims=True)
        norm2 = jnp.where(row == j, d, norm2)
        if j + 1 < RANK:
            coef = jnp.where(row > j, d / d[j:j + 1], 0.0)
            w = w - coef * v
    return w / jnp.sqrt(norm2)


def far_first(near_planes, cores):
    places = [(i, fy, fx, fc) for i in range(4) for fy in range(2) for fx in range(2) for fc in range(cores)]
    places.remove((3, 0, 0, 0))
    return sorted(places, key=lambda p: -(near_planes[p[0]] + p[1] + p[2]))


def flip(bit, by):
    return bit + by - 2 * bit * by


def reduce_kernel(n, a_hbm, z_hbm, dy_hbm, qt_hbm, e_hbm, pleft_ref, pt_ref, q_ref, m_ref,
                  parts, g, z_v, dy_v, a_v, at_v, qt_v, qs, p_acc, h_acc, p_own, p_recv, p_all,
                  y_mate, y_own, y_recv,
                  in_sem, q_sem, a_sem, ps_sem, pr_sem, pbs_sem, pbr_sem,
                  ms_sem, mr_sem, ys_sem, yr_sem, ybs_sem, ybr_sem, qs_sem, qm_sem):
    me = lax.axis_index("data")
    d_in, d_out = m_ref.shape
    tokens = z_v.shape[0]
    n_p = d_in // 128
    n_half = y_own.shape[0]
    cw = d_out // (2 * n_half)
    core = lax.rem(me, 2)
    fx = lax.rem(lax.div(me, 2), 2)
    fy = lax.rem(lax.div(me, 4), 2)
    fz = lax.div(me, 8)
    place = fx + 2 * fy
    p_owner = (fz >= 2) & (core == 1)
    p_mine = jnp.minimum(jnp.maximum(fz - 2, 0), 1) + 2 * place
    y_owner = (fz >= 1) & (fz <= 2)
    y_mine = jnp.minimum(jnp.maximum(fz - 1, 0), 1) + 2 * place

    barrier = pltpu.get_barrier_semaphore()

    def e_copy(c):
        cols = pl.ds(pl.multiple_of(c * CB, CB), CB)
        return pltpu.make_async_copy(e_hbm.at[0, :, cols], m_ref.at[:, cols], in_sem.at[c])

    def z_copy(c):
        cols = pl.ds(pl.multiple_of(c * CB, CB), CB)
        return pltpu.make_async_copy(z_hbm.at[:, cols], z_v.at[:, cols], in_sem.at[c])

    def dy_copy(c):
        cols = pl.ds(pl.multiple_of(c * CB, CB), CB)
        return pltpu.make_async_copy(dy_hbm.at[:, cols], dy_v.at[:, cols], in_sem.at[c])

    nc = d_out // CB
    q_copy = pltpu.make_async_copy(qt_hbm, qt_v, q_sem)
    a_copy = pltpu.make_async_copy(a_hbm, a_v, a_sem)
    q_copy.start()

    @pl.loop(0, nc)
    def _(c):
        z_copy(c).start()
        dy_copy(c).start()
        e_copy(c).start()

        @pl.when(c == nc // 2)
        def _():
            a_copy.start()

    @pl.loop(1, n)
    def _(k):
        pl.semaphore_signal(barrier, inc=1, device_id=(lax.rem(me + k, n),), device_id_type=MESH)

    p_acc[...] = jnp.zeros_like(p_acc)
    h_acc[...] = jnp.zeros_like(h_acc)
    q_copy.wait()
    qt = qt_v[...]
    q_max = jnp.max(jnp.abs(qt), axis=1, keepdims=True)
    qs[...] = stack3((qt / q_max) * (1.0 / d_out))

    def arrive(c):
        whole = parts.at[pl.ds(2 * c, 2), pl.ds(0, 2 * (d_in + tokens))]
        pltpu.make_async_copy(whole, whole, in_sem.at[c]).wait()

    def stream(first, count):
        for i in range(count):
            arrive(first + i)
        for i in range(count):
            c = first + i
            cols = pl.ds(pl.multiple_of(c * CB, CB), CB)
            qc = qs[:, cols]
            for r in range(d_in // RB):
                rows = pl.ds(r * RB, RB)
                e1, e2, e3 = split3(m_ref[rows, cols])
                p_acc[:, rows] += (mm_nt(qc, e3) + mm_nt(qc, e2)) + mm_nt(qc, e1)
                if r % 2 == 1 and r // 2 < tokens // RB:
                    rows = pl.ds(r // 2 * RB, RB)
                    gb = gelu_grad(z_v[rows, cols], dy_v[rows, cols]).astype(BF16)
                    for h in range(CB // 128):
                        g[2 * c + h, rows, :] = gb[:, h * 128:(h + 1) * 128]
                    h_acc[:, rows] += mm_nt(qc, gb)

    stream(0, 1)

    @pl.loop(0, (nc - 2) // 2)
    def _(s):
        stream(1 + 2 * s, 2)

    stream(nc - 1, 1)

    a_copy.wait()
    hs = stack3(fold3(h_acc[...]))
    pt = (fold3(p_acc[...]) + fold3(mm(hs, a_v[...])) * (1.0 / tokens)) * q_max * float(d_out)
    for b in range(n_p):
        p_own[b] = pt[:, b * 128:(b + 1) * 128]

    pl.semaphore_wait(barrier, n - 1)

    def remote(src, dst, send_sem, recv_sem, device):
        return pltpu.make_async_remote_copy(
            src_ref=src, dst_ref=dst, send_sem=send_sem, recv_sem=recv_sem, device_id=(device,), device_id_type=MESH)

    def bulk(ref, send_sem, recv_sem):
        return remote(ref, ref, send_sem, recv_sem, me)

    def chip_at(z, gy, gx):
        return 4 * z + 2 * flip(fy, gy) + flip(fx, gx)

    @pl.loop(0, n_p)
    def _(k):
        gy, gx = 1 - lax.div(k, 4), 1 - lax.rem(lax.div(k, 2), 2)
        half = lax.rem(k + fz, 2)
        owner = 2 * chip_at(2 + half, gy, gx) + 1
        b = half + 2 * (flip(fx, gx) + 2 * flip(fy, gy))

        @pl.when(me != owner)
        def _():
            remote(p_own.at[b], p_recv.at[lax.rem(me - owner + 2 * n - 1, n)], ps_sem, pr_sem, owner).start()

    @pl.loop(0, d_in // RB)
    def _(r):
        rows = pl.ds(pl.multiple_of(r * RB, RB), RB)
        at_v[rows, :] = a_v[:, rows].T

    def build(c):
        cols = pl.ds(pl.multiple_of(c * CB, CB), CB)
        gc = jnp.concatenate([g[2 * c + h] for h in range(CB // 128)], axis=1)
        for r in range(d_in // RB):
            rows = pl.ds(r * RB, RB)
            m = mm(at_v[rows, :], gc) * (1.0 / tokens) + m_ref[rows, cols]
            m_ref[rows, cols] = m
            for i, part in enumerate(split3(m)):
                for h in range(CB // 128):
                    parts[2 * c + h, pl.ds(i * d_in + r * RB, RB), :] = part[:, h * 128:(h + 1) * 128]

    early = jnp.minimum(2 + 3 * ((1 - fx) + (1 - fy) + (3 - fz)), nc)
    pl.loop(0, early)(build)

    @pl.when(p_owner)
    def _():
        bulk(p_recv, ps_sem, pr_sem).wait_recv()
        p_all[p_mine] = p_own[p_mine] + jnp.sum(p_recv[...], axis=0)
        tile = p_all.at[p_mine]
        for plane, gy, gx, gc in far_first((2.5, 1.5, 1, 0), 2):
            z = (0, 3, 1, 2)[plane] * (3 - fz) + plane * (fz - 2)
            remote(tile, tile, pbs_sem, pbr_sem, 2 * chip_at(z, gy, gx) + (1 - gc)).start()

    pl.loop(early, nc)(build)

    @pl.when(p_owner)
    def _():
        bulk(p_all.at[pl.ds(0, n_p - 1)], pbs_sem, pbr_sem).wait_recv()

    @pl.when(jnp.logical_not(p_owner))
    def _():
        bulk(p_all, pbs_sem, pbr_sem).wait_recv()

    p = orthonormalize(jnp.concatenate([p_all[b] for b in range(n_p)], axis=1))
    pt_ref[...] = p
    ps = stack3(p)

    def y_tile(t):
        def part(i):
            return jnp.concatenate(
                [parts[t * (cw // 128) + h, pl.ds(i * d_in, d_in), :] for h in range(cw // 128)], axis=1)
        y = mm(ps, part(2)) + mm(ps, part(1))
        return fold3(y + mm(ps, part(0)))

    mate = me + 1 - 2 * core

    def pair(k):
        gy, gx = 1 - lax.div(k, 2), 1 - lax.rem(k, 2)
        column = 2 * (flip(fx, gx) + 2 * flip(fy, gy))
        return [(lax.rem(fz + i, 2) + column, chip_at(1 + lax.rem(fz + i, 2), gy, gx)) for i in range(2)]

    @pl.loop(0, n_half // 2)
    def _(k):
        for s, _ in pair(k):
            y_mate[s] = y_tile((1 - core) * n_half + s)
        for s, _ in pair(k):
            remote(y_mate.at[s], y_mate.at[n_half + s], ms_sem, mr_sem.at[s], mate).start()

    @pl.loop(0, n_half // 2)
    def _(k):
        for s, _ in pair(k):
            bulk(y_mate.at[n_half + s], ms_sem, mr_sem.at[s]).wait_recv()
        for s, _ in pair(k):
            y_own[s] = y_tile(core * n_half + s) + y_mate[n_half + s]
        for s, chip in pair(k):
            slot = lax.rem(lax.div(me, 2) - chip + n - 1, n // 2)

            @pl.when(me != 2 * chip + core)
            def _():
                remote(y_own.at[s], y_recv.at[slot], ys_sem, yr_sem, 2 * chip + core).start()

    p1, p2, p3 = [x.astype(F32) for x in split3(p)]
    fill = jnp.zeros((128 - 9 * RANK, d_in), F32)
    pleft_ref[...] = jnp.concatenate([p1] * 3 + [p2] * 3 + [p3] * 3 + [fill], axis=0).T.astype(BF16)
    q_mine = core * n_half + y_mine

    @pl.when(y_owner)
    def _():
        bulk(y_recv, ys_sem, yr_sem).wait_recv()
        q_ref[q_mine] = (y_own[y_mine] + jnp.sum(y_recv[...], axis=0)) * (1.0 / n)
        tile = q_ref.at[q_mine]
        for plane, gy, gx, _ in far_first((2, 1, 1, 0), 1):
            there = (3, 0, 2, 1)[plane]
            z = there * (2 - fz) + (3 - there) * (fz - 1)
            remote(tile, tile, ybs_sem, ybr_sem.at[y_mine], 2 * chip_at(z, gy, gx) + core).start()
        remote(tile, tile, ybs_sem, qm_sem, mate).start()

    for s in range(n_half):
        @pl.when(jnp.logical_not(y_owner) | (y_mine != s))
        def _():
            tile = q_ref.at[core * n_half + s]
            bulk(tile, ybs_sem, ybr_sem.at[s]).wait_recv()
            remote(tile, tile, qs_sem, qm_sem, mate).start()

    bulk(q_ref.at[pl.ds(0, n_half)], qs_sem, qm_sem).wait_recv()
    bulk(y_mate.at[pl.ds(0, n_half)], ms_sem, yr_sem).wait_send()

    @pl.when(p_owner)
    def _():
        bulk(p_own.at[pl.ds(0, n_p - 1)], ps_sem, pr_sem).wait_send()
        bulk(p_recv, pbs_sem, pr_sem).wait_send()

    @pl.when(jnp.logical_not(p_owner))
    def _():
        bulk(p_own, ps_sem, pr_sem).wait_send()

    @pl.when(y_owner)
    def _():
        bulk(y_own.at[pl.ds(0, n_half - 1)], ys_sem, yr_sem).wait_send()
        bulk(q_ref, ybs_sem, qm_sem).wait_send()
        bulk(q_ref.at[pl.ds(0, n_half - 1)], qs_sem, qm_sem).wait_send()

    @pl.when(jnp.logical_not(y_owner))
    def _():
        bulk(y_own, ys_sem, yr_sem).wait_send()
        bulk(q_ref.at[pl.ds(0, n_half)], qs_sem, qm_sem).wait_send()


def apply_kernel(pleft_ref, pt_ref, q_ref, m_ref, p_out, q_out, e_out, stage, p_sem, q_sem, e_sem):
    d_in, d_out = m_ref.shape
    n_y, _, cw = q_ref.shape
    p_copy = pltpu.make_async_copy(pt_ref, p_out, p_sem)
    fill = jnp.zeros((128 - 9 * RANK, cw), F32)

    def q_copy(c):
        cols = pl.ds(pl.multiple_of(c * cw, cw), cw)
        return pltpu.make_async_copy(q_ref.at[c], q_out.at[:, cols], q_sem)

    def e_copy(c):
        cols = pl.ds(pl.multiple_of(c * cw, cw), cw)
        return pltpu.make_async_copy(stage.at[:, cols], e_out.at[0, :, cols], e_sem)

    @pl.loop(0, n_y)
    def _(c):
        cols = pl.ds(pl.multiple_of(c * cw, cw), cw)
        three = [x.astype(F32) for x in split3(q_ref[c])]
        qc = jnp.concatenate(three * 3 + [fill], axis=0).astype(BF16)
        for r in range(d_in // RB):
            rows = pl.ds(r * RB, RB)
            stage[rows, cols] = m_ref[rows, cols] - mm(pleft_ref[rows, :], qc)
        e_copy(c).start()

    p_copy.start()

    @pl.loop(0, n_y)
    def _(c):
        q_copy(c).start()

    p_copy.wait()
    pltpu.make_async_copy(q_ref, q_ref, q_sem).wait()
    pltpu.make_async_copy(stage, e_out.at[0], e_sem).wait()


def solution(mesh):
    n = mesh.shape["data"]

    def per_device(act_in, pre_act, grad_out, q_init, err_mem):
        tokens, d_in = act_in.shape
        d_out = pre_act.shape[1]
        nc, n_p, n_y = d_out // CB, d_in // 128, n // 2
        cw = d_out // n_y
        hbm = pl.BlockSpec(memory_space=pltpu.HBM)
        vmem = pl.BlockSpec(memory_space=pltpu.VMEM)
        pleft, pt, q, m = pl.pallas_call(
            functools.partial(reduce_kernel, n),
            out_shape=(
                pltpu.VMEM((d_in, 128), BF16),
                pltpu.VMEM((RANK, d_in), F32),
                pltpu.VMEM((n_y, RANK, cw), F32),
                pltpu.VMEM((d_in, d_out), F32),
            ),
            in_specs=[hbm] * 5,
            out_specs=(vmem,) * 4,
            scratch_shapes=[
                pltpu.VMEM((d_out // 128, 3 * d_in, 128), BF16),
                pltpu.VMEM((d_out // 128, tokens, 128), BF16),
                pltpu.VMEM((tokens, d_out), BF16),
                pltpu.VMEM((tokens, d_out), BF16),
                pltpu.VMEM((tokens, d_in), BF16),
                pltpu.VMEM((d_in, tokens), BF16),
                pltpu.VMEM((RANK, d_out), F32),
                pltpu.VMEM((32, d_out), BF16),
                pltpu.VMEM((32, d_in), F32),
                pltpu.VMEM((32, tokens), F32),
                pltpu.VMEM((n_p, RANK, 128), F32),
                pltpu.VMEM((n - 1, RANK, 128), F32),
                pltpu.VMEM((n_p, RANK, 128), F32),
                pltpu.VMEM((n_y, RANK, cw), F32),
                pltpu.VMEM((n_y // 2, RANK, cw), F32),
                pltpu.VMEM((n // 2 - 1, RANK, cw), F32),
                pltpu.SemaphoreType.DMA((nc,)),
            ] + [pltpu.SemaphoreType.DMA] * 7 + [pltpu.SemaphoreType.DMA((n_y // 2,))]
            + [pltpu.SemaphoreType.DMA] * 3 + [pltpu.SemaphoreType.DMA((n_y // 2,))] + [pltpu.SemaphoreType.DMA] * 2,
            compiler_params=pltpu.CompilerParams(
                collective_id=0, has_side_effects=True, vmem_limit_bytes=46 * 1024 * 1024),
            name="reduce_kernel",
        )(act_in, pre_act, grad_out, q_init.T, err_mem)
        p_t, q_t, err_new = pl.pallas_call(
            apply_kernel,
            out_shape=(
                jax.ShapeDtypeStruct((RANK, d_in), F32),
                jax.ShapeDtypeStruct((RANK, d_out), F32),
                jax.ShapeDtypeStruct((1, d_in, d_out), F32),
            ),
            in_specs=[vmem] * 4,
            out_specs=(hbm,) * 3,
            scratch_shapes=[
                pltpu.VMEM((d_in, d_out), F32),
            ] + [pltpu.SemaphoreType.DMA] * 3,
            compiler_params=pltpu.CompilerParams(vmem_limit_bytes=24 * 1024 * 1024),
            name="apply_kernel",
        )(pleft, pt, q, m)
        return p_t.T, q_t.T, err_new

    return jax.shard_map(
        per_device, mesh=mesh,
        in_specs=(P("data", None), P("data", None), P("data", None), P(None, None), P("data", None, None)),
        out_specs=(P(None, None), P(None, None), P("data", None, None)), check_vma=False)
```

```python
import functools

import jax
import jax.numpy as jnp
from jax import lax
from jax.experimental import pallas as pl
from jax.experimental.pallas import tpu as pltpu
from jax.sharding import PartitionSpec as P

F32 = jnp.float32
BF16 = jnp.bfloat16
MESH = pl.DeviceIdType.MESH
RANK = 8
CB = 256
AHEAD = 4
RB = 256
NT = (((1,), (1,)), ((), ()))


def split3(x):
    hi = x.astype(BF16)
    rest = x - hi.astype(F32)
    mid = rest.astype(BF16)
    low = (rest - mid.astype(F32)).astype(BF16)
    return hi, mid, low


def stack3(x):
    parts = [p.astype(F32) for p in split3(x)]
    return jnp.concatenate(parts + [jnp.zeros_like(x)], axis=0).astype(BF16)


def fold3(y):
    return (y[16:24] + y[8:16]) + y[0:8]


def mm(a, b):
    return jnp.dot(a, b, preferred_element_type=F32)


def mm_nt(a, b):
    return lax.dot_general(a, b, NT, preferred_element_type=F32)


def gelu_grad(z, dy):
    c = 0.7978845608028654
    x = z.astype(F32)
    x2 = x * x
    t = jnp.tanh(x * (x2 * (c * 0.044715) + c))
    up = 1.0 + t
    slope = ((x * up) * (1.0 - t)) * (x2 * (1.5 * c * 0.044715) + 0.5 * c)
    return (0.5 * up + slope) * dy.astype(F32)


def orthonormalize(p):
    row = lax.broadcasted_iota(jnp.int32, (RANK, 1), 0)
    w = p
    norm2 = jnp.zeros((RANK, 1), F32)
    for j in range(RANK):
        v = w[j:j + 1]
        d = jnp.sum(jnp.where(row > j, p, w) * v, axis=1, keepdims=True)
        norm2 = jnp.where(row == j, d, norm2)
        if j + 1 < RANK:
            coef = jnp.where(row > j, d / d[j:j + 1], 0.0)
            w = w - coef * v
    return w / jnp.sqrt(norm2)


def far_first(near_planes, cores):
    places = [(i, fy, fx, fc) for i in range(4) for fy in range(2) for fx in range(2) for fc in range(cores)]
    places.remove((3, 0, 0, 0))
    return sorted(places, key=lambda p: -(near_planes[p[0]] + p[1] + p[2]))


def flip(bit, by):
    return bit + by - 2 * bit * by


def reduce_kernel(n, a_hbm, z_hbm, dy_hbm, qt_hbm, e_hbm, pleft_ref, pt_ref, q_ref, m_ref,
                  parts, g, z_v, dy_v, a_v, at_v, qt_v, qs, p_acc, h_acc, p_own, p_recv, p_all,
                  y_mate, y_own, y_recv,
                  in_sem, q_sem, a_sem, ps_sem, pr_sem, pbs_sem, pbr_sem,
                  ms_sem, mr_sem, ys_sem, yr_sem, ybs_sem, ybr_sem, qs_sem, qm_sem):
    me = lax.axis_index("data")
    d_in, d_out = m_ref.shape
    tokens = z_v.shape[0]
    n_p = d_in // 128
    n_half = y_own.shape[0]
    cw = d_out // (2 * n_half)
    core = lax.rem(me, 2)
    fx = lax.rem(lax.div(me, 2), 2)
    fy = lax.rem(lax.div(me, 4), 2)
    fz = lax.div(me, 8)
    place = fx + 2 * fy
    p_owner = (fz >= 2) & (core == 1)
    p_mine = jnp.minimum(jnp.maximum(fz - 2, 0), 1) + 2 * place
    y_owner = (fz >= 1) & (fz <= 2)
    y_mine = jnp.minimum(jnp.maximum(fz - 1, 0), 1) + 2 * place

    barrier = pltpu.get_barrier_semaphore()

    def e_copy(c):
        cols = pl.ds(pl.multiple_of(c * CB, CB), CB)
        return pltpu.make_async_copy(e_hbm.at[0, :, cols], m_ref.at[:, cols], in_sem.at[c])

    def z_copy(c):
        cols = pl.ds(pl.multiple_of(c * CB, CB), CB)
        return pltpu.make_async_copy(z_hbm.at[:, cols], z_v.at[:, cols], in_sem.at[c])

    def dy_copy(c):
        cols = pl.ds(pl.multiple_of(c * CB, CB), CB)
        return pltpu.make_async_copy(dy_hbm.at[:, cols], dy_v.at[:, cols], in_sem.at[c])

    nc = d_out // CB
    q_copy = pltpu.make_async_copy(qt_hbm, qt_v, q_sem)
    a_copy = pltpu.make_async_copy(a_hbm, a_v, a_sem)
    q_copy.start()

    def fetch(c):
        z_copy(c).start()
        dy_copy(c).start()
        e_copy(c).start()

    for c in range(AHEAD):
        fetch(c)

    @pl.loop(1, n)
    def _(k):
        pl.semaphore_signal(barrier, inc=1, device_id=(lax.rem(me + k, n),), device_id_type=MESH)

    p_acc[...] = jnp.zeros_like(p_acc)
    h_acc[...] = jnp.zeros_like(h_acc)
    q_copy.wait()
    qt = qt_v[...]
    q_max = jnp.max(jnp.abs(qt), axis=1, keepdims=True)
    qs[...] = stack3((qt / q_max) * (1.0 / d_out))

    def arrive(c):
        whole = parts.at[pl.ds(2 * c, 2), pl.ds(0, 2 * (d_in + tokens))]
        pltpu.make_async_copy(whole, whole, in_sem.at[c]).wait()

    def stream(first, count):
        for i in range(count):
            arrive(first + i)
        for i in range(count):
            if not isinstance(first, int) or first + AHEAD + i < nc:
                @pl.when(first + AHEAD + i < nc)
                def _():
                    fetch(first + AHEAD + i)
        for i in range(count):
            c = first + i
            cols = pl.ds(pl.multiple_of(c * CB, CB), CB)
            qc = qs[:, cols]
            for r in range(d_in // RB):
                rows = pl.ds(r * RB, RB)
                e1, e2, e3 = split3(m_ref[rows, cols])
                p_acc[:, rows] += (mm_nt(qc, e3) + mm_nt(qc, e2)) + mm_nt(qc, e1)
                if r % 2 == 1 and r // 2 < tokens // RB:
                    rows = pl.ds(r // 2 * RB, RB)
                    gb = gelu_grad(z_v[rows, cols], dy_v[rows, cols]).astype(BF16)
                    for h in range(CB // 128):
                        g[2 * c + h, rows, :] = gb[:, h * 128:(h + 1) * 128]
                    h_acc[:, rows] += mm_nt(qc, gb)

    stream(0, 1)

    @pl.loop(0, (nc - 2) // 2)
    def _(s):
        stream(1 + 2 * s, 2)

    a_copy.start()
    stream(nc - 1, 1)

    a_copy.wait()
    hs = stack3(fold3(h_acc[...]))
    pt = (fold3(p_acc[...]) + fold3(mm(hs, a_v[...])) * (1.0 / tokens)) * q_max * float(d_out)
    for b in range(n_p):
        p_own[b] = pt[:, b * 128:(b + 1) * 128]

    pl.semaphore_wait(barrier, n - 1)

    def remote(src, dst, send_sem, recv_sem, device):
        return pltpu.make_async_remote_copy(
            src_ref=src, dst_ref=dst, send_sem=send_sem, recv_sem=recv_sem, device_id=(device,), device_id_type=MESH)

    def bulk(ref, send_sem, recv_sem):
        return remote(ref, ref, send_sem, recv_sem, me)

    def chip_at(z, gy, gx):
        return 4 * z + 2 * flip(fy, gy) + flip(fx, gx)

    @pl.loop(0, n_p)
    def _(k):
        gy, gx = 1 - lax.div(k, 4), 1 - lax.rem(lax.div(k, 2), 2)
        half = lax.rem(k + fz, 2)
        owner = 2 * chip_at(2 + half, gy, gx) + 1
        b = half + 2 * (flip(fx, gx) + 2 * flip(fy, gy))

        @pl.when(me != owner)
        def _():
            remote(p_own.at[b], p_recv.at[lax.rem(me - owner + 2 * n - 1, n)], ps_sem, pr_sem, owner).start()

    @pl.loop(0, d_in // RB)
    def _(r):
        rows = pl.ds(pl.multiple_of(r * RB, RB), RB)
        at_v[rows, :] = a_v[:, rows].T

    def build(c):
        cols = pl.ds(pl.multiple_of(c * CB, CB), CB)
        gc = jnp.concatenate([g[2 * c + h] for h in range(CB // 128)], axis=1)
        for r in range(d_in // RB):
            rows = pl.ds(r * RB, RB)
            m = mm(at_v[rows, :], gc) * (1.0 / tokens) + m_ref[rows, cols]
            m_ref[rows, cols] = m
            for i, part in enumerate(split3(m)):
                for h in range(CB // 128):
                    parts[2 * c + h, pl.ds(i * d_in + r * RB, RB), :] = part[:, h * 128:(h + 1) * 128]

    early = jnp.minimum(2 + 3 * ((1 - fx) + (1 - fy) + (3 - fz)), nc)
    pl.loop(0, early)(build)

    @pl.when(p_owner)
    def _():
        bulk(p_recv, ps_sem, pr_sem).wait_recv()
        p_all[p_mine] = p_own[p_mine] + jnp.sum(p_recv[...], axis=0)
        tile = p_all.at[p_mine]
        for plane, gy, gx, gc in far_first((2.5, 1.5, 1, 0), 2):
            z = (0, 3, 1, 2)[plane] * (3 - fz) + plane * (fz - 2)
            remote(tile, tile, pbs_sem, pbr_sem, 2 * chip_at(z, gy, gx) + (1 - gc)).start()

    pl.loop(early, nc)(build)

    @pl.when(p_owner)
    def _():
        bulk(p_all.at[pl.ds(0, n_p - 1)], pbs_sem, pbr_sem).wait_recv()

    @pl.when(jnp.logical_not(p_owner))
    def _():
        bulk(p_all, pbs_sem, pbr_sem).wait_recv()

    p = orthonormalize(jnp.concatenate([p_all[b] for b in range(n_p)], axis=1))
    pt_ref[...] = p
    ps = stack3(p)

    def y_tile(t):
        def part(i):
            return jnp.concatenate(
                [parts[t * (cw // 128) + h, pl.ds(i * d_in, d_in), :] for h in range(cw // 128)], axis=1)
        y = mm(ps, part(2)) + mm(ps, part(1))
        return fold3(y + mm(ps, part(0)))

    mate = me + 1 - 2 * core

    def pair(k):
        gy, gx = 1 - lax.div(k, 2), 1 - lax.rem(k, 2)
        column = 2 * (flip(fx, gx) + 2 * flip(fy, gy))
        return [(lax.rem(fz + i, 2) + column, chip_at(1 + lax.rem(fz + i, 2), gy, gx)) for i in range(2)]

    @pl.loop(0, n_half // 2)
    def _(k):
        for s, _ in pair(k):
            y_mate[s] = y_tile((1 - core) * n_half + s)
        for s, _ in pair(k):
            remote(y_mate.at[s], y_mate.at[n_half + s], ms_sem, mr_sem.at[s], mate).start()

    @pl.loop(0, n_half // 2)
    def _(k):
        for s, _ in pair(k):
            bulk(y_mate.at[n_half + s], ms_sem, mr_sem.at[s]).wait_recv()
        for s, _ in pair(k):
            y_own[s] = y_tile(core * n_half + s) + y_mate[n_half + s]
        for s, chip in pair(k):
            slot = lax.rem(lax.div(me, 2) - chip + n - 1, n // 2)

            @pl.when(me != 2 * chip + core)
            def _():
                remote(y_own.at[s], y_recv.at[slot], ys_sem, yr_sem, 2 * chip + core).start()

    p1, p2, p3 = [x.astype(F32) for x in split3(p)]
    fill = jnp.zeros((128 - 9 * RANK, d_in), F32)
    pleft_ref[...] = jnp.concatenate([p1] * 3 + [p2] * 3 + [p3] * 3 + [fill], axis=0).T.astype(BF16)
    q_mine = core * n_half + y_mine

    @pl.when(y_owner)
    def _():
        bulk(y_recv, ys_sem, yr_sem).wait_recv()
        q_ref[q_mine] = (y_own[y_mine] + jnp.sum(y_recv[...], axis=0)) * (1.0 / n)
        tile = q_ref.at[q_mine]
        for plane, gy, gx, _ in far_first((2, 1, 1, 0), 1):
            there = (3, 0, 2, 1)[plane]
            z = there * (2 - fz) + (3 - there) * (fz - 1)
            remote(tile, tile, ybs_sem, ybr_sem.at[y_mine], 2 * chip_at(z, gy, gx) + core).start()
        remote(tile, tile, ybs_sem, qm_sem, mate).start()

    for s in range(n_half):
        @pl.when(jnp.logical_not(y_owner) | (y_mine != s))
        def _():
            tile = q_ref.at[core * n_half + s]
            bulk(tile, ybs_sem, ybr_sem.at[s]).wait_recv()
            remote(tile, tile, qs_sem, qm_sem, mate).start()

    bulk(q_ref.at[pl.ds(0, n_half)], qs_sem, qm_sem).wait_recv()
    bulk(y_mate.at[pl.ds(0, n_half)], ms_sem, yr_sem).wait_send()

    @pl.when(p_owner)
    def _():
        bulk(p_own.at[pl.ds(0, n_p - 1)], ps_sem, pr_sem).wait_send()
        bulk(p_recv, pbs_sem, pr_sem).wait_send()

    @pl.when(jnp.logical_not(p_owner))
    def _():
        bulk(p_own, ps_sem, pr_sem).wait_send()

    @pl.when(y_owner)
    def _():
        bulk(y_own.at[pl.ds(0, n_half - 1)], ys_sem, yr_sem).wait_send()
        bulk(q_ref, ybs_sem, qm_sem).wait_send()
        bulk(q_ref.at[pl.ds(0, n_half - 1)], qs_sem, qm_sem).wait_send()

    @pl.when(jnp.logical_not(y_owner))
    def _():
        bulk(y_own, ys_sem, yr_sem).wait_send()
        bulk(q_ref.at[pl.ds(0, n_half)], qs_sem, qm_sem).wait_send()


def apply_kernel(pleft_ref, pt_ref, q_ref, m_ref, p_out, q_out, e_out, stage, p_sem, q_sem, e_sem):
    d_in, d_out = m_ref.shape
    n_y, _, cw = q_ref.shape
    p_copy = pltpu.make_async_copy(pt_ref, p_out, p_sem)
    fill = jnp.zeros((128 - 9 * RANK, cw), F32)

    def q_copy(c):
        cols = pl.ds(pl.multiple_of(c * cw, cw), cw)
        return pltpu.make_async_copy(q_ref.at[c], q_out.at[:, cols], q_sem)

    def e_copy(c):
        cols = pl.ds(pl.multiple_of(c * cw, cw), cw)
        return pltpu.make_async_copy(stage.at[:, cols], e_out.at[0, :, cols], e_sem)

    @pl.loop(0, n_y)
    def _(c):
        cols = pl.ds(pl.multiple_of(c * cw, cw), cw)
        three = [x.astype(F32) for x in split3(q_ref[c])]
        qc = jnp.concatenate(three * 3 + [fill], axis=0).astype(BF16)
        for r in range(d_in // RB):
            rows = pl.ds(r * RB, RB)
            stage[rows, cols] = m_ref[rows, cols] - mm(pleft_ref[rows, :], qc)
        e_copy(c).start()

    p_copy.start()

    @pl.loop(0, n_y)
    def _(c):
        q_copy(c).start()

    p_copy.wait()
    pltpu.make_async_copy(q_ref, q_ref, q_sem).wait()
    pltpu.make_async_copy(stage, e_out.at[0], e_sem).wait()


def solution(mesh):
    n = mesh.shape["data"]

    def per_device(act_in, pre_act, grad_out, q_init, err_mem):
        tokens, d_in = act_in.shape
        d_out = pre_act.shape[1]
        nc, n_p, n_y = d_out // CB, d_in // 128, n // 2
        cw = d_out // n_y
        hbm = pl.BlockSpec(memory_space=pltpu.HBM)
        vmem = pl.BlockSpec(memory_space=pltpu.VMEM)
        pleft, pt, q, m = pl.pallas_call(
            functools.partial(reduce_kernel, n),
            out_shape=(
                pltpu.VMEM((d_in, 128), BF16),
                pltpu.VMEM((RANK, d_in), F32),
                pltpu.VMEM((n_y, RANK, cw), F32),
                pltpu.VMEM((d_in, d_out), F32),
            ),
            in_specs=[hbm] * 5,
            out_specs=(vmem,) * 4,
            scratch_shapes=[
                pltpu.VMEM((d_out // 128, 3 * d_in, 128), BF16),
                pltpu.VMEM((d_out // 128, tokens, 128), BF16),
                pltpu.VMEM((tokens, d_out), BF16),
                pltpu.VMEM((tokens, d_out), BF16),
                pltpu.VMEM((tokens, d_in), BF16),
                pltpu.VMEM((d_in, tokens), BF16),
                pltpu.VMEM((RANK, d_out), F32),
                pltpu.VMEM((32, d_out), BF16),
                pltpu.VMEM((32, d_in), F32),
                pltpu.VMEM((32, tokens), F32),
                pltpu.VMEM((n_p, RANK, 128), F32),
                pltpu.VMEM((n - 1, RANK, 128), F32),
                pltpu.VMEM((n_p, RANK, 128), F32),
                pltpu.VMEM((n_y, RANK, cw), F32),
                pltpu.VMEM((n_y // 2, RANK, cw), F32),
                pltpu.VMEM((n // 2 - 1, RANK, cw), F32),
                pltpu.SemaphoreType.DMA((nc,)),
            ] + [pltpu.SemaphoreType.DMA] * 7 + [pltpu.SemaphoreType.DMA((n_y // 2,))]
            + [pltpu.SemaphoreType.DMA] * 3 + [pltpu.SemaphoreType.DMA((n_y // 2,))] + [pltpu.SemaphoreType.DMA] * 2,
            compiler_params=pltpu.CompilerParams(
                collective_id=0, has_side_effects=True, vmem_limit_bytes=46 * 1024 * 1024),
            name="reduce_kernel",
        )(act_in, pre_act, grad_out, q_init.T, err_mem)
        p_t, q_t, err_new = pl.pallas_call(
            apply_kernel,
            out_shape=(
                jax.ShapeDtypeStruct((RANK, d_in), F32),
                jax.ShapeDtypeStruct((RANK, d_out), F32),
                jax.ShapeDtypeStruct((1, d_in, d_out), F32),
            ),
            in_specs=[vmem] * 4,
            out_specs=(hbm,) * 3,
            scratch_shapes=[
                pltpu.VMEM((d_in, d_out), F32),
            ] + [pltpu.SemaphoreType.DMA] * 3,
            compiler_params=pltpu.CompilerParams(vmem_limit_bytes=24 * 1024 * 1024),
            name="apply_kernel",
        )(pleft, pt, q, m)
        return p_t.T, q_t.T, err_new

    return jax.shard_map(
        per_device, mesh=mesh,
        in_specs=(P("data", None), P("data", None), P("data", None), P(None, None), P("data", None, None)),
        out_specs=(P(None, None), P(None, None), P("data", None, None)), check_vma=False)
```

```python
import functools

import jax
import jax.numpy as jnp
from jax import lax
from jax.experimental import pallas as pl
from jax.experimental.pallas import tpu as pltpu
from jax.sharding import PartitionSpec as P

F32 = jnp.float32
BF16 = jnp.bfloat16
MESH = pl.DeviceIdType.MESH
RANK = 8
CB = 256
RB = 256
SB = 128
NT = (((1,), (1,)), ((), ()))


def split3(x):
    hi = x.astype(BF16)
    rest = x - hi.astype(F32)
    mid = rest.astype(BF16)
    low = (rest - mid.astype(F32)).astype(BF16)
    return hi, mid, low


def stack3(x):
    parts = [p.astype(F32) for p in split3(x)]
    return jnp.concatenate(parts + [jnp.zeros_like(x)], axis=0).astype(BF16)


def fold3(y):
    return (y[16:24] + y[8:16]) + y[0:8]


def mm(a, b):
    return jnp.dot(a, b, preferred_element_type=F32)


def mm_nt(a, b):
    return lax.dot_general(a, b, NT, preferred_element_type=F32)


def gelu_grad(z, dy):
    c = 0.7978845608028654
    x = z.astype(F32)
    x2 = x * x
    t = jnp.tanh(x * (x2 * (c * 0.044715) + c))
    up = 1.0 + t
    slope = ((x * up) * (1.0 - t)) * (x2 * (1.5 * c * 0.044715) + 0.5 * c)
    return (0.5 * up + slope) * dy.astype(F32)


def orthonormalize(p):
    row = lax.broadcasted_iota(jnp.int32, (RANK, 1), 0)
    w = p
    norm2 = jnp.zeros((RANK, 1), F32)
    for j in range(RANK):
        v = w[j:j + 1]
        d = jnp.sum(jnp.where(row > j, p, w) * v, axis=1, keepdims=True)
        norm2 = jnp.where(row == j, d, norm2)
        if j + 1 < RANK:
            coef = jnp.where(row > j, d / d[j:j + 1], 0.0)
            w = w - coef * v
    return w / jnp.sqrt(norm2)


def far_first(near_planes, cores):
    places = [(i, fy, fx, fc) for i in range(4) for fy in range(2) for fx in range(2) for fc in range(cores)]
    places.remove((3, 0, 0, 0))
    return sorted(places, key=lambda p: -(near_planes[p[0]] + p[1] + p[2]))


def flip(bit, by):
    return bit + by - 2 * bit * by


def reduce_kernel(n, a_hbm, z_hbm, dy_hbm, qt_hbm, e_hbm, pleft_ref, pt_ref, q_ref, m_ref,
                  parts, g, z_v, dy_v, a_v, at_v, qt_v, qs, p_acc, h_acc, p_own, p_recv, p_all,
                  y_mate, y_own, y_recv,
                  in_sem, q_sem, a_sem, ps_sem, pr_sem, pbs_sem, pbr_sem,
                  ms_sem, mr_sem, ys_sem, yr_sem, ybs_sem, ybr_sem, qs_sem, qm_sem):
    me = lax.axis_index("data")
    d_in, d_out = m_ref.shape
    tokens = z_v.shape[0]
    n_p = d_in // 128
    n_half = y_own.shape[0]
    cw = d_out // (2 * n_half)
    core = lax.rem(me, 2)
    fx = lax.rem(lax.div(me, 2), 2)
    fy = lax.rem(lax.div(me, 4), 2)
    fz = lax.div(me, 8)
    place = fx + 2 * fy
    p_owner = (fz >= 2) & (core == 1)
    p_mine = jnp.minimum(jnp.maximum(fz - 2, 0), 1) + 2 * place
    y_owner = (fz >= 1) & (fz <= 2)
    y_mine = jnp.minimum(jnp.maximum(fz - 1, 0), 1) + 2 * place

    barrier = pltpu.get_barrier_semaphore()

    def e_copy(c):
        cols = pl.ds(pl.multiple_of(c * CB, CB), CB)
        return pltpu.make_async_copy(e_hbm.at[0, :, cols], m_ref.at[:, cols], in_sem.at[c])

    def z_copy(c):
        cols = pl.ds(pl.multiple_of(c * CB, CB), CB)
        return pltpu.make_async_copy(z_hbm.at[:, cols], z_v.at[:, cols], in_sem.at[c])

    def dy_copy(c):
        cols = pl.ds(pl.multiple_of(c * CB, CB), CB)
        return pltpu.make_async_copy(dy_hbm.at[:, cols], dy_v.at[:, cols], in_sem.at[c])

    nc = d_out // CB
    q_copy = pltpu.make_async_copy(qt_hbm, qt_v, q_sem)
    a_copy = pltpu.make_async_copy(a_hbm, a_v, a_sem)
    q_copy.start()

    @pl.loop(0, nc)
    def _(c):
        z_copy(c).start()
        dy_copy(c).start()
        e_copy(c).start()

        @pl.when(c == nc // 2)
        def _():
            a_copy.start()

    @pl.loop(1, n)
    def _(k):
        pl.semaphore_signal(barrier, inc=1, device_id=(lax.rem(me + k, n),), device_id_type=MESH)

    p_acc[...] = jnp.zeros_like(p_acc)
    h_acc[...] = jnp.zeros_like(h_acc)
    q_copy.wait()
    qt = qt_v[...]
    q_max = jnp.max(jnp.abs(qt), axis=1, keepdims=True)
    qs[...] = stack3((qt / q_max) * (1.0 / d_out))

    def arrive(c):
        whole = parts.at[pl.ds(2 * c, 2), pl.ds(0, 2 * (d_in + tokens))]
        pltpu.make_async_copy(whole, whole, in_sem.at[c]).wait()

    def stream(first, count):
        for i in range(count):
            arrive(first + i)
        for i in range(count):
            c = first + i
            cols = pl.ds(pl.multiple_of(c * CB, CB), CB)
            qc = qs[:, cols]
            q3 = jnp.concatenate([qc] * 3, axis=1)
            for r in range(d_in // SB):
                rows = pl.ds(r * SB, SB)
                e1, e2, e3 = split3(m_ref[rows, cols])
                p_acc[:, rows] += mm_nt(q3, jnp.concatenate([e3, e2, e1], axis=1))
                if r % 2 == 1 and r // 2 < tokens // SB:
                    rows = pl.ds(r // 2 * SB, SB)
                    gb = gelu_grad(z_v[rows, cols], dy_v[rows, cols]).astype(BF16)
                    for h in range(CB // 128):
                        g[2 * c + h, rows, :] = gb[:, h * 128:(h + 1) * 128]
                    h_acc[:, rows] += mm_nt(qc, gb)

    stream(0, 1)

    @pl.loop(0, (nc - 2) // 2)
    def _(s):
        stream(1 + 2 * s, 2)

    stream(nc - 1, 1)

    a_copy.wait()
    hs = stack3(fold3(h_acc[...]))
    pt = (fold3(p_acc[...]) + fold3(mm(hs, a_v[...])) * (1.0 / tokens)) * q_max * float(d_out)
    for b in range(n_p):
        p_own[b] = pt[:, b * 128:(b + 1) * 128]

    pl.semaphore_wait(barrier, n - 1)

    def remote(src, dst, send_sem, recv_sem, device):
        return pltpu.make_async_remote_copy(
            src_ref=src, dst_ref=dst, send_sem=send_sem, recv_sem=recv_sem, device_id=(device,), device_id_type=MESH)

    def bulk(ref, send_sem, recv_sem):
        return remote(ref, ref, send_sem, recv_sem, me)

    def chip_at(z, gy, gx):
        return 4 * z + 2 * flip(fy, gy) + flip(fx, gx)

    @pl.loop(0, n_p)
    def _(k):
        gy, gx = 1 - lax.div(k, 4), 1 - lax.rem(lax.div(k, 2), 2)
        half = lax.rem(k + fz, 2)
        owner = 2 * chip_at(2 + half, gy, gx) + 1
        b = half + 2 * (flip(fx, gx) + 2 * flip(fy, gy))

        @pl.when(me != owner)
        def _():
            remote(p_own.at[b], p_recv.at[lax.rem(me - owner + 2 * n - 1, n)], ps_sem, pr_sem, owner).start()

    @pl.loop(0, d_in // RB)
    def _(r):
        rows = pl.ds(pl.multiple_of(r * RB, RB), RB)
        at_v[rows, :] = a_v[:, rows].T

    def build(c):
        cols = pl.ds(pl.multiple_of(c * CB, CB), CB)
        gc = jnp.concatenate([g[2 * c + h] for h in range(CB // 128)], axis=1)
        for r in range(d_in // RB):
            rows = pl.ds(r * RB, RB)
            m = mm(at_v[rows, :], gc) * (1.0 / tokens) + m_ref[rows, cols]
            m_ref[rows, cols] = m
            for i, part in enumerate(split3(m)):
                for h in range(CB // 128):
                    parts[2 * c + h, pl.ds(i * d_in + r * RB, RB), :] = part[:, h * 128:(h + 1) * 128]

    early = jnp.minimum(2 + 3 * ((1 - fx) + (1 - fy) + (3 - fz)), nc)
    pl.loop(0, early)(build)

    @pl.when(p_owner)
    def _():
        bulk(p_recv, ps_sem, pr_sem).wait_recv()
        p_all[p_mine] = p_own[p_mine] + jnp.sum(p_recv[...], axis=0)
        tile = p_all.at[p_mine]
        for plane, gy, gx, gc in far_first((2.5, 1.5, 1, 0), 2):
            z = (0, 3, 1, 2)[plane] * (3 - fz) + plane * (fz - 2)
            remote(tile, tile, pbs_sem, pbr_sem, 2 * chip_at(z, gy, gx) + (1 - gc)).start()

    pl.loop(early, nc)(build)

    @pl.when(p_owner)
    def _():
        bulk(p_all.at[pl.ds(0, n_p - 1)], pbs_sem, pbr_sem).wait_recv()

    @pl.when(jnp.logical_not(p_owner))
    def _():
        bulk(p_all, pbs_sem, pbr_sem).wait_recv()

    p = orthonormalize(jnp.concatenate([p_all[b] for b in range(n_p)], axis=1))
    pt_ref[...] = p
    ps = stack3(p)

    def y_tile(t):
        def part(i):
            return jnp.concatenate(
                [parts[t * (cw // 128) + h, pl.ds(i * d_in, d_in), :] for h in range(cw // 128)], axis=1)
        y = mm(ps, part(2)) + mm(ps, part(1))
        return fold3(y + mm(ps, part(0)))

    mate = me + 1 - 2 * core

    def pair(k):
        gy, gx = 1 - lax.div(k, 2), 1 - lax.rem(k, 2)
        column = 2 * (flip(fx, gx) + 2 * flip(fy, gy))
        return [(lax.rem(fz + i, 2) + column, chip_at(1 + lax.rem(fz + i, 2), gy, gx)) for i in range(2)]

    @pl.loop(0, n_half // 2)
    def _(k):
        for s, _ in pair(k):
            y_mate[s] = y_tile((1 - core) * n_half + s)
        for s, _ in pair(k):
            remote(y_mate.at[s], y_mate.at[n_half + s], ms_sem, mr_sem.at[s], mate).start()

    @pl.loop(0, n_half // 2)
    def _(k):
        for s, _ in pair(k):
            bulk(y_mate.at[n_half + s], ms_sem, mr_sem.at[s]).wait_recv()
        for s, _ in pair(k):
            y_own[s] = y_tile(core * n_half + s) + y_mate[n_half + s]
        for s, chip in pair(k):
            slot = lax.rem(lax.div(me, 2) - chip + n - 1, n // 2)

            @pl.when(me != 2 * chip + core)
            def _():
                remote(y_own.at[s], y_recv.at[slot], ys_sem, yr_sem, 2 * chip + core).start()

    p1, p2, p3 = [x.astype(F32) for x in split3(p)]
    fill = jnp.zeros((128 - 9 * RANK, d_in), F32)
    pleft_ref[...] = jnp.concatenate([p1] * 3 + [p2] * 3 + [p3] * 3 + [fill], axis=0).T.astype(BF16)
    q_mine = core * n_half + y_mine

    @pl.when(y_owner)
    def _():
        bulk(y_recv, ys_sem, yr_sem).wait_recv()
        q_ref[q_mine] = (y_own[y_mine] + jnp.sum(y_recv[...], axis=0)) * (1.0 / n)
        tile = q_ref.at[q_mine]
        for plane, gy, gx, _ in far_first((2, 1, 1, 0), 1):
            there = (3, 0, 2, 1)[plane]
            z = there * (2 - fz) + (3 - there) * (fz - 1)
            remote(tile, tile, ybs_sem, ybr_sem.at[y_mine], 2 * chip_at(z, gy, gx) + core).start()
        remote(tile, tile, ybs_sem, qm_sem, mate).start()

    for s in range(n_half):
        @pl.when(jnp.logical_not(y_owner) | (y_mine != s))
        def _():
            tile = q_ref.at[core * n_half + s]
            bulk(tile, ybs_sem, ybr_sem.at[s]).wait_recv()
            remote(tile, tile, qs_sem, qm_sem, mate).start()

    bulk(q_ref.at[pl.ds(0, n_half)], qs_sem, qm_sem).wait_recv()
    bulk(y_mate.at[pl.ds(0, n_half)], ms_sem, yr_sem).wait_send()

    @pl.when(p_owner)
    def _():
        bulk(p_own.at[pl.ds(0, n_p - 1)], ps_sem, pr_sem).wait_send()
        bulk(p_recv, pbs_sem, pr_sem).wait_send()

    @pl.when(jnp.logical_not(p_owner))
    def _():
        bulk(p_own, ps_sem, pr_sem).wait_send()

    @pl.when(y_owner)
    def _():
        bulk(y_own.at[pl.ds(0, n_half - 1)], ys_sem, yr_sem).wait_send()
        bulk(q_ref, ybs_sem, qm_sem).wait_send()
        bulk(q_ref.at[pl.ds(0, n_half - 1)], qs_sem, qm_sem).wait_send()

    @pl.when(jnp.logical_not(y_owner))
    def _():
        bulk(y_own, ys_sem, yr_sem).wait_send()
        bulk(q_ref.at[pl.ds(0, n_half)], qs_sem, qm_sem).wait_send()


def apply_kernel(pleft_ref, pt_ref, q_ref, m_ref, p_out, q_out, e_out, stage, p_sem, q_sem, e_sem):
    d_in, d_out = m_ref.shape
    n_y, _, cw = q_ref.shape
    p_copy = pltpu.make_async_copy(pt_ref, p_out, p_sem)
    fill = jnp.zeros((128 - 9 * RANK, cw), F32)

    def q_copy(c):
        cols = pl.ds(pl.multiple_of(c * cw, cw), cw)
        return pltpu.make_async_copy(q_ref.at[c], q_out.at[:, cols], q_sem)

    def e_copy(c):
        cols = pl.ds(pl.multiple_of(c * cw, cw), cw)
        return pltpu.make_async_copy(stage.at[:, cols], e_out.at[0, :, cols], e_sem)

    @pl.loop(0, n_y)
    def _(c):
        cols = pl.ds(pl.multiple_of(c * cw, cw), cw)
        three = [x.astype(F32) for x in split3(q_ref[c])]
        qc = jnp.concatenate(three * 3 + [fill], axis=0).astype(BF16)
        for r in range(d_in // RB):
            rows = pl.ds(r * RB, RB)
            stage[rows, cols] = m_ref[rows, cols] - mm(pleft_ref[rows, :], qc)
        e_copy(c).start()

    p_copy.start()

    @pl.loop(0, n_y)
    def _(c):
        q_copy(c).start()

    p_copy.wait()
    pltpu.make_async_copy(q_ref, q_ref, q_sem).wait()
    pltpu.make_async_copy(stage, e_out.at[0], e_sem).wait()


def solution(mesh):
    n = mesh.shape["data"]

    def per_device(act_in, pre_act, grad_out, q_init, err_mem):
        tokens, d_in = act_in.shape
        d_out = pre_act.shape[1]
        nc, n_p, n_y = d_out // CB, d_in // 128, n // 2
        cw = d_out // n_y
        hbm = pl.BlockSpec(memory_space=pltpu.HBM)
        vmem = pl.BlockSpec(memory_space=pltpu.VMEM)
        pleft, pt, q, m = pl.pallas_call(
            functools.partial(reduce_kernel, n),
            out_shape=(
                pltpu.VMEM((d_in, 128), BF16),
                pltpu.VMEM((RANK, d_in), F32),
                pltpu.VMEM((n_y, RANK, cw), F32),
                pltpu.VMEM((d_in, d_out), F32),
            ),
            in_specs=[hbm] * 5,
            out_specs=(vmem,) * 4,
            scratch_shapes=[
                pltpu.VMEM((d_out // 128, 3 * d_in, 128), BF16),
                pltpu.VMEM((d_out // 128, tokens, 128), BF16),
                pltpu.VMEM((tokens, d_out), BF16),
                pltpu.VMEM((tokens, d_out), BF16),
                pltpu.VMEM((tokens, d_in), BF16),
                pltpu.VMEM((d_in, tokens), BF16),
                pltpu.VMEM((RANK, d_out), F32),
                pltpu.VMEM((32, d_out), BF16),
                pltpu.VMEM((32, d_in), F32),
                pltpu.VMEM((32, tokens), F32),
                pltpu.VMEM((n_p, RANK, 128), F32),
                pltpu.VMEM((n - 1, RANK, 128), F32),
                pltpu.VMEM((n_p, RANK, 128), F32),
                pltpu.VMEM((n_y, RANK, cw), F32),
                pltpu.VMEM((n_y // 2, RANK, cw), F32),
                pltpu.VMEM((n // 2 - 1, RANK, cw), F32),
                pltpu.SemaphoreType.DMA((nc,)),
            ] + [pltpu.SemaphoreType.DMA] * 7 + [pltpu.SemaphoreType.DMA((n_y // 2,))]
            + [pltpu.SemaphoreType.DMA] * 3 + [pltpu.SemaphoreType.DMA((n_y // 2,))] + [pltpu.SemaphoreType.DMA] * 2,
            compiler_params=pltpu.CompilerParams(
                collective_id=0, has_side_effects=True, vmem_limit_bytes=46 * 1024 * 1024),
            name="reduce_kernel",
        )(act_in, pre_act, grad_out, q_init.T, err_mem)
        p_t, q_t, err_new = pl.pallas_call(
            apply_kernel,
            out_shape=(
                jax.ShapeDtypeStruct((RANK, d_in), F32),
                jax.ShapeDtypeStruct((RANK, d_out), F32),
                jax.ShapeDtypeStruct((1, d_in, d_out), F32),
            ),
            in_specs=[vmem] * 4,
            out_specs=(hbm,) * 3,
            scratch_shapes=[
                pltpu.VMEM((d_in, d_out), F32),
            ] + [pltpu.SemaphoreType.DMA] * 3,
            compiler_params=pltpu.CompilerParams(vmem_limit_bytes=24 * 1024 * 1024),
            name="apply_kernel",
        )(pleft, pt, q, m)
        return p_t.T, q_t.T, err_new

    return jax.shard_map(
        per_device, mesh=mesh,
        in_specs=(P("data", None), P("data", None), P("data", None), P(None, None), P("data", None, None)),
        out_specs=(P(None, None), P(None, None), P("data", None, None)), check_vma=False)
```

```python
import functools

import jax
import jax.numpy as jnp
from jax import lax
from jax.experimental import pallas as pl
from jax.experimental.pallas import tpu as pltpu
from jax.sharding import PartitionSpec as P

F32 = jnp.float32
BF16 = jnp.bfloat16
MESH = pl.DeviceIdType.MESH
RANK = 8
CB = 256
RB = 256
NT = (((1,), (1,)), ((), ()))


def split3(x):
    hi = x.astype(BF16)
    rest = x - hi.astype(F32)
    mid = rest.astype(BF16)
    low = (rest - mid.astype(F32)).astype(BF16)
    return hi, mid, low


def stack3(x):
    parts = [p.astype(F32) for p in split3(x)]
    return jnp.concatenate(parts + [jnp.zeros_like(x)], axis=0).astype(BF16)


def fold3(y):
    return (y[16:24] + y[8:16]) + y[0:8]


def mm(a, b):
    return jnp.dot(a, b, preferred_element_type=F32)


def mm_nt(a, b):
    return lax.dot_general(a, b, NT, preferred_element_type=F32)


def gelu_grad(z, dy):
    c = 0.7978845608028654
    x = z.astype(F32)
    x2 = x * x
    t = jnp.tanh(x * (x2 * (c * 0.044715) + c))
    up = 1.0 + t
    slope = ((x * up) * (1.0 - t)) * (x2 * (1.5 * c * 0.044715) + 0.5 * c)
    return (0.5 * up + slope) * dy.astype(F32)


def orthonormalize(p):
    row = lax.broadcasted_iota(jnp.int32, (RANK, 1), 0)
    w = p
    norm2 = jnp.zeros((RANK, 1), F32)
    for j in range(RANK):
        v = w[j:j + 1]
        d = jnp.sum(jnp.where(row > j, p, w) * v, axis=1, keepdims=True)
        norm2 = jnp.where(row == j, d, norm2)
        if j + 1 < RANK:
            coef = jnp.where(row > j, d / d[j:j + 1], 0.0)
            w = w - coef * v
    return w / jnp.sqrt(norm2)


def far_first(near_planes, cores):
    places = [(i, fy, fx, fc) for i in range(4) for fy in range(2) for fx in range(2) for fc in range(cores)]
    places.remove((3, 0, 0, 0))
    return sorted(places, key=lambda p: -(near_planes[p[0]] + p[1] + p[2]))


def flip(bit, by):
    return bit + by - 2 * bit * by


def reduce_kernel(n, a_hbm, z_hbm, dy_hbm, qt_hbm, e_hbm, pleft_ref, pt_ref, q_ref, m_ref,
                  parts, g, z_v, dy_v, a_v, at_v, qt_v, qs, p_acc, h_acc, p_own, p_recv, p_all,
                  y_mate, y_own, y_recv,
                  in_sem, q_sem, a_sem, ps_sem, pr_sem, pbs_sem, pbr_sem,
                  ms_sem, mr_sem, ys_sem, yr_sem, ybs_sem, ybr_sem, qs_sem, qm_sem):
    me = lax.axis_index("data")
    d_in, d_out = m_ref.shape
    tokens = z_v.shape[0]
    n_p = d_in // 128
    n_half = y_own.shape[0]
    cw = d_out // (2 * n_half)
    core = lax.rem(me, 2)
    fx = lax.rem(lax.div(me, 2), 2)
    fy = lax.rem(lax.div(me, 4), 2)
    fz = lax.div(me, 8)
    place = fx + 2 * fy
    here = lax.div(me, 2)
    last = n // 2 - 1
    p_owner = (here >= last - 2) | (here == last - 4)
    p_mine = 2 * jnp.minimum(last - here, n_p // 2 - 1) + core
    y_owner = fz <= 1
    y_mine = jnp.minimum(fz, 1) + 2 * place

    barrier = pltpu.get_barrier_semaphore()

    def e_copy(c):
        cols = pl.ds(pl.multiple_of(c * CB, CB), CB)
        return pltpu.make_async_copy(e_hbm.at[0, :, cols], m_ref.at[:, cols], in_sem.at[c])

    def z_copy(c):
        cols = pl.ds(pl.multiple_of(c * CB, CB), CB)
        return pltpu.make_async_copy(z_hbm.at[:, cols], z_v.at[:, cols], in_sem.at[c])

    def dy_copy(c):
        cols = pl.ds(pl.multiple_of(c * CB, CB), CB)
        return pltpu.make_async_copy(dy_hbm.at[:, cols], dy_v.at[:, cols], in_sem.at[c])

    nc = d_out // CB
    q_copy = pltpu.make_async_copy(qt_hbm, qt_v, q_sem)
    a_copy = pltpu.make_async_copy(a_hbm, a_v, a_sem)
    q_copy.start()

    @pl.loop(0, nc)
    def _(c):
        z_copy(c).start()
        dy_copy(c).start()
        e_copy(c).start()

        @pl.when(c == nc // 2)
        def _():
            a_copy.start()

    @pl.loop(1, n)
    def _(k):
        pl.semaphore_signal(barrier, inc=1, device_id=(lax.rem(me + k, n),), device_id_type=MESH)

    p_acc[...] = jnp.zeros_like(p_acc)
    h_acc[...] = jnp.zeros_like(h_acc)
    q_copy.wait()
    qt = qt_v[...]
    q_max = jnp.max(jnp.abs(qt), axis=1, keepdims=True)
    qs[...] = stack3((qt / q_max) * (1.0 / d_out))

    def arrive(c):
        whole = parts.at[pl.ds(2 * c, 2), pl.ds(0, 2 * (d_in + tokens))]
        pltpu.make_async_copy(whole, whole, in_sem.at[c]).wait()

    def stream(first, count):
        for i in range(count):
            arrive(first + i)
        for i in range(count):
            c = first + i
            cols = pl.ds(pl.multiple_of(c * CB, CB), CB)
            qc = qs[:, cols]
            for r in range(d_in // RB):
                rows = pl.ds(r * RB, RB)
                e1, e2, e3 = split3(m_ref[rows, cols])
                p_acc[:, rows] += (mm_nt(qc, e3) + mm_nt(qc, e2)) + mm_nt(qc, e1)
                if r % 2 == 1 and r // 2 < tokens // RB:
                    rows = pl.ds(r // 2 * RB, RB)
                    gb = gelu_grad(z_v[rows, cols], dy_v[rows, cols]).astype(BF16)
                    for h in range(CB // 128):
                        g[2 * c + h, rows, :] = gb[:, h * 128:(h + 1) * 128]
                    h_acc[:, rows] += mm_nt(qc, gb)

    stream(0, 1)

    @pl.loop(0, (nc - 2) // 2)
    def _(s):
        stream(1 + 2 * s, 2)

    stream(nc - 1, 1)

    a_copy.wait()
    hs = stack3(fold3(h_acc[...]))
    pt = (fold3(p_acc[...]) + fold3(mm(hs, a_v[...])) * (1.0 / tokens)) * q_max * float(d_out)
    for b in range(n_p):
        p_own[b] = pt[:, b * 128:(b + 1) * 128]

    pl.semaphore_wait(barrier, n - 1)

    def remote(src, dst, send_sem, recv_sem, device):
        return pltpu.make_async_remote_copy(
            src_ref=src, dst_ref=dst, send_sem=send_sem, recv_sem=recv_sem, device_id=(device,), device_id_type=MESH)

    def bulk(ref, send_sem, recv_sem):
        return remote(ref, ref, send_sem, recv_sem, me)

    def chip_at(z, gy, gx):
        return 4 * z + 2 * flip(fy, gy) + flip(fx, gx)

    @pl.loop(0, n_p)
    def _(k):
        b = lax.rem(k + me, n_p)
        near = lax.div(b, 2)
        owner = 2 * (last - near - lax.div(near, 3)) + lax.rem(b, 2)

        @pl.when(me != owner)
        def _():
            remote(p_own.at[b], p_recv.at[lax.rem(me - owner + 2 * n - 1, n)], ps_sem, pr_sem, owner).start()

    @pl.loop(0, d_in // RB)
    def _(r):
        rows = pl.ds(pl.multiple_of(r * RB, RB), RB)
        at_v[rows, :] = a_v[:, rows].T

    def build(c):
        cols = pl.ds(pl.multiple_of(c * CB, CB), CB)
        gc = jnp.concatenate([g[2 * c + h] for h in range(CB // 128)], axis=1)
        for r in range(d_in // RB):
            rows = pl.ds(r * RB, RB)
            m = mm(at_v[rows, :], gc) * (1.0 / tokens) + m_ref[rows, cols]
            m_ref[rows, cols] = m
            for i, part in enumerate(split3(m)):
                for h in range(CB // 128):
                    parts[2 * c + h, pl.ds(i * d_in + r * RB, RB), :] = part[:, h * 128:(h + 1) * 128]

    early = jnp.where(here == last, 3, 6)
    pl.loop(0, early)(build)

    @pl.when(p_owner)
    def _():
        bulk(p_recv, ps_sem, pr_sem).wait_recv()
        p_all[p_mine] = p_own[p_mine] + jnp.sum(p_recv[...], axis=0)
        tile = p_all.at[p_mine]
        for plane, gy, gx, gc in far_first((3, 2, 1, 0), 2):
            z = (0, 1, 5 - fz, fz)[plane]
            there = chip_at(z, gy, gx)
            remote(tile, tile, pbs_sem, pbr_sem, 2 * there + flip(core, gc)).start()

    pl.loop(early, nc)(build)

    @pl.when(p_owner)
    def _():
        bulk(p_all.at[pl.ds(0, n_p - 1)], pbs_sem, pbr_sem).wait_recv()

    @pl.when(jnp.logical_not(p_owner))
    def _():
        bulk(p_all, pbs_sem, pbr_sem).wait_recv()

    p = orthonormalize(jnp.concatenate([p_all[b] for b in range(n_p)], axis=1))
    pt_ref[...] = p
    ps = stack3(p)

    def y_tile(t):
        def part(i):
            return jnp.concatenate(
                [parts[t * (cw // 128) + h, pl.ds(i * d_in, d_in), :] for h in range(cw // 128)], axis=1)
        y = mm(ps, part(2)) + mm(ps, part(1))
        return fold3(y + mm(ps, part(0)))

    mate = me + 1 - 2 * core

    def pair(k):
        gy, gx = 1 - lax.div(k, 2), 1 - lax.rem(k, 2)
        column = 2 * (flip(fx, gx) + 2 * flip(fy, gy))
        return [(lax.rem(fz + i, 2) + column, chip_at(lax.rem(fz + i, 2), gy, gx)) for i in range(2)]

    @pl.loop(0, n_half // 2)
    def _(k):
        for s, _ in pair(k):
            y_mate[s] = y_tile((1 - core) * n_half + s)
        for s, _ in pair(k):
            remote(y_mate.at[s], y_mate.at[n_half + s], ms_sem, mr_sem.at[s], mate).start()

    @pl.loop(0, n_half // 2)
    def _(k):
        for s, _ in pair(k):
            bulk(y_mate.at[n_half + s], ms_sem, mr_sem.at[s]).wait_recv()
        for s, _ in pair(k):
            y_own[s] = y_tile(core * n_half + s) + y_mate[n_half + s]
        for s, chip in pair(k):
            slot = lax.rem(lax.div(me, 2) - chip + n - 1, n // 2)

            @pl.when(me != 2 * chip + core)
            def _():
                remote(y_own.at[s], y_recv.at[slot], ys_sem, yr_sem, 2 * chip + core).start()

    p1, p2, p3 = [x.astype(F32) for x in split3(p)]
    fill = jnp.zeros((128 - 9 * RANK, d_in), F32)
    pleft_ref[...] = jnp.concatenate([p1] * 3 + [p2] * 3 + [p3] * 3 + [fill], axis=0).T.astype(BF16)
    q_mine = core * n_half + y_mine

    @pl.when(y_owner)
    def _():
        bulk(y_recv, ys_sem, yr_sem).wait_recv()
        q_ref[q_mine] = (y_own[y_mine] + jnp.sum(y_recv[...], axis=0)) * (1.0 / n)
        tile = q_ref.at[q_mine]

        @pl.when(here != 0)
        def _():
            remote(tile, tile, ybs_sem, ybr_sem.at[y_mine], core).start()
            remote(tile, tile, ybs_sem, qm_sem, 1 - core).start()

        for plane, gy, gx, _ in far_first((2.5, 1.5, 1, 0), 1):
            there = chip_at((3, 2, 1 - fz, fz)[plane], gy, gx)

            @pl.when(there != 0)
            def _():
                remote(tile, tile, ybs_sem, ybr_sem.at[y_mine], 2 * there + core).start()

        remote(tile, tile, ybs_sem, qm_sem, mate).start()

    for s in range(n_half):
        @pl.when(jnp.logical_not(y_owner) | (y_mine != s))
        def _():
            tile = q_ref.at[core * n_half + s]
            bulk(tile, ybs_sem, ybr_sem.at[s]).wait_recv()

            @pl.when(here != 0)
            def _():
                remote(tile, tile, qs_sem, qm_sem, mate).start()

    bulk(q_ref.at[pl.ds(0, n_half)], qs_sem, qm_sem).wait_recv()
    bulk(y_mate.at[pl.ds(0, n_half)], ms_sem, yr_sem).wait_send()

    @pl.when(p_owner)
    def _():
        bulk(p_own.at[pl.ds(0, n_p - 1)], ps_sem, pr_sem).wait_send()
        bulk(p_recv, pbs_sem, pr_sem).wait_send()

    @pl.when(jnp.logical_not(p_owner))
    def _():
        bulk(p_own, ps_sem, pr_sem).wait_send()

    @pl.when(y_owner)
    def _():
        bulk(y_own.at[pl.ds(0, n_half - 1)], ys_sem, yr_sem).wait_send()

    @pl.when(here == 0)
    def _():
        bulk(q_ref, ybs_sem, qm_sem).wait_send()

    @pl.when(y_owner & (here != 0))
    def _():
        bulk(parts.at[0, pl.ds(0, (2 * n_half + 1) * RANK * cw // 64)], ybs_sem, qm_sem).wait_send()
        bulk(q_ref.at[pl.ds(0, n_half - 1)], qs_sem, qm_sem).wait_send()

    @pl.when(jnp.logical_not(y_owner))
    def _():
        bulk(y_own, ys_sem, yr_sem).wait_send()
        bulk(q_ref.at[pl.ds(0, n_half)], qs_sem, qm_sem).wait_send()


def apply_kernel(pleft_ref, pt_ref, q_ref, m_ref, p_out, q_out, e_out, stage, p_sem, q_sem, e_sem):
    d_in, d_out = m_ref.shape
    n_y, _, cw = q_ref.shape
    p_copy = pltpu.make_async_copy(pt_ref, p_out, p_sem)
    fill = jnp.zeros((128 - 9 * RANK, cw), F32)

    def q_copy(c):
        cols = pl.ds(pl.multiple_of(c * cw, cw), cw)
        return pltpu.make_async_copy(q_ref.at[c], q_out.at[:, cols], q_sem)

    def e_copy(c):
        cols = pl.ds(pl.multiple_of(c * cw, cw), cw)
        return pltpu.make_async_copy(stage.at[:, cols], e_out.at[0, :, cols], e_sem)

    @pl.loop(0, n_y)
    def _(c):
        cols = pl.ds(pl.multiple_of(c * cw, cw), cw)
        three = [x.astype(F32) for x in split3(q_ref[c])]
        qc = jnp.concatenate(three * 3 + [fill], axis=0).astype(BF16)
        for r in range(d_in // RB):
            rows = pl.ds(r * RB, RB)
            stage[rows, cols] = m_ref[rows, cols] - mm(pleft_ref[rows, :], qc)
        e_copy(c).start()

    p_copy.start()

    @pl.loop(0, n_y)
    def _(c):
        q_copy(c).start()

    p_copy.wait()
    pltpu.make_async_copy(q_ref, q_ref, q_sem).wait()
    pltpu.make_async_copy(stage, e_out.at[0], e_sem).wait()


def solution(mesh):
    n = mesh.shape["data"]

    def per_device(act_in, pre_act, grad_out, q_init, err_mem):
        tokens, d_in = act_in.shape
        d_out = pre_act.shape[1]
        nc, n_p, n_y = d_out // CB, d_in // 128, n // 2
        cw = d_out // n_y
        hbm = pl.BlockSpec(memory_space=pltpu.HBM)
        vmem = pl.BlockSpec(memory_space=pltpu.VMEM)
        pleft, pt, q, m = pl.pallas_call(
            functools.partial(reduce_kernel, n),
            out_shape=(
                pltpu.VMEM((d_in, 128), BF16),
                pltpu.VMEM((RANK, d_in), F32),
                pltpu.VMEM((n_y, RANK, cw), F32),
                pltpu.VMEM((d_in, d_out), F32),
            ),
            in_specs=[hbm] * 5,
            out_specs=(vmem,) * 4,
            scratch_shapes=[
                pltpu.VMEM((d_out // 128, 3 * d_in, 128), BF16),
                pltpu.VMEM((d_out // 128, tokens, 128), BF16),
                pltpu.VMEM((tokens, d_out), BF16),
                pltpu.VMEM((tokens, d_out), BF16),
                pltpu.VMEM((tokens, d_in), BF16),
                pltpu.VMEM((d_in, tokens), BF16),
                pltpu.VMEM((RANK, d_out), F32),
                pltpu.VMEM((32, d_out), BF16),
                pltpu.VMEM((32, d_in), F32),
                pltpu.VMEM((32, tokens), F32),
                pltpu.VMEM((n_p, RANK, 128), F32),
                pltpu.VMEM((n - 1, RANK, 128), F32),
                pltpu.VMEM((n_p, RANK, 128), F32),
                pltpu.VMEM((n_y, RANK, cw), F32),
                pltpu.VMEM((n_y // 2, RANK, cw), F32),
                pltpu.VMEM((n // 2 - 1, RANK, cw), F32),
                pltpu.SemaphoreType.DMA((nc,)),
            ] + [pltpu.SemaphoreType.DMA] * 7 + [pltpu.SemaphoreType.DMA((n_y // 2,))]
            + [pltpu.SemaphoreType.DMA] * 3 + [pltpu.SemaphoreType.DMA((n_y // 2,))] + [pltpu.SemaphoreType.DMA] * 2,
            compiler_params=pltpu.CompilerParams(
                collective_id=0, has_side_effects=True, vmem_limit_bytes=46 * 1024 * 1024),
            name="reduce_kernel",
        )(act_in, pre_act, grad_out, q_init.T, err_mem)
        p_t, q_t, err_new = pl.pallas_call(
            apply_kernel,
            out_shape=(
                jax.ShapeDtypeStruct((RANK, d_in), F32),
                jax.ShapeDtypeStruct((RANK, d_out), F32),
                jax.ShapeDtypeStruct((1, d_in, d_out), F32),
            ),
            in_specs=[vmem] * 4,
            out_specs=(hbm,) * 3,
            scratch_shapes=[
                pltpu.VMEM((d_in, d_out), F32),
            ] + [pltpu.SemaphoreType.DMA] * 3,
            compiler_params=pltpu.CompilerParams(vmem_limit_bytes=24 * 1024 * 1024),
            name="apply_kernel",
        )(pleft, pt, q, m)
        return p_t.T, q_t.T, err_new

    return jax.shard_map(
        per_device, mesh=mesh,
        in_specs=(P("data", None), P("data", None), P("data", None), P(None, None), P("data", None, None)),
        out_specs=(P(None, None), P(None, None), P("data", None, None)), check_vma=False)
```

```python
import functools

import jax
import jax.numpy as jnp
from jax import lax
from jax.experimental import pallas as pl
from jax.experimental.pallas import tpu as pltpu
from jax.sharding import PartitionSpec as P

F32 = jnp.float32
BF16 = jnp.bfloat16
MESH = pl.DeviceIdType.MESH
RANK = 8
CB = 256
RB = 256
NT = (((1,), (1,)), ((), ()))


def split3(x):
    hi = x.astype(BF16)
    rest = x - hi.astype(F32)
    mid = rest.astype(BF16)
    low = (rest - mid.astype(F32)).astype(BF16)
    return hi, mid, low


def stack3(x):
    parts = [p.astype(F32) for p in split3(x)]
    return jnp.concatenate(parts + [jnp.zeros_like(x)], axis=0).astype(BF16)


def fold3(y):
    return (y[16:24] + y[8:16]) + y[0:8]


def mm(a, b):
    return jnp.dot(a, b, preferred_element_type=F32)


def mm_nt(a, b):
    return lax.dot_general(a, b, NT, preferred_element_type=F32)


def gelu_grad(z, dy):
    c = 0.7978845608028654
    x = z.astype(F32)
    x2 = x * x
    t = jnp.tanh(x * (x2 * (c * 0.044715) + c))
    up = 1.0 + t
    slope = ((x * up) * (1.0 - t)) * (x2 * (1.5 * c * 0.044715) + 0.5 * c)
    return (0.5 * up + slope) * dy.astype(F32)


def orthonormalize(p):
    row = lax.broadcasted_iota(jnp.int32, (RANK, 1), 0)
    w = p
    norm2 = jnp.zeros((RANK, 1), F32)
    for j in range(RANK):
        v = w[j:j + 1]
        d = jnp.sum(jnp.where(row > j, p, w) * v, axis=1, keepdims=True)
        norm2 = jnp.where(row == j, d, norm2)
        if j + 1 < RANK:
            coef = jnp.where(row > j, d / d[j:j + 1], 0.0)
            w = w - coef * v
    return w / jnp.sqrt(norm2)


def far_first():
    places = [(i, fy, fx, fc) for i in range(4) for fy in range(2) for fx in range(2) for fc in range(2)]
    places.remove((3, 0, 0, 0))
    return sorted(places, key=lambda p: -((2, 1, 1, 0)[p[0]] + p[1] + p[2]))


def reduce_kernel(n, a_hbm, z_hbm, dy_hbm, qt_hbm, e_hbm, pleft_ref, pt_ref, q_ref, m_ref,
                  parts, g, z_v, dy_v, a_v, at_v, qt_v, qs, p_acc, h_acc, p_own, p_recv, p_all,
                  y_mate, y_own, y_recv,
                  in_sem, q_sem, a_sem, ps_sem, pr_sem, pbs_sem, pbr_sem,
                  ms_sem, mr_sem, ys_sem, yr_sem, ybs_sem, ybr_sem):
    me = lax.axis_index("data")
    d_in, tokens = at_v.shape
    d_out = qt_v.shape[1]
    n_p = d_in // 128
    n_half = y_own.shape[0]
    cw = d_out // (2 * n_half)
    core = lax.rem(me, 2)
    fx = lax.rem(lax.div(me, 2), 2)
    fy = lax.rem(lax.div(me, 4), 2)
    fz = lax.div(me, 8)
    central = (fz >= 1) & (fz <= 2)
    mine = jnp.minimum(jnp.maximum(fz - 1, 0), 1) + 2 * (fx + 2 * fy)

    def owner_chip(s):
        return 4 * (1 + lax.rem(s, 2)) + lax.div(s, 2)

    barrier = pltpu.get_barrier_semaphore()

    def fetch(c):
        for h in range(CB // 128):
            i = c * (CB // 128) + h
            cols = pl.ds(pl.multiple_of(i * 128, 128), 128)
            pltpu.make_async_copy(z_hbm.at[:, cols], z_v.at[i], in_sem.at[c]).start()
            pltpu.make_async_copy(dy_hbm.at[:, cols], dy_v.at[i], in_sem.at[c]).start()
            pltpu.make_async_copy(e_hbm.at[0, :, cols], m_ref.at[i], in_sem.at[c]).start()

    def wide(ref, c, rows):
        return jnp.concatenate([ref[c * (CB // 128) + h, rows, :] for h in range(CB // 128)], axis=1)

    nc = d_out // CB
    q_copy = pltpu.make_async_copy(qt_hbm, qt_v, q_sem)
    a_copy = pltpu.make_async_copy(a_hbm, a_v, a_sem)
    q_copy.start()

    @pl.loop(0, nc)
    def _(c):
        fetch(c)

        @pl.when(c == nc // 2)
        def _():
            a_copy.start()

    @pl.loop(1, n)
    def _(k):
        pl.semaphore_signal(barrier, inc=1, device_id=(lax.rem(me + k, n),), device_id_type=MESH)

    p_acc[...] = jnp.zeros_like(p_acc)
    h_acc[...] = jnp.zeros_like(h_acc)
    q_copy.wait()
    qt = qt_v[...]
    q_max = jnp.max(jnp.abs(qt), axis=1, keepdims=True)
    qs[...] = stack3((qt / q_max) * (1.0 / d_out))

    def arrive(c):
        whole = parts.at[pl.ds(2 * c, 2), pl.ds(0, 2 * (d_in + tokens))]
        pltpu.make_async_copy(whole, whole, in_sem.at[c]).wait()

    def stream(first, count):
        for i in range(count):
            arrive(first + i)
        for i in range(count):
            c = first + i
            cols = pl.ds(pl.multiple_of(c * CB, CB), CB)
            qc = qs[:, cols]
            for r in range(d_in // RB):
                rows = pl.ds(r * RB, RB)
                e1, e2, e3 = split3(wide(m_ref, c, rows))
                p_acc[:, rows] += (mm_nt(qc, e3) + mm_nt(qc, e2)) + mm_nt(qc, e1)
                if r % 2 == 1 and r // 2 < tokens // RB:
                    rows = pl.ds(r // 2 * RB, RB)
                    gb = gelu_grad(wide(z_v, c, rows), wide(dy_v, c, rows)).astype(BF16)
                    for h in range(CB // 128):
                        g[2 * c + h, rows, :] = gb[:, h * 128:(h + 1) * 128]
                    h_acc[:, rows] += mm_nt(qc, gb)

    stream(0, 1)

    @pl.loop(0, (nc - 2) // 2)
    def _(s):
        stream(1 + 2 * s, 2)

    stream(nc - 1, 1)

    a_copy.wait()
    hs = stack3(fold3(h_acc[...]))
    pt = (fold3(p_acc[...]) + fold3(mm(hs, a_v[...])) * (1.0 / tokens)) * q_max * float(d_out)
    for b in range(n_p):
        p_own[b] = pt[:, b * 128:(b + 1) * 128]

    pl.semaphore_wait(barrier, n - 1)

    def remote(src, dst, send_sem, recv_sem, device):
        return pltpu.make_async_remote_copy(
            src_ref=src, dst_ref=dst, send_sem=send_sem, recv_sem=recv_sem, device_id=(device,), device_id_type=MESH)

    def bulk(ref, send_sem, recv_sem):
        return remote(ref, ref, send_sem, recv_sem, me)

    def broadcast(buf, index, send_sem, recv_sem):
        for plane, gy, gx, gc in far_first():
            there = (3, 0, 2, 1)[plane]
            z = there * (2 - fz) + (3 - there) * (fz - 1)
            y = 1 - fy if gy else fy
            x = 1 - fx if gx else fx
            c = 1 - core if gc else core
            remote(buf.at[index], buf.at[index], send_sem, recv_sem, z * 8 + y * 4 + x * 2 + c).start()

    p_owner = central & (core == 1)

    @pl.loop(0, n_p)
    def _(b):
        owner = 2 * owner_chip(b) + 1

        @pl.when(me != owner)
        def _():
            remote(p_own.at[b], p_recv.at[lax.rem(me - owner + 2 * n - 1, n)], ps_sem, pr_sem, owner).start()

    @pl.loop(0, d_in // RB)
    def _(r):
        rows = pl.ds(pl.multiple_of(r * RB, RB), RB)
        at_v[rows, :] = a_v[:, rows].T

    def build(c):
        gc = wide(g, c, pl.ds(0, tokens))
        for r in range(d_in // RB):
            rows = pl.ds(r * RB, RB)
            m = mm(at_v[rows, :], gc) * (1.0 / tokens) + wide(m_ref, c, rows)
            for h in range(CB // 128):
                m_ref[2 * c + h, rows, :] = m[:, h * 128:(h + 1) * 128]
            for i, part in enumerate(split3(m)):
                for h in range(CB // 128):
                    parts[2 * c + h, pl.ds(i * d_in + r * RB, RB), :] = part[:, h * 128:(h + 1) * 128]

    pl.loop(0, nc // 2 + 1)(build)

    @pl.when(p_owner)
    def _():
        bulk(p_recv, ps_sem, pr_sem).wait_recv()
        p_all[mine] = p_own[mine] + jnp.sum(p_recv[...], axis=0)
        broadcast(p_all, mine, pbs_sem, pbr_sem)

    pl.loop(nc // 2 + 1, nc)(build)

    @pl.when(p_owner)
    def _():
        bulk(p_all.at[pl.ds(0, n_p - 1)], pbs_sem, pbr_sem).wait_recv()

    @pl.when(jnp.logical_not(p_owner))
    def _():
        bulk(p_all, pbs_sem, pbr_sem).wait_recv()

    p = orthonormalize(jnp.concatenate([p_all[b] for b in range(n_p)], axis=1))
    pt_ref[...] = p
    ps = stack3(p)

    def y_tile(t):
        def part(i):
            return jnp.concatenate(
                [parts[t * (cw // 128) + h, pl.ds(i * d_in, d_in), :] for h in range(cw // 128)], axis=1)
        y = mm(ps, part(2)) + mm(ps, part(1))
        return fold3(y + mm(ps, part(0)))

    mate = me + 1 - 2 * core

    @pl.loop(0, n_half // 2)
    def _(k):
        for i in range(2):
            s = 2 * k + i
            y_mate[s] = y_tile((1 - core) * n_half + s)
        for i in range(2):
            s = 2 * k + i
            remote(y_mate.at[s], y_mate.at[n_half + s], ms_sem, mr_sem.at[s], mate).start()

    @pl.loop(0, n_half // 2)
    def _(k):
        for i in range(2):
            s = 2 * k + i
            bulk(y_mate.at[n_half + s], ms_sem, mr_sem.at[s]).wait_recv()
        for i in range(2):
            s = 2 * k + i
            y_own[s] = y_tile(core * n_half + s) + y_mate[n_half + s]
        for i in range(2):
            s = 2 * k + i
            chip = owner_chip(s)
            slot = lax.rem(lax.div(me, 2) - chip + n - 1, n // 2)

            @pl.when(me != 2 * chip + core)
            def _():
                remote(y_own.at[s], y_recv.at[slot], ys_sem, yr_sem, 2 * chip + core).start()

    p1, p2, p3 = [x.astype(F32) for x in split3(p)]
    fill = jnp.zeros((128 - 9 * RANK, d_in), F32)
    pleft_ref[...] = jnp.concatenate([p1] * 3 + [p2] * 3 + [p3] * 3 + [fill], axis=0).T.astype(BF16)
    q_mine = core * n_half + mine

    @pl.when(central)
    def _():
        bulk(y_recv, ys_sem, yr_sem).wait_recv()
        q_ref[q_mine] = (y_own[mine] + jnp.sum(y_recv[...], axis=0)) * (1.0 / n)
        broadcast(q_ref, q_mine, ybs_sem, ybr_sem)

    bulk(y_mate.at[pl.ds(0, n_half)], ms_sem, yr_sem).wait_send()

    @pl.when(p_owner)
    def _():
        bulk(p_own.at[pl.ds(0, n_p - 1)], ps_sem, pr_sem).wait_send()
        bulk(p_recv, pbs_sem, pr_sem).wait_send()

    @pl.when(jnp.logical_not(p_owner))
    def _():
        bulk(p_own, ps_sem, pr_sem).wait_send()

    @pl.when(central)
    def _():
        bulk(y_own.at[pl.ds(0, n_half - 1)], ys_sem, yr_sem).wait_send()
        bulk(q_ref.at[pl.ds(0, 2 * n_half - 1)], ybs_sem, ybr_sem).wait_recv()
        bulk(parts.at[0, pl.ds(0, (n - 1) * RANK * cw // 64)], ybs_sem, yr_sem).wait_send()

    @pl.when(jnp.logical_not(central))
    def _():
        bulk(y_own, ys_sem, yr_sem).wait_send()
        bulk(q_ref, ybs_sem, ybr_sem).wait_recv()


def apply_kernel(pleft_ref, pt_ref, q_ref, m_ref, p_out, q_out, e_out, stage, p_sem, q_sem, e_sem):
    d_in = pleft_ref.shape[0]
    n_y, _, cw = q_ref.shape
    p_copy = pltpu.make_async_copy(pt_ref, p_out, p_sem)
    fill = jnp.zeros((128 - 9 * RANK, cw), F32)

    def q_copy(c):
        cols = pl.ds(pl.multiple_of(c * cw, cw), cw)
        return pltpu.make_async_copy(q_ref.at[c], q_out.at[:, cols], q_sem)

    def e_copy(c):
        cols = pl.ds(pl.multiple_of(c * cw, cw), cw)
        return pltpu.make_async_copy(stage.at[:, cols], e_out.at[0, :, cols], e_sem)

    @pl.loop(0, n_y)
    def _(c):
        cols = pl.ds(pl.multiple_of(c * cw, cw), cw)
        three = [x.astype(F32) for x in split3(q_ref[c])]
        qc = jnp.concatenate(three * 3 + [fill], axis=0).astype(BF16)
        for r in range(d_in // RB):
            rows = pl.ds(r * RB, RB)
            m = jnp.concatenate([m_ref[c * (cw // 128) + h, rows, :] for h in range(cw // 128)], axis=1)
            stage[rows, cols] = m - mm(pleft_ref[rows, :], qc)
        e_copy(c).start()

    p_copy.start()

    @pl.loop(0, n_y)
    def _(c):
        q_copy(c).start()

    p_copy.wait()
    pltpu.make_async_copy(q_ref, q_ref, q_sem).wait()
    pltpu.make_async_copy(stage, e_out.at[0], e_sem).wait()


def solution(mesh):
    n = mesh.shape["data"]

    def per_device(act_in, pre_act, grad_out, q_init, err_mem):
        tokens, d_in = act_in.shape
        d_out = pre_act.shape[1]
        nc, n_p, n_y = d_out // CB, d_in // 128, n // 2
        cw = d_out // n_y
        hbm = pl.BlockSpec(memory_space=pltpu.HBM)
        vmem = pl.BlockSpec(memory_space=pltpu.VMEM)
        pleft, pt, q, m = pl.pallas_call(
            functools.partial(reduce_kernel, n),
            out_shape=(
                pltpu.VMEM((d_in, 128), BF16),
                pltpu.VMEM((RANK, d_in), F32),
                pltpu.VMEM((n_y, RANK, cw), F32),
                pltpu.VMEM((d_out // 128, d_in, 128), F32),
            ),
            in_specs=[hbm] * 5,
            out_specs=(vmem,) * 4,
            scratch_shapes=[
                pltpu.VMEM((d_out // 128, 3 * d_in, 128), BF16),
                pltpu.VMEM((d_out // 128, tokens, 128), BF16),
                pltpu.VMEM((d_out // 128, tokens, 128), BF16),
                pltpu.VMEM((d_out // 128, tokens, 128), BF16),
                pltpu.VMEM((tokens, d_in), BF16),
                pltpu.VMEM((d_in, tokens), BF16),
                pltpu.VMEM((RANK, d_out), F32),
                pltpu.VMEM((32, d_out), BF16),
                pltpu.VMEM((32, d_in), F32),
                pltpu.VMEM((32, tokens), F32),
                pltpu.VMEM((n_p, RANK, 128), F32),
                pltpu.VMEM((n - 1, RANK, 128), F32),
                pltpu.VMEM((n_p, RANK, 128), F32),
                pltpu.VMEM((n_y, RANK, cw), F32),
                pltpu.VMEM((n_y // 2, RANK, cw), F32),
                pltpu.VMEM((n // 2 - 1, RANK, cw), F32),
                pltpu.SemaphoreType.DMA((nc,)),
            ] + [pltpu.SemaphoreType.DMA] * 7 + [pltpu.SemaphoreType.DMA((n_y // 2,))]
            + [pltpu.SemaphoreType.DMA] * 4,
            compiler_params=pltpu.CompilerParams(
                collective_id=0, has_side_effects=True, vmem_limit_bytes=46 * 1024 * 1024),
            name="reduce_kernel",
        )(act_in, pre_act, grad_out, q_init.T, err_mem)
        p_t, q_t, err_new = pl.pallas_call(
            apply_kernel,
            out_shape=(
                jax.ShapeDtypeStruct((RANK, d_in), F32),
                jax.ShapeDtypeStruct((RANK, d_out), F32),
                jax.ShapeDtypeStruct((1, d_in, d_out), F32),
            ),
            in_specs=[vmem] * 4,
            out_specs=(hbm,) * 3,
            scratch_shapes=[
                pltpu.VMEM((d_in, d_out), F32),
            ] + [pltpu.SemaphoreType.DMA] * 3,
            compiler_params=pltpu.CompilerParams(vmem_limit_bytes=24 * 1024 * 1024),
            name="apply_kernel",
        )(pleft, pt, q, m)
        return p_t.T, q_t.T, err_new

    return jax.shard_map(
        per_device, mesh=mesh,
        in_specs=(P("data", None), P("data", None), P("data", None), P(None, None), P("data", None, None)),
        out_specs=(P(None, None), P(None, None), P("data", None, None)), check_vma=False)
```

```python
import functools

import jax
import jax.numpy as jnp
from jax import lax
from jax.experimental import pallas as pl
from jax.experimental.pallas import tpu as pltpu
from jax.sharding import PartitionSpec as P

F32 = jnp.float32
BF16 = jnp.bfloat16
MESH = pl.DeviceIdType.MESH
RANK = 8
CB = 256
RB = 256
NT = (((1,), (1,)), ((), ()))


def split3(x):
    hi = x.astype(BF16)
    rest = x - hi.astype(F32)
    mid = rest.astype(BF16)
    low = (rest - mid.astype(F32)).astype(BF16)
    return hi, mid, low


def stack3(x):
    parts = [p.astype(F32) for p in split3(x)]
    return jnp.concatenate(parts + [jnp.zeros_like(x)], axis=0).astype(BF16)


def fold3(y):
    return (y[16:24] + y[8:16]) + y[0:8]


def mm(a, b):
    return jnp.dot(a, b, preferred_element_type=F32)


def mm_nt(a, b):
    return lax.dot_general(a, b, NT, preferred_element_type=F32)


def gelu_grad(z, dy):
    c = 0.7978845608028654
    x = z.astype(F32)
    x2 = x * x
    t = jnp.tanh(x * (x2 * (c * 0.044715) + c))
    up = 1.0 + t
    slope = ((x * up) * (1.0 - t)) * (x2 * (1.5 * c * 0.044715) + 0.5 * c)
    return (0.5 * up + slope) * dy.astype(F32)


def orthonormalize(p):
    row = lax.broadcasted_iota(jnp.int32, (RANK, 1), 0)
    w = p
    norm2 = jnp.zeros((RANK, 1), F32)
    for j in range(RANK):
        v = w[j:j + 1]
        d = jnp.sum(jnp.where(row > j, p, w) * v, axis=1, keepdims=True)
        norm2 = jnp.where(row == j, d, norm2)
        if j + 1 < RANK:
            coef = jnp.where(row > j, d / d[j:j + 1], 0.0)
            w = w - coef * v
    return w / jnp.sqrt(norm2)


def far_first():
    places = [(i, fy, fx, fc) for i in range(4) for fy in range(2) for fx in range(2) for fc in range(2)]
    places.remove((3, 0, 0, 0))
    return sorted(places, key=lambda p: -((2, 1, 1, 0)[p[0]] + p[1] + p[2]))


def reduce_kernel(n, a_hbm, z_hbm, dy_hbm, qt_hbm, e_hbm, pleft_ref, pt_ref, q_ref, m_ref,
                  parts, g, z_v, dy_v, a_v, at_v, qt_v, qs, p_acc, h_acc, p_own, p_recv, p_all,
                  y_mate, y_own, y_recv,
                  in_sem, q_sem, a_sem, ps_sem, pr_sem, pbs_sem, pbr_sem,
                  ms_sem, mr_sem, ys_sem, yr_sem, ybs_sem, ybr_sem):
    me = lax.axis_index("data")
    d_in, d_out = m_ref.shape
    tokens = z_v.shape[0]
    n_p = d_in // 128
    n_half = y_own.shape[0]
    cw = d_out // (2 * n_half)
    core = lax.rem(me, 2)
    fx = lax.rem(lax.div(me, 2), 2)
    fy = lax.rem(lax.div(me, 4), 2)
    fz = lax.div(me, 8)
    central = (fz >= 1) & (fz <= 2)
    mine = jnp.minimum(jnp.maximum(fz - 1, 0), 1) + 2 * (fx + 2 * fy)

    def owner_chip(s):
        return 4 * (1 + lax.rem(s, 2)) + lax.div(s, 2)

    barrier = pltpu.get_barrier_semaphore()

    def e_copy(c):
        cols = pl.ds(pl.multiple_of(c * CB, CB), CB)
        return pltpu.make_async_copy(e_hbm.at[0, :, cols], m_ref.at[:, cols], in_sem.at[c])

    def z_copy(c):
        cols = pl.ds(pl.multiple_of(c * CB, CB), CB)
        return pltpu.make_async_copy(z_hbm.at[:, cols], z_v.at[:, cols], in_sem.at[c])

    def dy_copy(c):
        cols = pl.ds(pl.multiple_of(c * CB, CB), CB)
        return pltpu.make_async_copy(dy_hbm.at[:, cols], dy_v.at[:, cols], in_sem.at[c])

    nc = d_out // CB
    q_copy = pltpu.make_async_copy(qt_hbm, qt_v, q_sem)
    a_copy = pltpu.make_async_copy(a_hbm, a_v, a_sem)
    q_copy.start()

    @pl.loop(0, nc)
    def _(c):
        z_copy(c).start()
        dy_copy(c).start()
        e_copy(c).start()

        @pl.when(c == nc // 2)
        def _():
            a_copy.start()

    @pl.loop(1, n)
    def _(k):
        pl.semaphore_signal(barrier, inc=1, device_id=(lax.rem(me + k, n),), device_id_type=MESH)

    p_acc[...] = jnp.zeros_like(p_acc)
    h_acc[...] = jnp.zeros_like(h_acc)
    q_copy.wait()
    qt = qt_v[...]
    q_max = jnp.max(jnp.abs(qt), axis=1, keepdims=True)
    qs[...] = stack3((qt / q_max) * (1.0 / d_out))

    def arrive(c):
        whole = parts.at[pl.ds(2 * c, 2), pl.ds(0, 2 * (d_in + tokens))]
        pltpu.make_async_copy(whole, whole, in_sem.at[c]).wait()

    def stream(first, count):
        for i in range(count):
            arrive(first + i)
        for i in range(count):
            c = first + i
            cols = pl.ds(pl.multiple_of(c * CB, CB), CB)
            qc = qs[:, cols]
            for r in range(d_in // RB):
                rows = pl.ds(r * RB, RB)
                e1, e2, e3 = split3(m_ref[rows, cols])
                p_acc[:, rows] += (mm_nt(qc, e3) + mm_nt(qc, e2)) + mm_nt(qc, e1)
                if r % 2 == 1 and r // 2 < tokens // RB:
                    rows = pl.ds(r // 2 * RB, RB)
                    gb = gelu_grad(z_v[rows, cols], dy_v[rows, cols]).astype(BF16)
                    for h in range(CB // 128):
                        g[2 * c + h, rows, :] = gb[:, h * 128:(h + 1) * 128]
                    h_acc[:, rows] += mm_nt(qc, gb)

    stream(0, 1)

    @pl.loop(0, (nc - 2) // 2)
    def _(s):
        stream(1 + 2 * s, 2)

    stream(nc - 1, 1)

    a_copy.wait()
    hs = stack3(fold3(h_acc[...]))
    pt = (fold3(p_acc[...]) + fold3(mm(hs, a_v[...])) * (1.0 / tokens)) * q_max * float(d_out)
    for b in range(n_p):
        p_own[b] = pt[:, b * 128:(b + 1) * 128]

    pl.semaphore_wait(barrier, n - 1)

    def remote(src, dst, send_sem, recv_sem, device):
        return pltpu.make_async_remote_copy(
            src_ref=src, dst_ref=dst, send_sem=send_sem, recv_sem=recv_sem, device_id=(device,), device_id_type=MESH)

    def bulk(ref, send_sem, recv_sem):
        return remote(ref, ref, send_sem, recv_sem, me)

    def broadcast(buf, index, send_sem, recv_sem, first=0):
        for there in range(first):
            remote(buf.at[index], buf.at[index], send_sem, recv_sem, there).start()
        for plane, gy, gx, gc in far_first():
            there = (3, 0, 2, 1)[plane]
            z = there * (2 - fz) + (3 - there) * (fz - 1)
            y = 1 - fy if gy else fy
            x = 1 - fx if gx else fx
            c = 1 - core if gc else core
            there = z * 8 + y * 4 + x * 2 + c

            @pl.when(there >= first)
            def _():
                remote(buf.at[index], buf.at[index], send_sem, recv_sem, there).start()

    p_owner = central & (core == 1)

    @pl.loop(0, n_p)
    def _(b):
        owner = 2 * owner_chip(b) + 1

        @pl.when(me != owner)
        def _():
            remote(p_own.at[b], p_recv.at[lax.rem(me - owner + 2 * n - 1, n)], ps_sem, pr_sem, owner).start()

    @pl.loop(0, d_in // RB)
    def _(r):
        rows = pl.ds(pl.multiple_of(r * RB, RB), RB)
        at_v[rows, :] = a_v[:, rows].T

    def build(c):
        cols = pl.ds(pl.multiple_of(c * CB, CB), CB)
        gc = jnp.concatenate([g[2 * c + h] for h in range(CB // 128)], axis=1)
        for r in range(d_in // RB):
            rows = pl.ds(r * RB, RB)
            m = mm(at_v[rows, :], gc) * (1.0 / tokens) + m_ref[rows, cols]
            m_ref[rows, cols] = m
            for i, part in enumerate(split3(m)):
                for h in range(CB // 128):
                    parts[2 * c + h, pl.ds(i * d_in + r * RB, RB), :] = part[:, h * 128:(h + 1) * 128]

    pl.loop(0, nc // 2 + 1)(build)

    @pl.when(p_owner)
    def _():
        bulk(p_recv, ps_sem, pr_sem).wait_recv()
        p_all[mine] = p_own[mine] + jnp.sum(p_recv[...], axis=0)
        broadcast(p_all, mine, pbs_sem, pbr_sem)

    pl.loop(nc // 2 + 1, nc)(build)

    @pl.when(p_owner)
    def _():
        bulk(p_all.at[pl.ds(0, n_p - 1)], pbs_sem, pbr_sem).wait_recv()

    @pl.when(jnp.logical_not(p_owner))
    def _():
        bulk(p_all, pbs_sem, pbr_sem).wait_recv()

    p = orthonormalize(jnp.concatenate([p_all[b] for b in range(n_p)], axis=1))
    pt_ref[...] = p
    ps = stack3(p)

    def y_tile(t):
        def part(i):
            return jnp.concatenate(
                [parts[t * (cw // 128) + h, pl.ds(i * d_in, d_in), :] for h in range(cw // 128)], axis=1)
        y = mm(ps, part(2)) + mm(ps, part(1))
        return fold3(y + mm(ps, part(0)))

    mate = me + 1 - 2 * core

    @pl.loop(0, n_half // 2)
    def _(k):
        for i in range(2):
            s = 2 * k + i
            y_mate[s] = y_tile((1 - core) * n_half + s)
        for i in range(2):
            s = 2 * k + i
            remote(y_mate.at[s], y_mate.at[n_half + s], ms_sem, mr_sem.at[s], mate).start()

    @pl.loop(0, n_half // 2)
    def _(k):
        for i in range(2):
            s = 2 * k + i
            bulk(y_mate.at[n_half + s], ms_sem, mr_sem.at[s]).wait_recv()
        for i in range(2):
            s = 2 * k + i
            y_own[s] = y_tile(core * n_half + s) + y_mate[n_half + s]
        for i in range(2):
            s = 2 * k + i
            chip = owner_chip(s)
            slot = lax.rem(lax.div(me, 2) - chip + n - 1, n // 2)

            @pl.when(me != 2 * chip + core)
            def _():
                remote(y_own.at[s], y_recv.at[slot], ys_sem, yr_sem, 2 * chip + core).start()

    p1, p2, p3 = [x.astype(F32) for x in split3(p)]
    fill = jnp.zeros((128 - 9 * RANK, d_in), F32)
    pleft_ref[...] = jnp.concatenate([p1] * 3 + [p2] * 3 + [p3] * 3 + [fill], axis=0).T.astype(BF16)
    q_mine = core * n_half + mine

    @pl.when(central)
    def _():
        bulk(y_recv, ys_sem, yr_sem).wait_recv()
        q_ref[q_mine] = (y_own[mine] + jnp.sum(y_recv[...], axis=0)) * (1.0 / n)
        broadcast(q_ref, q_mine, ybs_sem, ybr_sem, first=2)

    bulk(y_mate.at[pl.ds(0, n_half)], ms_sem, yr_sem).wait_send()

    @pl.when(p_owner)
    def _():
        bulk(p_own.at[pl.ds(0, n_p - 1)], ps_sem, pr_sem).wait_send()
        bulk(p_recv, pbs_sem, pr_sem).wait_send()

    @pl.when(jnp.logical_not(p_owner))
    def _():
        bulk(p_own, ps_sem, pr_sem).wait_send()

    @pl.when(central)
    def _():
        bulk(y_own.at[pl.ds(0, n_half - 1)], ys_sem, yr_sem).wait_send()
        bulk(q_ref.at[pl.ds(0, 2 * n_half - 1)], ybs_sem, ybr_sem).wait_recv()
        bulk(parts.at[0, pl.ds(0, (n - 1) * RANK * cw // 64)], ybs_sem, yr_sem).wait_send()

    @pl.when(jnp.logical_not(central))
    def _():
        bulk(y_own, ys_sem, yr_sem).wait_send()
        bulk(q_ref, ybs_sem, ybr_sem).wait_recv()


def apply_kernel(pleft_ref, pt_ref, q_ref, m_ref, p_out, q_out, e_out, stage, p_sem, q_sem, e_sem):
    d_in, d_out = m_ref.shape
    n_y, _, cw = q_ref.shape
    p_copy = pltpu.make_async_copy(pt_ref, p_out, p_sem)
    fill = jnp.zeros((128 - 9 * RANK, cw), F32)

    def q_copy(c):
        cols = pl.ds(pl.multiple_of(c * cw, cw), cw)
        return pltpu.make_async_copy(q_ref.at[c], q_out.at[:, cols], q_sem)

    def e_copy(c):
        cols = pl.ds(pl.multiple_of(c * cw, cw), cw)
        return pltpu.make_async_copy(stage.at[:, cols], e_out.at[0, :, cols], e_sem)

    @pl.loop(0, n_y)
    def _(c):
        cols = pl.ds(pl.multiple_of(c * cw, cw), cw)
        three = [x.astype(F32) for x in split3(q_ref[c])]
        qc = jnp.concatenate(three * 3 + [fill], axis=0).astype(BF16)
        for r in range(d_in // RB):
            rows = pl.ds(r * RB, RB)
            stage[rows, cols] = m_ref[rows, cols] - mm(pleft_ref[rows, :], qc)
        e_copy(c).start()

    p_copy.start()

    @pl.loop(0, n_y)
    def _(c):
        q_copy(c).start()

    p_copy.wait()
    pltpu.make_async_copy(q_ref, q_ref, q_sem).wait()
    pltpu.make_async_copy(stage, e_out.at[0], e_sem).wait()


def solution(mesh):
    n = mesh.shape["data"]

    def per_device(act_in, pre_act, grad_out, q_init, err_mem):
        tokens, d_in = act_in.shape
        d_out = pre_act.shape[1]
        nc, n_p, n_y = d_out // CB, d_in // 128, n // 2
        cw = d_out // n_y
        hbm = pl.BlockSpec(memory_space=pltpu.HBM)
        vmem = pl.BlockSpec(memory_space=pltpu.VMEM)
        pleft, pt, q, m = pl.pallas_call(
            functools.partial(reduce_kernel, n),
            out_shape=(
                pltpu.VMEM((d_in, 128), BF16),
                pltpu.VMEM((RANK, d_in), F32),
                pltpu.VMEM((n_y, RANK, cw), F32),
                pltpu.VMEM((d_in, d_out), F32),
            ),
            in_specs=[hbm] * 5,
            out_specs=(vmem,) * 4,
            scratch_shapes=[
                pltpu.VMEM((d_out // 128, 3 * d_in, 128), BF16),
                pltpu.VMEM((d_out // 128, tokens, 128), BF16),
                pltpu.VMEM((tokens, d_out), BF16),
                pltpu.VMEM((tokens, d_out), BF16),
                pltpu.VMEM((tokens, d_in), BF16),
                pltpu.VMEM((d_in, tokens), BF16),
                pltpu.VMEM((RANK, d_out), F32),
                pltpu.VMEM((32, d_out), BF16),
                pltpu.VMEM((32, d_in), F32),
                pltpu.VMEM((32, tokens), F32),
                pltpu.VMEM((n_p, RANK, 128), F32),
                pltpu.VMEM((n - 1, RANK, 128), F32),
                pltpu.VMEM((n_p, RANK, 128), F32),
                pltpu.VMEM((n_y, RANK, cw), F32),
                pltpu.VMEM((n_y // 2, RANK, cw), F32),
                pltpu.VMEM((n // 2 - 1, RANK, cw), F32),
                pltpu.SemaphoreType.DMA((nc,)),
            ] + [pltpu.SemaphoreType.DMA] * 7 + [pltpu.SemaphoreType.DMA((n_y // 2,))]
            + [pltpu.SemaphoreType.DMA] * 4,
            compiler_params=pltpu.CompilerParams(
                collective_id=0, has_side_effects=True, vmem_limit_bytes=46 * 1024 * 1024),
            name="reduce_kernel",
        )(act_in, pre_act, grad_out, q_init.T, err_mem)
        p_t, q_t, err_new = pl.pallas_call(
            apply_kernel,
            out_shape=(
                jax.ShapeDtypeStruct((RANK, d_in), F32),
                jax.ShapeDtypeStruct((RANK, d_out), F32),
                jax.ShapeDtypeStruct((1, d_in, d_out), F32),
            ),
            in_specs=[vmem] * 4,
            out_specs=(hbm,) * 3,
            scratch_shapes=[
                pltpu.VMEM((d_in, d_out), F32),
            ] + [pltpu.SemaphoreType.DMA] * 3,
            compiler_params=pltpu.CompilerParams(vmem_limit_bytes=24 * 1024 * 1024),
            name="apply_kernel",
        )(pleft, pt, q, m)
        return p_t.T, q_t.T, err_new

    return jax.shard_map(
        per_device, mesh=mesh,
        in_specs=(P("data", None), P("data", None), P("data", None), P(None, None), P("data", None, None)),
        out_specs=(P(None, None), P(None, None), P("data", None, None)), check_vma=False)
```

```python
import functools

import jax
import jax.numpy as jnp
from jax import lax
from jax.experimental import pallas as pl
from jax.experimental.pallas import tpu as pltpu
from jax.sharding import PartitionSpec as P

F32 = jnp.float32
BF16 = jnp.bfloat16
MESH = pl.DeviceIdType.MESH
RANK = 8
CB = 256
RB = 256
NT = (((1,), (1,)), ((), ()))


def split3(x):
    hi = x.astype(BF16)
    rest = x - hi.astype(F32)
    mid = rest.astype(BF16)
    low = (rest - mid.astype(F32)).astype(BF16)
    return hi, mid, low


def stack3(x):
    parts = [p.astype(F32) for p in split3(x)]
    return jnp.concatenate(parts + [jnp.zeros_like(x)], axis=0).astype(BF16)


def fold3(y):
    return (y[16:24] + y[8:16]) + y[0:8]


def mm(a, b):
    return jnp.dot(a, b, preferred_element_type=F32)


def mm_nt(a, b):
    return lax.dot_general(a, b, NT, preferred_element_type=F32)


def gelu_grad(z, dy):
    c = 0.7978845608028654
    x = z.astype(F32)
    x2 = x * x
    t = jnp.tanh(x * (x2 * (c * 0.044715) + c))
    up = 1.0 + t
    slope = ((x * up) * (1.0 - t)) * (x2 * (1.5 * c * 0.044715) + 0.5 * c)
    return (0.5 * up + slope) * dy.astype(F32)


def orthonormalize(p):
    row = lax.broadcasted_iota(jnp.int32, (RANK, 1), 0)
    w = p
    norm2 = jnp.zeros((RANK, 1), F32)
    for j in range(RANK):
        v = w[j:j + 1]
        d = jnp.sum(jnp.where(row > j, p, w) * v, axis=1, keepdims=True)
        norm2 = jnp.where(row == j, d, norm2)
        if j + 1 < RANK:
            coef = jnp.where(row > j, d / d[j:j + 1], 0.0)
            w = w - coef * v
    return w / jnp.sqrt(norm2)


def far_first():
    places = [(i, fy, fx, fc) for i in range(4) for fy in range(2) for fx in range(2) for fc in range(2)]
    places.remove((3, 0, 0, 0))
    return sorted(places, key=lambda p: -((2, 1, 1, 0)[p[0]] + p[1] + p[2]))


def reduce_kernel(n, a_hbm, z_hbm, dy_hbm, qt_hbm, e_hbm, pleft_ref, pt_ref, q_ref, m_ref,
                  parts, g, z_v, dy_v, a_v, at_v, qt_v, qs, p_acc, h_acc, p_own, p_recv, p_all,
                  y_mate, y_own, y_recv,
                  in_sem, q_sem, a_sem, ps_sem, pr_sem, pbs_sem, pbr_sem,
                  ms_sem, mr_sem, ys_sem, yr_sem, ybs_sem, ybr_sem):
    me = lax.axis_index("data")
    d_in, d_out = m_ref.shape
    tokens = z_v.shape[0]
    n_p = d_in // 128
    n_half = y_own.shape[0]
    cw = d_out // (2 * n_half)
    core = lax.rem(me, 2)
    fx = lax.rem(lax.div(me, 2), 2)
    fy = lax.rem(lax.div(me, 4), 2)
    fz = lax.div(me, 8)
    central = (fz >= 1) & (fz <= 2)
    mine = jnp.minimum(jnp.maximum(fz - 1, 0), 1) + 2 * (fx + 2 * fy)

    def owner_chip(s):
        return 4 * (1 + lax.rem(s, 2)) + lax.div(s, 2)

    y_mine = jnp.minimum(jnp.maximum(2 - fz, 0), 1) + 2 * (3 - fx - 2 * fy)

    def y_chip(s):
        return 4 * (2 - lax.rem(s, 2)) + 3 - lax.div(s, 2)

    barrier = pltpu.get_barrier_semaphore()

    def e_copy(c):
        cols = pl.ds(pl.multiple_of(c * CB, CB), CB)
        return pltpu.make_async_copy(e_hbm.at[0, :, cols], m_ref.at[:, cols], in_sem.at[c])

    def z_copy(c):
        cols = pl.ds(pl.multiple_of(c * CB, CB), CB)
        return pltpu.make_async_copy(z_hbm.at[:, cols], z_v.at[:, cols], in_sem.at[c])

    def dy_copy(c):
        cols = pl.ds(pl.multiple_of(c * CB, CB), CB)
        return pltpu.make_async_copy(dy_hbm.at[:, cols], dy_v.at[:, cols], in_sem.at[c])

    nc = d_out // CB
    q_copy = pltpu.make_async_copy(qt_hbm, qt_v, q_sem)
    a_copy = pltpu.make_async_copy(a_hbm, a_v, a_sem)
    q_copy.start()

    @pl.loop(0, nc)
    def _(c):
        z_copy(c).start()
        dy_copy(c).start()
        e_copy(c).start()

        @pl.when(c == nc // 2)
        def _():
            a_copy.start()

    @pl.loop(1, n)
    def _(k):
        pl.semaphore_signal(barrier, inc=1, device_id=(lax.rem(me + k, n),), device_id_type=MESH)

    p_acc[...] = jnp.zeros_like(p_acc)
    h_acc[...] = jnp.zeros_like(h_acc)
    q_copy.wait()
    qt = qt_v[...]
    q_max = jnp.max(jnp.abs(qt), axis=1, keepdims=True)
    qs[...] = stack3((qt / q_max) * (1.0 / d_out))

    def arrive(c):
        whole = parts.at[pl.ds(2 * c, 2), pl.ds(0, 2 * (d_in + tokens))]
        pltpu.make_async_copy(whole, whole, in_sem.at[c]).wait()

    def stream(first, count):
        for i in range(count):
            arrive(first + i)
        for i in range(count):
            c = first + i
            cols = pl.ds(pl.multiple_of(c * CB, CB), CB)
            qc = qs[:, cols]
            for r in range(d_in // RB):
                rows = pl.ds(r * RB, RB)
                e1, e2, e3 = split3(m_ref[rows, cols])
                p_acc[:, rows] += (mm_nt(qc, e3) + mm_nt(qc, e2)) + mm_nt(qc, e1)
                if r % 2 == 1 and r // 2 < tokens // RB:
                    rows = pl.ds(r // 2 * RB, RB)
                    gb = gelu_grad(z_v[rows, cols], dy_v[rows, cols]).astype(BF16)
                    for h in range(CB // 128):
                        g[2 * c + h, rows, :] = gb[:, h * 128:(h + 1) * 128]
                    h_acc[:, rows] += mm_nt(qc, gb)

    stream(0, 1)

    @pl.loop(0, (nc - 2) // 2)
    def _(s):
        stream(1 + 2 * s, 2)

    stream(nc - 1, 1)

    a_copy.wait()
    hs = stack3(fold3(h_acc[...]))
    pt = (fold3(p_acc[...]) + fold3(mm(hs, a_v[...])) * (1.0 / tokens)) * q_max * float(d_out)
    for b in range(n_p):
        p_own[b] = pt[:, b * 128:(b + 1) * 128]

    pl.semaphore_wait(barrier, n - 1)

    def remote(src, dst, send_sem, recv_sem, device):
        return pltpu.make_async_remote_copy(
            src_ref=src, dst_ref=dst, send_sem=send_sem, recv_sem=recv_sem, device_id=(device,), device_id_type=MESH)

    def bulk(ref, send_sem, recv_sem):
        return remote(ref, ref, send_sem, recv_sem, me)

    def broadcast(buf, index, send_sem, recv_sem, first=0):
        for there in range(first):
            remote(buf.at[index], buf.at[index], send_sem, recv_sem, there).start()
        for plane, gy, gx, gc in far_first():
            there = (3, 0, 2, 1)[plane]
            z = there * (2 - fz) + (3 - there) * (fz - 1)
            y = 1 - fy if gy else fy
            x = 1 - fx if gx else fx
            c = 1 - core if gc else core
            there = z * 8 + y * 4 + x * 2 + c

            @pl.when(there >= first)
            def _():
                remote(buf.at[index], buf.at[index], send_sem, recv_sem, there).start()

    p_owner = central & (core == 1)

    @pl.loop(0, n_p)
    def _(b):
        owner = 2 * owner_chip(b) + 1

        @pl.when(me != owner)
        def _():
            remote(p_own.at[b], p_recv.at[lax.rem(me - owner + 2 * n - 1, n)], ps_sem, pr_sem, owner).start()

    @pl.loop(0, d_in // RB)
    def _(r):
        rows = pl.ds(pl.multiple_of(r * RB, RB), RB)
        at_v[rows, :] = a_v[:, rows].T

    def build(c):
        cols = pl.ds(pl.multiple_of(c * CB, CB), CB)
        gc = jnp.concatenate([g[2 * c + h] for h in range(CB // 128)], axis=1)
        for r in range(d_in // RB):
            rows = pl.ds(r * RB, RB)
            m = mm(at_v[rows, :], gc) * (1.0 / tokens) + m_ref[rows, cols]
            m_ref[rows, cols] = m
            for i, part in enumerate(split3(m)):
                for h in range(CB // 128):
                    parts[2 * c + h, pl.ds(i * d_in + r * RB, RB), :] = part[:, h * 128:(h + 1) * 128]

    pl.loop(0, nc // 2 + 1)(build)

    @pl.when(p_owner)
    def _():
        bulk(p_recv, ps_sem, pr_sem).wait_recv()
        p_all[mine] = p_own[mine] + jnp.sum(p_recv[...], axis=0)
        broadcast(p_all, mine, pbs_sem, pbr_sem)

    pl.loop(nc // 2 + 1, nc)(build)

    @pl.when(p_owner)
    def _():
        bulk(p_all.at[pl.ds(0, n_p - 1)], pbs_sem, pbr_sem).wait_recv()

    @pl.when(jnp.logical_not(p_owner))
    def _():
        bulk(p_all, pbs_sem, pbr_sem).wait_recv()

    p = orthonormalize(jnp.concatenate([p_all[b] for b in range(n_p)], axis=1))
    pt_ref[...] = p
    ps = stack3(p)

    def y_tile(t):
        def part(i):
            return jnp.concatenate(
                [parts[t * (cw // 128) + h, pl.ds(i * d_in, d_in), :] for h in range(cw // 128)], axis=1)
        y = mm(ps, part(2)) + mm(ps, part(1))
        return fold3(y + mm(ps, part(0)))

    mate = me + 1 - 2 * core

    @pl.loop(0, n_half // 2)
    def _(k):
        for i in range(2):
            s = 2 * k + i
            y_mate[s] = y_tile((1 - core) * n_half + s)
        for i in range(2):
            s = 2 * k + i
            remote(y_mate.at[s], y_mate.at[n_half + s], ms_sem, mr_sem.at[s], mate).start()

    @pl.loop(0, n_half // 2)
    def _(k):
        for i in range(2):
            s = 2 * k + i
            bulk(y_mate.at[n_half + s], ms_sem, mr_sem.at[s]).wait_recv()
        for i in range(2):
            s = 2 * k + i
            y_own[s] = y_tile(core * n_half + s) + y_mate[n_half + s]
        for i in range(2):
            s = 2 * k + i
            chip = y_chip(s)
            slot = lax.rem(lax.div(me, 2) - chip + n - 1, n // 2)

            @pl.when(me != 2 * chip + core)
            def _():
                remote(y_own.at[s], y_recv.at[slot], ys_sem, yr_sem, 2 * chip + core).start()

    p1, p2, p3 = [x.astype(F32) for x in split3(p)]
    fill = jnp.zeros((128 - 9 * RANK, d_in), F32)
    pleft_ref[...] = jnp.concatenate([p1] * 3 + [p2] * 3 + [p3] * 3 + [fill], axis=0).T.astype(BF16)
    q_mine = core * n_half + y_mine

    @pl.when(central)
    def _():
        bulk(y_recv, ys_sem, yr_sem).wait_recv()
        q_ref[q_mine] = (y_own[y_mine] + jnp.sum(y_recv[...], axis=0)) * (1.0 / n)
        broadcast(q_ref, q_mine, ybs_sem, ybr_sem, first=2)

    bulk(y_mate.at[pl.ds(0, n_half)], ms_sem, yr_sem).wait_send()

    @pl.when(p_owner)
    def _():
        bulk(p_own.at[pl.ds(0, n_p - 1)], ps_sem, pr_sem).wait_send()
        bulk(p_recv, pbs_sem, pr_sem).wait_send()

    @pl.when(jnp.logical_not(p_owner))
    def _():
        bulk(p_own, ps_sem, pr_sem).wait_send()

    @pl.when(central)
    def _():
        bulk(y_own.at[pl.ds(0, n_half - 1)], ys_sem, yr_sem).wait_send()
        bulk(q_ref.at[pl.ds(0, 2 * n_half - 1)], ybs_sem, ybr_sem).wait_recv()
        bulk(parts.at[0, pl.ds(0, (n - 1) * RANK * cw // 64)], ybs_sem, yr_sem).wait_send()

    @pl.when(jnp.logical_not(central))
    def _():
        bulk(y_own, ys_sem, yr_sem).wait_send()
        bulk(q_ref, ybs_sem, ybr_sem).wait_recv()


def apply_kernel(pleft_ref, pt_ref, q_ref, m_ref, p_out, q_out, e_out, stage, p_sem, q_sem, e_sem):
    d_in, d_out = m_ref.shape
    n_y, _, cw = q_ref.shape
    p_copy = pltpu.make_async_copy(pt_ref, p_out, p_sem)
    fill = jnp.zeros((128 - 9 * RANK, cw), F32)

    def q_copy(c):
        cols = pl.ds(pl.multiple_of(c * cw, cw), cw)
        return pltpu.make_async_copy(q_ref.at[c], q_out.at[:, cols], q_sem)

    def e_copy(c):
        cols = pl.ds(pl.multiple_of(c * cw, cw), cw)
        return pltpu.make_async_copy(stage.at[:, cols], e_out.at[0, :, cols], e_sem)

    @pl.loop(0, n_y)
    def _(c):
        cols = pl.ds(pl.multiple_of(c * cw, cw), cw)
        three = [x.astype(F32) for x in split3(q_ref[c])]
        qc = jnp.concatenate(three * 3 + [fill], axis=0).astype(BF16)
        for r in range(d_in // RB):
            rows = pl.ds(r * RB, RB)
            stage[rows, cols] = m_ref[rows, cols] - mm(pleft_ref[rows, :], qc)
        e_copy(c).start()

    p_copy.start()

    @pl.loop(0, n_y)
    def _(c):
        q_copy(c).start()

    p_copy.wait()
    pltpu.make_async_copy(q_ref, q_ref, q_sem).wait()
    pltpu.make_async_copy(stage, e_out.at[0], e_sem).wait()


def solution(mesh):
    n = mesh.shape["data"]

    def per_device(act_in, pre_act, grad_out, q_init, err_mem):
        tokens, d_in = act_in.shape
        d_out = pre_act.shape[1]
        nc, n_p, n_y = d_out // CB, d_in // 128, n // 2
        cw = d_out // n_y
        hbm = pl.BlockSpec(memory_space=pltpu.HBM)
        vmem = pl.BlockSpec(memory_space=pltpu.VMEM)
        pleft, pt, q, m = pl.pallas_call(
            functools.partial(reduce_kernel, n),
            out_shape=(
                pltpu.VMEM((d_in, 128), BF16),
                pltpu.VMEM((RANK, d_in), F32),
                pltpu.VMEM((n_y, RANK, cw), F32),
                pltpu.VMEM((d_in, d_out), F32),
            ),
            in_specs=[hbm] * 5,
            out_specs=(vmem,) * 4,
            scratch_shapes=[
                pltpu.VMEM((d_out // 128, 3 * d_in, 128), BF16),
                pltpu.VMEM((d_out // 128, tokens, 128), BF16),
                pltpu.VMEM((tokens, d_out), BF16),
                pltpu.VMEM((tokens, d_out), BF16),
                pltpu.VMEM((tokens, d_in), BF16),
                pltpu.VMEM((d_in, tokens), BF16),
                pltpu.VMEM((RANK, d_out), F32),
                pltpu.VMEM((32, d_out), BF16),
                pltpu.VMEM((32, d_in), F32),
                pltpu.VMEM((32, tokens), F32),
                pltpu.VMEM((n_p, RANK, 128), F32),
                pltpu.VMEM((n - 1, RANK, 128), F32),
                pltpu.VMEM((n_p, RANK, 128), F32),
                pltpu.VMEM((n_y, RANK, cw), F32),
                pltpu.VMEM((n_y // 2, RANK, cw), F32),
                pltpu.VMEM((n // 2 - 1, RANK, cw), F32),
                pltpu.SemaphoreType.DMA((nc,)),
            ] + [pltpu.SemaphoreType.DMA] * 7 + [pltpu.SemaphoreType.DMA((n_y // 2,))]
            + [pltpu.SemaphoreType.DMA] * 4,
            compiler_params=pltpu.CompilerParams(
                collective_id=0, has_side_effects=True, vmem_limit_bytes=46 * 1024 * 1024),
            name="reduce_kernel",
        )(act_in, pre_act, grad_out, q_init.T, err_mem)
        p_t, q_t, err_new = pl.pallas_call(
            apply_kernel,
            out_shape=(
                jax.ShapeDtypeStruct((RANK, d_in), F32),
                jax.ShapeDtypeStruct((RANK, d_out), F32),
                jax.ShapeDtypeStruct((1, d_in, d_out), F32),
            ),
            in_specs=[vmem] * 4,
            out_specs=(hbm,) * 3,
            scratch_shapes=[
                pltpu.VMEM((d_in, d_out), F32),
            ] + [pltpu.SemaphoreType.DMA] * 3,
            compiler_params=pltpu.CompilerParams(vmem_limit_bytes=24 * 1024 * 1024),
            name="apply_kernel",
        )(pleft, pt, q, m)
        return p_t.T, q_t.T, err_new

    return jax.shard_map(
        per_device, mesh=mesh,
        in_specs=(P("data", None), P("data", None), P("data", None), P(None, None), P("data", None, None)),
        out_specs=(P(None, None), P(None, None), P("data", None, None)), check_vma=False)
```

```python
import functools

import jax
import jax.numpy as jnp
from jax import lax
from jax.experimental import pallas as pl
from jax.experimental.pallas import tpu as pltpu
from jax.sharding import PartitionSpec as P

F32 = jnp.float32
BF16 = jnp.bfloat16
MESH = pl.DeviceIdType.MESH
RANK = 8
CB = 256
RB = 256
NT = (((1,), (1,)), ((), ()))


def split3(x):
    hi = x.astype(BF16)
    rest = x - hi.astype(F32)
    mid = rest.astype(BF16)
    low = (rest - mid.astype(F32)).astype(BF16)
    return hi, mid, low


def stack3(x):
    parts = [p.astype(F32) for p in split3(x)]
    return jnp.concatenate(parts + [jnp.zeros_like(x)], axis=0).astype(BF16)


def fold3(y):
    return (y[16:24] + y[8:16]) + y[0:8]


def mm(a, b):
    return jnp.dot(a, b, preferred_element_type=F32)


def mm_nt(a, b):
    return lax.dot_general(a, b, NT, preferred_element_type=F32)


def gelu_grad(z, dy):
    c = 0.7978845608028654
    x = z.astype(F32)
    x2 = x * x
    t = jnp.tanh(x * (x2 * (c * 0.044715) + c))
    up = 1.0 + t
    slope = ((x * up) * (1.0 - t)) * (x2 * (1.5 * c * 0.044715) + 0.5 * c)
    return (0.5 * up + slope) * dy.astype(F32)


def orthonormalize(p):
    row = lax.broadcasted_iota(jnp.int32, (RANK, 1), 0)
    w = p
    norm2 = jnp.zeros((RANK, 1), F32)
    for j in range(RANK):
        v = w[j:j + 1]
        d = jnp.sum(jnp.where(row > j, p, w) * v, axis=1, keepdims=True)
        norm2 = jnp.where(row == j, d, norm2)
        if j + 1 < RANK:
            coef = jnp.where(row > j, d / d[j:j + 1], 0.0)
            w = w - coef * v
    return w / jnp.sqrt(norm2)


def far_first(planes):
    places = [(i, fy, fx, fc) for i in range(4) for fy in range(2) for fx in range(2) for fc in range(2)]
    places.remove((3, 0, 0, 0))
    return sorted(places, key=lambda p: -(planes[p[0]] + p[1] + p[2]))


def reduce_kernel(n, a_hbm, z_hbm, dy_hbm, qt_hbm, e_hbm, pleft_ref, pt_ref, q_ref, m_ref,
                  parts, g, z_v, dy_v, a_v, at_v, qt_v, qs, p_acc, h_acc, p_own, p_recv, p_all,
                  y_mate, y_own, y_recv,
                  in_sem, q_sem, a_sem, ps_sem, pr_sem, pbs_sem, pbr_sem,
                  ms_sem, mr_sem, ys_sem, yr_sem, ybs_sem, ybr_sem):
    me = lax.axis_index("data")
    d_in, d_out = m_ref.shape
    tokens = z_v.shape[0]
    n_p = d_in // 128
    n_half = y_own.shape[0]
    cw = d_out // (2 * n_half)
    core = lax.rem(me, 2)
    fx = lax.rem(lax.div(me, 2), 2)
    fy = lax.rem(lax.div(me, 4), 2)
    fz = lax.div(me, 8)
    central = (fz >= 1) & (fz <= 2)
    mine = jnp.minimum(jnp.maximum(fz - 1, 0), 1) + 2 * (fx + 2 * fy)

    def owner_chip(s):
        return 4 * (1 + lax.rem(s, 2)) + lax.div(s, 2)

    barrier = pltpu.get_barrier_semaphore()

    def e_copy(c):
        cols = pl.ds(pl.multiple_of(c * CB, CB), CB)
        return pltpu.make_async_copy(e_hbm.at[0, :, cols], m_ref.at[:, cols], in_sem.at[c])

    def z_copy(c):
        cols = pl.ds(pl.multiple_of(c * CB, CB), CB)
        return pltpu.make_async_copy(z_hbm.at[:, cols], z_v.at[:, cols], in_sem.at[c])

    def dy_copy(c):
        cols = pl.ds(pl.multiple_of(c * CB, CB), CB)
        return pltpu.make_async_copy(dy_hbm.at[:, cols], dy_v.at[:, cols], in_sem.at[c])

    nc = d_out // CB
    q_copy = pltpu.make_async_copy(qt_hbm, qt_v, q_sem)
    a_copy = pltpu.make_async_copy(a_hbm, a_v, a_sem)
    q_copy.start()

    @pl.loop(0, nc)
    def _(c):
        z_copy(c).start()
        dy_copy(c).start()
        e_copy(c).start()

        @pl.when(c == nc // 2)
        def _():
            a_copy.start()

    @pl.loop(1, n)
    def _(k):
        pl.semaphore_signal(barrier, inc=1, device_id=(lax.rem(me + k, n),), device_id_type=MESH)

    p_acc[...] = jnp.zeros_like(p_acc)
    h_acc[...] = jnp.zeros_like(h_acc)
    q_copy.wait()
    qt = qt_v[...]
    q_max = jnp.max(jnp.abs(qt), axis=1, keepdims=True)
    qs[...] = stack3((qt / q_max) * (1.0 / d_out))

    def arrive(c):
        whole = parts.at[pl.ds(2 * c, 2), pl.ds(0, 2 * (d_in + tokens))]
        pltpu.make_async_copy(whole, whole, in_sem.at[c]).wait()

    def stream(first, count):
        for i in range(count):
            arrive(first + i)
        for i in range(count):
            c = first + i
            cols = pl.ds(pl.multiple_of(c * CB, CB), CB)
            qc = qs[:, cols]
            for r in range(d_in // RB):
                rows = pl.ds(r * RB, RB)
                e1, e2, e3 = split3(m_ref[rows, cols])
                p_acc[:, rows] += (mm_nt(qc, e3) + mm_nt(qc, e2)) + mm_nt(qc, e1)
                if r % 2 == 1 and r // 2 < tokens // RB:
                    rows = pl.ds(r // 2 * RB, RB)
                    gb = gelu_grad(z_v[rows, cols], dy_v[rows, cols]).astype(BF16)
                    for h in range(CB // 128):
                        g[2 * c + h, rows, :] = gb[:, h * 128:(h + 1) * 128]
                    h_acc[:, rows] += mm_nt(qc, gb)

    stream(0, 1)

    @pl.loop(0, (nc - 2) // 2)
    def _(s):
        stream(1 + 2 * s, 2)

    stream(nc - 1, 1)

    a_copy.wait()
    hs = stack3(fold3(h_acc[...]))
    pt = (fold3(p_acc[...]) + fold3(mm(hs, a_v[...])) * (1.0 / tokens)) * q_max * float(d_out)
    for b in range(n_p):
        p_own[b] = pt[:, b * 128:(b + 1) * 128]

    pl.semaphore_wait(barrier, n - 1)

    def remote(src, dst, send_sem, recv_sem, device):
        return pltpu.make_async_remote_copy(
            src_ref=src, dst_ref=dst, send_sem=send_sem, recv_sem=recv_sem, device_id=(device,), device_id_type=MESH)

    def bulk(ref, send_sem, recv_sem):
        return remote(ref, ref, send_sem, recv_sem, me)

    def broadcast(buf, index, send_sem, recv_sem, first=0):
        for there in range(first):
            remote(buf.at[index], buf.at[index], send_sem, recv_sem, there).start()
        for plane, gy, gx, gc in far_first((2, 1, 1, 0)):
            there = (3, 0, 2, 1)[plane]
            z = there * (2 - fz) + (3 - there) * (fz - 1)
            y = 1 - fy if gy else fy
            x = 1 - fx if gx else fx
            c = 1 - core if gc else core
            there = z * 8 + y * 4 + x * 2 + c

            @pl.when(there >= first)
            def _():
                remote(buf.at[index], buf.at[index], send_sem, recv_sem, there).start()

    here = lax.div(me, 2)
    last = n // 2 - 1
    p_owner = (here >= last - 2) | (here == last - 4)
    p_mine = 2 * jnp.minimum(last - here, n_p // 2 - 1) + core

    @pl.loop(0, n_p)
    def _(k):
        b = lax.rem(k + me, n_p)
        near = lax.div(b, 2)
        owner = 2 * (last - near - lax.div(near, 3)) + lax.rem(b, 2)

        @pl.when(me != owner)
        def _():
            remote(p_own.at[b], p_recv.at[lax.rem(me - owner + 2 * n - 1, n)], ps_sem, pr_sem, owner).start()

    @pl.loop(0, d_in // RB)
    def _(r):
        rows = pl.ds(pl.multiple_of(r * RB, RB), RB)
        at_v[rows, :] = a_v[:, rows].T

    def build(c):
        cols = pl.ds(pl.multiple_of(c * CB, CB), CB)
        gc = jnp.concatenate([g[2 * c + h] for h in range(CB // 128)], axis=1)
        for r in range(d_in // RB):
            rows = pl.ds(r * RB, RB)
            m = mm(at_v[rows, :], gc) * (1.0 / tokens) + m_ref[rows, cols]
            m_ref[rows, cols] = m
            for i, part in enumerate(split3(m)):
                for h in range(CB // 128):
                    parts[2 * c + h, pl.ds(i * d_in + r * RB, RB), :] = part[:, h * 128:(h + 1) * 128]

    early = jnp.where(here == last, 3, 6)
    pl.loop(0, early)(build)

    @pl.when(p_owner)
    def _():
        bulk(p_recv, ps_sem, pr_sem).wait_recv()
        p_all[p_mine] = p_own[p_mine] + jnp.sum(p_recv[...], axis=0)
        tile = p_all.at[p_mine]
        for plane, gy, gx, gc in far_first((3, 2, 1, 0)):
            z = (0, 1, 5 - fz, fz)[plane]
            y = 1 - fy if gy else fy
            x = 1 - fx if gx else fx
            c = 1 - core if gc else core
            remote(tile, tile, pbs_sem, pbr_sem, z * 8 + y * 4 + x * 2 + c).start()

    pl.loop(early, nc)(build)

    @pl.when(p_owner)
    def _():
        bulk(p_all.at[pl.ds(0, n_p - 1)], pbs_sem, pbr_sem).wait_recv()

    @pl.when(jnp.logical_not(p_owner))
    def _():
        bulk(p_all, pbs_sem, pbr_sem).wait_recv()

    p = orthonormalize(jnp.concatenate([p_all[b] for b in range(n_p)], axis=1))
    pt_ref[...] = p
    ps = stack3(p)

    def y_tile(t):
        def part(i):
            return jnp.concatenate(
                [parts[t * (cw // 128) + h, pl.ds(i * d_in, d_in), :] for h in range(cw // 128)], axis=1)
        y = mm(ps, part(2)) + mm(ps, part(1))
        return fold3(y + mm(ps, part(0)))

    mate = me + 1 - 2 * core

    @pl.loop(0, n_half // 2)
    def _(k):
        for i in range(2):
            s = 2 * k + i
            y_mate[s] = y_tile((1 - core) * n_half + s)
        for i in range(2):
            s = 2 * k + i
            remote(y_mate.at[s], y_mate.at[n_half + s], ms_sem, mr_sem.at[s], mate).start()

    @pl.loop(0, n_half // 2)
    def _(k):
        for i in range(2):
            s = 2 * k + i
            bulk(y_mate.at[n_half + s], ms_sem, mr_sem.at[s]).wait_recv()
        for i in range(2):
            s = 2 * k + i
            y_own[s] = y_tile(core * n_half + s) + y_mate[n_half + s]
        for i in range(2):
            s = 2 * k + i
            chip = owner_chip(s)
            slot = lax.rem(lax.div(me, 2) - chip + n - 1, n // 2)

            @pl.when(me != 2 * chip + core)
            def _():
                remote(y_own.at[s], y_recv.at[slot], ys_sem, yr_sem, 2 * chip + core).start()

    p1, p2, p3 = [x.astype(F32) for x in split3(p)]
    fill = jnp.zeros((128 - 9 * RANK, d_in), F32)
    pleft_ref[...] = jnp.concatenate([p1] * 3 + [p2] * 3 + [p3] * 3 + [fill], axis=0).T.astype(BF16)
    q_mine = core * n_half + mine

    @pl.when(central)
    def _():
        bulk(y_recv, ys_sem, yr_sem).wait_recv()
        q_ref[q_mine] = (y_own[mine] + jnp.sum(y_recv[...], axis=0)) * (1.0 / n)
        broadcast(q_ref, q_mine, ybs_sem, ybr_sem, first=2)

    bulk(y_mate.at[pl.ds(0, n_half)], ms_sem, yr_sem).wait_send()

    @pl.when(p_owner)
    def _():
        bulk(p_own.at[pl.ds(0, n_p - 1)], ps_sem, pr_sem).wait_send()
        bulk(p_recv, pbs_sem, pr_sem).wait_send()

    @pl.when(jnp.logical_not(p_owner))
    def _():
        bulk(p_own, ps_sem, pr_sem).wait_send()

    @pl.when(central)
    def _():
        bulk(y_own.at[pl.ds(0, n_half - 1)], ys_sem, yr_sem).wait_send()
        bulk(q_ref.at[pl.ds(0, 2 * n_half - 1)], ybs_sem, ybr_sem).wait_recv()
        bulk(parts.at[0, pl.ds(0, (n - 1) * RANK * cw // 64)], ybs_sem, yr_sem).wait_send()

    @pl.when(jnp.logical_not(central))
    def _():
        bulk(y_own, ys_sem, yr_sem).wait_send()
        bulk(q_ref, ybs_sem, ybr_sem).wait_recv()


def apply_kernel(pleft_ref, pt_ref, q_ref, m_ref, p_out, q_out, e_out, stage, p_sem, q_sem, e_sem):
    d_in, d_out = m_ref.shape
    n_y, _, cw = q_ref.shape
    p_copy = pltpu.make_async_copy(pt_ref, p_out, p_sem)
    fill = jnp.zeros((128 - 9 * RANK, cw), F32)

    def q_copy(c):
        cols = pl.ds(pl.multiple_of(c * cw, cw), cw)
        return pltpu.make_async_copy(q_ref.at[c], q_out.at[:, cols], q_sem)

    def e_copy(c):
        cols = pl.ds(pl.multiple_of(c * cw, cw), cw)
        return pltpu.make_async_copy(stage.at[:, cols], e_out.at[0, :, cols], e_sem)

    @pl.loop(0, n_y)
    def _(c):
        cols = pl.ds(pl.multiple_of(c * cw, cw), cw)
        three = [x.astype(F32) for x in split3(q_ref[c])]
        qc = jnp.concatenate(three * 3 + [fill], axis=0).astype(BF16)
        for r in range(d_in // RB):
            rows = pl.ds(r * RB, RB)
            stage[rows, cols] = m_ref[rows, cols] - mm(pleft_ref[rows, :], qc)
        e_copy(c).start()

    p_copy.start()

    @pl.loop(0, n_y)
    def _(c):
        q_copy(c).start()

    p_copy.wait()
    pltpu.make_async_copy(q_ref, q_ref, q_sem).wait()
    pltpu.make_async_copy(stage, e_out.at[0], e_sem).wait()


def solution(mesh):
    n = mesh.shape["data"]

    def per_device(act_in, pre_act, grad_out, q_init, err_mem):
        tokens, d_in = act_in.shape
        d_out = pre_act.shape[1]
        nc, n_p, n_y = d_out // CB, d_in // 128, n // 2
        cw = d_out // n_y
        hbm = pl.BlockSpec(memory_space=pltpu.HBM)
        vmem = pl.BlockSpec(memory_space=pltpu.VMEM)
        pleft, pt, q, m = pl.pallas_call(
            functools.partial(reduce_kernel, n),
            out_shape=(
                pltpu.VMEM((d_in, 128), BF16),
                pltpu.VMEM((RANK, d_in), F32),
                pltpu.VMEM((n_y, RANK, cw), F32),
                pltpu.VMEM((d_in, d_out), F32),
            ),
            in_specs=[hbm] * 5,
            out_specs=(vmem,) * 4,
            scratch_shapes=[
                pltpu.VMEM((d_out // 128, 3 * d_in, 128), BF16),
                pltpu.VMEM((d_out // 128, tokens, 128), BF16),
                pltpu.VMEM((tokens, d_out), BF16),
                pltpu.VMEM((tokens, d_out), BF16),
                pltpu.VMEM((tokens, d_in), BF16),
                pltpu.VMEM((d_in, tokens), BF16),
                pltpu.VMEM((RANK, d_out), F32),
                pltpu.VMEM((32, d_out), BF16),
                pltpu.VMEM((32, d_in), F32),
                pltpu.VMEM((32, tokens), F32),
                pltpu.VMEM((n_p, RANK, 128), F32),
                pltpu.VMEM((n - 1, RANK, 128), F32),
                pltpu.VMEM((n_p, RANK, 128), F32),
                pltpu.VMEM((n_y, RANK, cw), F32),
                pltpu.VMEM((n_y // 2, RANK, cw), F32),
                pltpu.VMEM((n // 2 - 1, RANK, cw), F32),
                pltpu.SemaphoreType.DMA((nc,)),
            ] + [pltpu.SemaphoreType.DMA] * 7 + [pltpu.SemaphoreType.DMA((n_y // 2,))]
            + [pltpu.SemaphoreType.DMA] * 4,
            compiler_params=pltpu.CompilerParams(
                collective_id=0, has_side_effects=True, vmem_limit_bytes=46 * 1024 * 1024),
            name="reduce_kernel",
        )(act_in, pre_act, grad_out, q_init.T, err_mem)
        p_t, q_t, err_new = pl.pallas_call(
            apply_kernel,
            out_shape=(
                jax.ShapeDtypeStruct((RANK, d_in), F32),
                jax.ShapeDtypeStruct((RANK, d_out), F32),
                jax.ShapeDtypeStruct((1, d_in, d_out), F32),
            ),
            in_specs=[vmem] * 4,
            out_specs=(hbm,) * 3,
            scratch_shapes=[
                pltpu.VMEM((d_in, d_out), F32),
            ] + [pltpu.SemaphoreType.DMA] * 3,
            compiler_params=pltpu.CompilerParams(vmem_limit_bytes=24 * 1024 * 1024),
            name="apply_kernel",
        )(pleft, pt, q, m)
        return p_t.T, q_t.T, err_new

    return jax.shard_map(
        per_device, mesh=mesh,
        in_specs=(P("data", None), P("data", None), P("data", None), P(None, None), P("data", None, None)),
        out_specs=(P(None, None), P(None, None), P("data", None, None)), check_vma=False)
```
